32 devices in a mesh: pts: 8 (over y, x, core), cam: 4 (over z).
Axes of the slice: x: 2, y: 2, z: 4, core: 2. Of those that a mesh axis runs over, the one named last changes fastest.
Arguments:
- cameras: float32 [9, 4096], P(None, ('pts', 'cam')), may hold values from -0.5 to 2
- increment: float32 [9, 4096], P(None, ('pts', 'cam')), may hold values from -0.3 to 0.3
- points: float32 [3, 524288], P(None, 'pts'), may hold values from -6 to 2
- point_gradient: float32 [3, 524288], P(None, 'pts'), may hold values from -1.8 to 1.8
- point_inverse: float32 [9, 524288], P(None, 'pts'), may hold values from -0.35 to 1.6, as said below
- cam_jacobian: bfloat16 [18, 8388608], P(None, ('pts', 'cam')), may hold values from -3 to 3
- point_jacobian: bfloat16 [6, 8388608], P(None, ('pts', 'cam')), may hold values from -3 to 3
- observed: float32 [2, 8388608], P(None, ('pts', 'cam')), may hold values from -10 to 10
- tile_block: int32 [32768], P(('pts', 'cam')), may hold values from 0 to 31
- tile_points: int32 [32768], P(('pts', 'cam')), may hold values from 0 to 255
- obs_camera: int32 [8388608], P(('pts', 'cam')), may hold values from 0 to 127
- obs_point: int32 [8388608], P(('pts', 'cam')), may hold values from 0 to 255
- accept: int32 [], replicated, may hold values from 0 to 1073741823
Outputs:
- residual: float32 [2, 8388608], P(None, ('pts', 'cam'))
- trial_cost: float32 [], replicated
- accepted_points: float32 [3, 524288], P(None, 'pts')
- accepted_cameras: float32 [9, 4096], P(None, ('pts', 'cam'))
The draws below stay inside these ranges and needn't reach their ends.
Inputs may be any that keep to these rules, and one draw needn't show every extreme that they name: `tile_block`: the block of 128 cameras that all 256 observations of a tile look at. `tile_points`: the block of 256 points of its point group that all 256 observations of a tile look at. `obs_camera`: an observation's camera within its tile's block. `obs_point`: an observation's point within its tile's point block. `accept`: an odd word accepts the step, an even one keeps the old parameters. `point_inverse`: each 3 x 3 block is symmetric with a dominant positive diagonal.
All inputs are finite; a program needn't handle non-finite values.
Results may differ from the reference program's by a relative error of at most 0.0003.
Values sent between devices are 32-bit elements; how exact they have to be, the bound alone decides.
A program may use at most 192 MiB of HBM per device.

```python
import math
import jax
import jax.numpy as jnp
from jax import lax

CB = 128
PB = 256
TILE = 256
PTS_DEV = 65536
OBS_GROUP = 1048576
NOBS = 8388608
NPTS = 524288
CAMS = 4096
N_PTS = 8


def draw_cameras(key, part):
    keys = jax.random.split(jax.random.fold_in(key, 11), 4)
    rotation = jax.random.uniform(keys[0], (3, CAMS), jnp.float32, -0.3, 0.3)
    shifted = jnp.clip(0.2 * jax.random.normal(keys[1], (3, CAMS), jnp.float32), -0.5, 0.5)
    focal = jax.random.uniform(keys[2], (1, CAMS), jnp.float32, 0.6, 1.4)
    radial = jax.random.uniform(keys[3], (2, CAMS), jnp.float32, -1.0, 1.0) * jnp.array([[0.05], [0.005]], jnp.float32)
    return jnp.concatenate([rotation, shifted, focal, radial], axis=0)


def draw_increment(key, part):
    keys = jax.random.split(jax.random.fold_in(key, 17), 1)
    scales = jnp.array([0.05, 0.05, 0.05, 0.1, 0.1, 0.1, 0.05, 0.01, 0.002], jnp.float32).reshape(9, 1)
    values = jnp.clip(jax.random.normal(keys[0], (9, CAMS), jnp.float32), -3.0, 3.0)
    return values * scales


def draw_points(key, part):
    keys = jax.random.split(jax.random.fold_in(key, 19), 2)
    planar = jax.random.uniform(keys[0], (2, NPTS), jnp.float32, -2.0, 2.0)
    height = jax.random.uniform(keys[1], (1, NPTS), jnp.float32, -6.0, -0.8)
    return jnp.concatenate([planar, height], axis=0)


def draw_point_inverse(key, part):
    keys = jax.random.split(jax.random.fold_in(key, 23), 2)
    diagonal = jax.random.uniform(keys[0], (3, NPTS), jnp.float32, 0.8, 1.6)
    offdiag = jax.random.uniform(keys[1], (3, NPTS), jnp.float32, -0.35, 0.35)
    return jnp.stack([diagonal[0], offdiag[0], offdiag[1], offdiag[0], diagonal[1], offdiag[2], offdiag[1], offdiag[2], diagonal[2]])


def draw_observed(key, part):
    keys = jax.random.split(jax.random.fold_in(key, 29), 2)
    position = lax_free_iota()
    level = 0.5 * jnp.exp(math.log(3.0) * position / NOBS)
    spread = jnp.exp(jax.random.uniform(keys[1], (2, NOBS), jnp.float32, math.log(0.5), math.log(2.0)))
    values = jnp.clip(jax.random.normal(keys[0], (2, NOBS), jnp.float32), -3.0, 3.0)
    return values * level * spread


def lax_free_iota():
    return jnp.arange(NOBS, dtype=jnp.float32).reshape(1, NOBS)


def plant(entries, key, smallest, high):
    shape = entries.shape
    place = [jax.random.randint(jax.random.fold_in(key, axis), (), 0, shape[axis]) for axis in range(len(shape))]
    entries = entries.at[tuple(place)].set(smallest)
    longest = shape.index(max(shape))
    place[longest] = (place[longest] + 1) % shape[longest]
    return entries.at[tuple(place)].set(high)


def block_scale(own_key, extent, cuts, low, high):
    factor_of, own = 1.0, jax.random.fold_in(own_key, 6)
    for dim, blocks in cuts:
        steps = jnp.exp(jax.random.uniform(jax.random.fold_in(own, dim), (blocks,), jnp.float32, low / len(cuts), high / len(cuts)))
        factor_of = factor_of * jnp.repeat(steps, extent[dim] // blocks).reshape([-1 if axis == dim else 1 for axis in range(len(extent))])
    return factor_of


def centred(rng, shape, width, most, pieces=(), kind=jnp.bfloat16):
    loudness = block_scale(rng, shape, pieces, -0.22, 0.18) if pieces else 1.0
    values = jax.random.normal(rng, shape, jnp.float32) * width * loudness
    return jnp.minimum(jnp.maximum(values, -most), most).astype(kind)


def setup_inputs(seed: int = 0) -> dict:
    arg_keys = jax.random.split(jax.random.key(seed), 14)
    return {
        "cameras": draw_cameras(jax.random.fold_in(arg_keys[13], 71), 0),
        "increment": draw_increment(jax.random.fold_in(arg_keys[13], 71), 0),
        "points": draw_points(jax.random.fold_in(arg_keys[13], 71), 0),
        "point_gradient": centred(arg_keys[3], (3, NPTS), 0.3, 1.8, ((1, 8),), jnp.float32),
        "point_inverse": draw_point_inverse(jax.random.fold_in(arg_keys[13], 71), 0),
        "cam_jacobian": centred(arg_keys[5], (18, NOBS), 0.5, 3.0, ((1, 32),)),
        "point_jacobian": centred(arg_keys[6], (6, NOBS), 0.5, 3.0, ((1, 32),)),
        "observed": draw_observed(jax.random.fold_in(arg_keys[13], 71), 0),
        "tile_block": plant(jax.random.randint(arg_keys[8], (NOBS // TILE,), 0, CAMS // CB), jax.random.fold_in(arg_keys[8], 1), 0, (CAMS // CB) - 1).astype(jnp.int32),
        "tile_points": plant(jax.random.randint(arg_keys[9], (NOBS // TILE,), 0, PTS_DEV // PB), jax.random.fold_in(arg_keys[9], 1), 0, (PTS_DEV // PB) - 1).astype(jnp.int32),
        "obs_camera": plant(jax.random.randint(arg_keys[10], (NOBS,), 0, CB), jax.random.fold_in(arg_keys[10], 1), 0, CB - 1).astype(jnp.int32),
        "obs_point": plant(jax.random.randint(arg_keys[11], (NOBS,), 0, PB), jax.random.fold_in(arg_keys[11], 1), 0, PB - 1).astype(jnp.int32),
        "accept": jax.random.randint(arg_keys[12], (), 0, 1073741824).astype(jnp.int32),
    }


def rotate_point(angles, coords):
    angle_size = jnp.sqrt(lax.optimization_barrier(jnp.sum(angles * angles, axis=0)))
    cosine = jnp.cos(angle_size)
    sine_ratio = jnp.sinc(angle_size / math.pi)
    cosine_ratio = 0.5 * jnp.square(jnp.sinc(angle_size / (2.0 * math.pi)))
    crossed = jnp.stack([angles[1] * coords[2] - angles[2] * coords[1], angles[2] * coords[0] - angles[0] * coords[2], angles[0] * coords[1] - angles[1] * coords[0]])
    inner_part = lax.optimization_barrier(jnp.sum(angles * coords, axis=0))
    return cosine * coords + sine_ratio * crossed + cosine_ratio * inner_part * angles

def project(camera, coords):
    placed = rotate_point(camera[0:3], coords) + camera[3:6]
    depth_clip = jnp.maximum(-placed[2], 1.0)
    planar = placed[0:2] / depth_clip
    radius = lax.optimization_barrier(jnp.sum(planar * planar, axis=0))
    factor = camera[6] * (1.0 + camera[7] * radius + camera[8] * radius * radius)
    return factor * planar

def couple(cam_rows, point_rows, cam_steps):
    cam_rows = cam_rows.astype(jnp.float32)
    point_rows = point_rows.astype(jnp.float32)
    first_row = lax.optimization_barrier(jnp.sum(cam_rows[0:9] * cam_steps, axis=0))
    second_row = lax.optimization_barrier(jnp.sum(cam_rows[9:18] * cam_steps, axis=0))
    return point_rows[0:3] * first_row + point_rows[3:6] * second_row

def solve_points(inverse, gradient, reduced):
    residue = gradient - reduced
    return jnp.stack([inverse[3 * target] * residue[0] + inverse[3 * target + 1] * residue[1] + inverse[3 * target + 2] * residue[2] for target in range(3)])

def reference(cameras, increment, points, point_gradient, point_inverse, cam_jacobian, point_jacobian, observed, tile_block, tile_points, obs_camera, obs_point, accept):
    trial_cameras = cameras + increment
    group_tiles = OBS_GROUP // TILE

    def segment_rows(values, owners):
        return jax.ops.segment_sum(values, owners, num_segments=PTS_DEV)

    def one_group(group_id):
        obs_start = (group_id * OBS_GROUP).astype(jnp.int32)
        tile_start = (group_id * group_tiles).astype(jnp.int32)
        chosen = lax.dynamic_slice_in_dim(tile_block, tile_start, group_tiles, 0)
        chosen_points = lax.dynamic_slice_in_dim(tile_points, tile_start, group_tiles, 0)
        cam_local = lax.dynamic_slice_in_dim(obs_camera, obs_start, OBS_GROUP, 0)
        cam_which = (jnp.repeat(chosen, TILE) * CB + cam_local).astype(jnp.int32)
        step_rows = jnp.take(increment, cam_which, axis=1)
        trial_rows = jnp.take(trial_cameras, cam_which, axis=1)
        coupling = couple(lax.dynamic_slice_in_dim(cam_jacobian, obs_start, OBS_GROUP, 1), lax.dynamic_slice_in_dim(point_jacobian, obs_start, OBS_GROUP, 1), step_rows)
        point_local = lax.dynamic_slice_in_dim(obs_point, obs_start, OBS_GROUP, 0)
        owners = (jnp.repeat(chosen_points, TILE) * PB + point_local).astype(jnp.int32)
        reduced = jax.vmap(segment_rows, in_axes=(0, None))(coupling, owners)
        point_start = (group_id * PTS_DEV).astype(jnp.int32)
        own_points = lax.dynamic_slice_in_dim(points, point_start, PTS_DEV, 1)
        point_step = solve_points(lax.dynamic_slice_in_dim(point_inverse, point_start, PTS_DEV, 1), lax.dynamic_slice_in_dim(point_gradient, point_start, PTS_DEV, 1), reduced)
        seen_points = jnp.take(own_points + point_step, owners, axis=1)
        residual = project(trial_rows, seen_points) - lax.dynamic_slice_in_dim(observed, obs_start, OBS_GROUP, 1)
        return (residual, point_step, jnp.sum(residual * residual))
    residuals, point_steps, partials = lax.map(one_group, jnp.arange(N_PTS, dtype=jnp.int32))
    residual = jnp.transpose(residuals, (1, 0, 2)).reshape(2, NOBS)
    point_step = jnp.transpose(point_steps, (1, 0, 2)).reshape(3, NPTS)
    trial_cost = jnp.sum(partials) / (2.0 * NOBS)
    accepted_flag = jnp.remainder(accept, 2).astype(jnp.float32)
    return (residual, trial_cost, points + accepted_flag * point_step, cameras + accepted_flag * increment)
```

```python
import functools
import math

import jax
import jax.numpy as jnp
from jax import lax
from jax.experimental import pallas as pl
from jax.experimental.pallas import tpu as pltpu
from jax.sharding import PartitionSpec as P

CB = 128
PB = 256
TILE = 256
LANES = 128
GROUP = 8
PITCH = 9
UNROLL = 16
TILES = 8
SPREAD = 8
BLOCKS_PER_STEP = 256
MESH = pl.DeviceIdType.MESH


LANE_GATHER = lax.GatherDimensionNumbers(
    offset_dims=(),
    collapsed_slice_dims=(1,),
    start_index_map=(1,),
    operand_batching_dims=(0,),
    start_indices_batching_dims=(0,),
)


def lane_take(slab, index):
    return lax.gather(
        slab, index[:, :, None], LANE_GATHER, (1, 1), mode=lax.GatherScatterMode.PROMISE_IN_BOUNDS
    )


def row_index(ref, row):
    return jnp.broadcast_to(ref[pl.ds(row, 1), :], (8, LANES))


def couple_kernel(
    tile_block, tile_points, cam_jac, point_jac, obs_cam, obs_point, table, out, total, *scratch
):
    step = pl.program_id(0)
    tiles_per_step = obs_cam.shape[0] // 2
    products, masked = scratch[:UNROLL], scratch[UNROLL:]

    @pl.when(step == 0)
    def _():
        total[...] = jnp.zeros_like(total)
        for buffer in masked:
            buffer[...] = jnp.zeros_like(buffer)

    wide = lax.broadcasted_iota(jnp.int32, (16, LANES), 0).astype(jnp.float32)
    ladders = [(wide + 16.0 * k).astype(jnp.bfloat16) for k in range(8)]
    one = jnp.ones((16, LANES), jnp.bfloat16)
    zero = jnp.zeros((16, LANES), jnp.bfloat16)

    def group(g, prod, mask_rows):
        row = pl.multiple_of(g * GROUP, GROUP)
        tile = step * tiles_per_step + g * (GROUP // 2)
        for s in range(GROUP):
            slab = table.at[tile_block[tile + s // 2]]
            index = row_index(obs_cam, row + s)
            lane = pl.multiple_of((row + s) * LANES, LANES)
            jac = cam_jac[:, pl.ds(lane, LANES)].astype(jnp.float32)
            prod[pl.ds(s, 8, stride=PITCH), :] = jac[0:8] * lane_take(slab[0:8, :], index)
            prod[pl.ds(8 * PITCH + s, 8, stride=PITCH), :] = jac[8:16] * lane_take(slab[8:16, :], index)
            tail = lane_take(slab[16:24, :], index)
            prod[pl.ds(16 * PITCH + s, 2, stride=PITCH), :] = jac[16:18] * tail[0:2]
            pjac = point_jac[:, pl.ds(lane, LANES)].astype(jnp.float32)
            prod[pl.ds(18 * PITCH + s, 6, stride=PITCH), :] = pjac
        rows = [prod[PITCH * m : PITCH * m + 8, :] for m in range(24)]
        first = sum(rows[1:9], rows[0])
        second = sum(rows[10:18], rows[9])
        upper = obs_point[pl.ds(row, GROUP), :] >= LANES
        for n in range(3):
            value = rows[18 + n] * first + rows[21 + n] * second
            mask_rows[PITCH * n : PITCH * n + 8, :] = jnp.where(upper, 0.0, value)
            mask_rows[PITCH * (n + 4) : PITCH * (n + 4) + 8, :] = jnp.where(upper, value, 0.0)
        for t in range(GROUP // 2):
            heads, hots = [], []
            for s in (2 * t, 2 * t + 1):
                value = mask_rows[pl.ds(s, 8, stride=PITCH), :]
                coarse = value.astype(jnp.bfloat16).astype(jnp.float32)
                heads.append(jnp.concatenate([coarse, value - coarse], axis=0).astype(jnp.bfloat16))
                local = (obs_point[pl.ds(row + s, 1), :] & (LANES - 1)).astype(jnp.float32)
                local = jnp.broadcast_to(local, (16, LANES)).astype(jnp.bfloat16)
                hots.append(
                    jnp.concatenate([jnp.where(step_k == local, one, zero) for step_k in ladders], axis=0)
                )
            summed = lax.dot_general(
                jnp.concatenate(heads, axis=1),
                jnp.concatenate(hots, axis=1),
                (((1,), (1,)), ((), ())),
                preferred_element_type=jnp.float32,
            )
            place = pl.ds(pl.multiple_of(tile_points[tile + t] * 8, 8), 8)
            total[place, :] = total[place, :] + (summed[0:8] + summed[8:16])

    def turn(i, carry):
        for u in range(UNROLL):
            group(i * UNROLL + u, products[u], masked[u])
        return carry

    lax.fori_loop(0, obs_cam.shape[0] // (GROUP * UNROLL), turn, 0)

    @pl.when(step == pl.num_programs(0) - 1)
    def _():
        for n in range(3):
            out[n] = total[pl.ds(n, out.shape[1], stride=4), :]


def project_kernel(
    tile_block, tile_points, obs_cam, obs_point, observed, cam_table, trial, residual, cost, point_table, *scratch
):
    step = pl.program_id(0)
    tiles_per_step = obs_cam.shape[0] // 2

    @pl.when(step == 0)
    def _():
        cost[...] = jnp.zeros_like(cost)
        for n in range(3):
            point_table[pl.ds(n, trial.shape[1], stride=4), :] = trial[n]
            point_table[pl.ds(3, trial.shape[1], stride=4), :] = jnp.zeros_like(trial[n])

    def group(block, buf):
        row = pl.multiple_of(block * 2 * TILES, 2 * TILES)
        tile = step * tiles_per_step + block * TILES
        for t in range(TILES):
            slab = cam_table.at[tile_block[tile + t]]
            buf[pl.ds(t, 8, stride=PITCH), :] = slab[0:8, :]
            buf[pl.ds(8 * PITCH + t, 2, stride=PITCH), :] = slab[8:10, :]
            place = pl.ds(pl.multiple_of(tile_points[tile + t] * 8, 8), 8)
            buf[pl.ds(10 * PITCH + t, 8, stride=PITCH), :] = point_table[place, :]
        sources = [buf[PITCH * m : PITCH * m + 8, :] for m in range(18)]
        total = None
        for h in range(2):
            at = pl.ds(row + h, TILES, stride=2)
            index = obs_cam[at, :]
            head, a, b, c, *shift, focal, k1, k2 = (lane_take(sources[m], index) for m in range(10))
            point = obs_point[at, :]
            local = point & (LANES - 1)
            upper = point >= LANES
            x, y, z = (
                jnp.where(upper, lane_take(sources[14 + n], local), lane_take(sources[10 + n], local))
                for n in range(3)
            )
            e, f, g = b * z - c * y, c * x - a * z, a * y - b * x
            px = x + shift[0] + (head * e + (b * g - c * f))
            py = y + shift[1] + (head * f + (c * e - a * g))
            pz = z + shift[2] + (head * g + (a * f - b * e))
            scale = 1.0 / jnp.maximum(-pz, 1.0)
            u, v = px * scale, py * scale
            q = u * u + v * v
            factor = focal * (1.0 + q * (k1 + k2 * q))
            at_u = pl.ds(2 * (row + h), TILES, stride=4)
            at_v = pl.ds(2 * (row + h) + 1, TILES, stride=4)
            ru = factor * u - observed[at_u, :]
            rv = factor * v - observed[at_v, :]
            residual[at_u, :] = ru
            residual[at_v, :] = rv
            square = ru * ru + rv * rv
            total = square if total is None else total + square
        return total

    def turn(i, carry):
        for u in range(SPREAD):
            carry = carry + group(i * SPREAD + u, scratch[u])
        return carry

    cost[...] += lax.fori_loop(
        0, obs_cam.shape[0] // (2 * TILES * SPREAD), turn, jnp.zeros((8, LANES), jnp.float32)
    )


def camera_rows(trial):
    w = trial[0:3]
    angle = jnp.sqrt(jnp.sum(w * w, axis=0, keepdims=True))
    head = math.sqrt(2.0) * jnp.cos(0.5 * angle)
    tail = math.sqrt(0.5) * jnp.sinc(angle / (2.0 * math.pi)) * w
    return jnp.concatenate([head, tail, trial[3:9]], axis=0)


def greet(axis, size, me):
    barrier = pltpu.get_barrier_semaphore()
    for d in range(1, size):
        pl.semaphore_signal(
            barrier, inc=1, device_id={axis: lax.rem(me + d, size)}, device_id_type=MESH
        )


def send_round(axis, size, me, source, target, send, recv):
    copies = []
    for d in range(1, size):
        peer = lax.rem(me + d, size)
        copies.append(
            pltpu.make_async_remote_copy(
                src_ref=source(peer, d),
                dst_ref=target(peer, d),
                send_sem=send.at[d - 1],
                recv_sem=recv.at[d - 1],
                device_id={axis: peer},
                device_id_type=MESH,
            )
        )
    for copy in copies:
        copy.start()
    return copies


def gather_kernel(n_pts, n_cam, own, out, local_sem, send_cam, recv_cam, send_pts, recv_pts):
    p, c = lax.axis_index("pts"), lax.axis_index("cam")
    greet("pts", n_pts, p)
    greet("cam", n_cam, c)
    pl.semaphore_wait(pltpu.get_barrier_semaphore(), n_pts + n_cam - 2)
    count = own.shape[0]
    mine = out.at[pl.ds((p * n_cam + c) * count, count)]
    local = pltpu.make_async_copy(own, mine, local_sem)
    local.start()
    copies = send_round("cam", n_cam, c, lambda *_: own, lambda *_: mine, send_cam, recv_cam)
    local.wait()
    for copy in copies:
        copy.wait()
    slab = out.at[pl.ds(p * n_cam * count, n_cam * count)]
    for copy in send_round("pts", n_pts, p, lambda *_: slab, lambda *_: slab, send_pts, recv_pts):
        copy.wait()


def solve_kernel(
    n_cam, planes, points, gradient, inverse, out,
    landed, own_points, own_gradient, own_inverse, work, in_sem, send_sum, recv_sum, send_out, recv_out,
):
    c = lax.axis_index("cam")
    rows = planes.shape[1] // n_cam
    span, pitch = rows * LANES, rows + 1
    own_lanes = pl.ds(pl.multiple_of(c * span, span), span)
    loads = [
        pltpu.make_async_copy(source.at[:, own_lanes], target, in_sem.at[i])
        for i, (source, target) in enumerate(
            ((points, own_points), (gradient, own_gradient), (inverse, own_inverse))
        )
    ]
    for load in loads:
        load.start()
    greet("cam", n_cam, c)
    pl.semaphore_wait(pltpu.get_barrier_semaphore(), n_cam - 1)

    def part(peer):
        return pl.ds(pl.multiple_of(peer * rows, 8), rows)

    copies = send_round(
        "cam", n_cam, c,
        lambda peer, d: planes.at[:, part(peer)], lambda peer, d: landed.at[d - 1], send_sum, recv_sum,
    )
    for load in loads:
        load.wait()

    def spread(i, carry):
        for u in range(8):
            k = i * 8 + u
            lanes = pl.ds(pl.multiple_of(k * LANES, LANES), LANES)
            work[pl.ds(k, 3, stride=pitch), :] = own_points[:, lanes]
            work[pl.ds(3 * pitch + k, 3, stride=pitch), :] = own_gradient[:, lanes]
            block = own_inverse[:, lanes]
            work[pl.ds(6 * pitch + k, 8, stride=pitch), :] = block[0:8]
            work[pl.ds(14 * pitch + k, 1), :] = block[8:9]
        return carry

    lax.fori_loop(0, rows // 8, spread, 0)
    for copy in copies:
        copy.wait()

    def solve(i, carry):
        at = pl.multiple_of(i * 8, 8)
        own = pl.multiple_of(c * rows + at, 8)

        def row(m):
            return work[pl.ds(m * pitch + at, 8), :]

        residue = []
        for n in range(3):
            value = planes[n, pl.ds(own, 8), :]
            for d in range(n_cam - 1):
                value = value + landed[d, n, pl.ds(at, 8), :]
            residue.append(row(3 + n) - value)
        for n in range(3):
            move = row(6 + 3 * n) * residue[0] + row(7 + 3 * n) * residue[1] + row(8 + 3 * n) * residue[2]
            out[n, pl.ds(own, 8), :] = row(n) + move
        return carry

    lax.fori_loop(0, rows // 8, solve, 0)
    mine = out.at[:, part(c)]
    for copy in send_round("cam", n_cam, c, lambda *_: mine, lambda *_: mine, send_out, recv_out):
        copy.wait()


def total_kernel(n_pts, n_cam, own, out, cam_slots, pts_slots, send_cam, recv_cam, send_pts, recv_pts):
    p, c = lax.axis_index("pts"), lax.axis_index("cam")
    greet("pts", n_pts, p)
    greet("cam", n_cam, c)
    cam_slots[c] = own[...]
    pl.semaphore_wait(pltpu.get_barrier_semaphore(), n_pts + n_cam - 2)
    slot = cam_slots.at[c]
    for copy in send_round("cam", n_cam, c, lambda *_: own, lambda *_: slot, send_cam, recv_cam):
        copy.wait()
    value = cam_slots[0]
    for i in range(1, n_cam):
        value = value + cam_slots[i]
    pts_slots[p] = value
    slot = pts_slots.at[p]
    for copy in send_round("pts", n_pts, p, lambda *_: slot, lambda *_: slot, send_pts, recv_pts):
        copy.wait()
    value = pts_slots[0]
    for i in range(1, n_pts):
        value = value + pts_slots[i]
    out[...] = value


def on_device(
    cameras, increment, points, point_gradient, point_inverse, cam_jacobian, point_jacobian,
    observed, tile_block, tile_points, obs_camera, obs_point, accept,
):
    own_blocks = cameras.shape[1] // CB
    own = jnp.concatenate(
        [increment, camera_rows(cameras + increment), jnp.zeros((5, cameras.shape[1]), jnp.float32)], axis=0
    )
    own = own.reshape(24, own_blocks, CB).transpose(1, 0, 2)
    n_pts, n_cam = lax.axis_size("pts"), lax.axis_size("cam")
    vmem = pl.BlockSpec(memory_space=pltpu.VMEM)

    def dma_sems(*counts):
        return [pltpu.SemaphoreType.DMA((count,)) for count in counts]

    def remote(ident):
        return pltpu.CompilerParams(
            collective_id=ident, has_side_effects=True, vmem_limit_bytes=50 * 2**20
        )

    every = pl.pallas_call(
        functools.partial(gather_kernel, n_pts, n_cam),
        in_specs=[vmem],
        out_specs=vmem,
        out_shape=jax.ShapeDtypeStruct((own_blocks * n_pts * n_cam, 24, CB), jnp.float32),
        scratch_shapes=[pltpu.SemaphoreType.DMA]
        + dma_sems(n_cam - 1, n_cam - 1, n_pts - 1, n_pts - 1),
        compiler_params=remote(0),
        name="cameras",
    )(own)
    cam_blocks = every.shape[0]
    steps = every[:, 0:9]
    step_table = jnp.concatenate([steps, steps, jnp.zeros((cam_blocks, 6, CB), jnp.float32)], axis=1)
    cam_table = jnp.concatenate([every[:, 9:19], jnp.zeros((cam_blocks, 6, CB), jnp.float32)], axis=1)

    obs_count = obs_camera.shape[0]
    rows = obs_count // LANES
    per = math.gcd(rows, BLOCKS_PER_STEP)
    grid = (rows // per,)
    point_blocks = points.shape[1] // PB
    oc = obs_camera.reshape(rows, LANES)
    op = obs_point.reshape(rows, LANES)

    def whole(*shape):
        return pl.BlockSpec(shape, lambda i, *_: (0,) * len(shape))

    params = pltpu.CompilerParams(dimension_semantics=("arbitrary",), vmem_limit_bytes=50 * 2**20)
    planes = pl.pallas_call(
        couple_kernel,
        grid_spec=pltpu.PrefetchScalarGridSpec(
            num_scalar_prefetch=2,
            grid=grid,
            in_specs=[
                pl.BlockSpec((18, per * LANES), lambda i, *_: (0, i)),
                pl.BlockSpec((6, per * LANES), lambda i, *_: (0, i)),
                pl.BlockSpec((per, LANES), lambda i, *_: (i, 0)),
                pl.BlockSpec((per, LANES), lambda i, *_: (i, 0)),
                whole(cam_blocks, 24, CB),
            ],
            out_specs=whole(3, 2 * point_blocks, LANES),
            scratch_shapes=[pltpu.VMEM((point_blocks * 8, LANES), jnp.float32)]
            + [pltpu.VMEM((24 * PITCH, LANES), jnp.float32)] * UNROLL
            + [pltpu.VMEM((8 * PITCH, LANES), jnp.float32)] * UNROLL,
        ),
        out_shape=jax.ShapeDtypeStruct((3, 2 * point_blocks, LANES), jnp.float32),
        compiler_params=params,
        name="couple",
    )(tile_block, tile_points, cam_jacobian, point_jacobian, oc, op, step_table)

    own_rows = 2 * point_blocks // n_cam
    hbm = pl.BlockSpec(memory_space=pl.ANY)
    trial = pl.pallas_call(
        functools.partial(solve_kernel, n_cam),
        in_specs=[vmem, hbm, hbm, hbm],
        out_specs=vmem,
        out_shape=jax.ShapeDtypeStruct(planes.shape, jnp.float32),
        scratch_shapes=[
            pltpu.VMEM((n_cam - 1, 3, own_rows, LANES), jnp.float32),
            pltpu.VMEM((3, own_rows * LANES), jnp.float32),
            pltpu.VMEM((3, own_rows * LANES), jnp.float32),
            pltpu.VMEM((9, own_rows * LANES), jnp.float32),
            pltpu.VMEM((15 * (own_rows + 1), LANES), jnp.float32),
        ]
        + dma_sems(3, n_cam - 1, n_cam - 1, n_cam - 1, n_cam - 1),
        compiler_params=remote(1),
        name="solve",
    )(planes, points, point_gradient, point_inverse)

    seen = observed.reshape(2, rows, LANES).transpose(1, 0, 2).reshape(2 * rows, LANES)
    residual, partial = pl.pallas_call(
        project_kernel,
        grid_spec=pltpu.PrefetchScalarGridSpec(
            num_scalar_prefetch=2,
            grid=grid,
            in_specs=[
                pl.BlockSpec((per, LANES), lambda i, *_: (i, 0)),
                pl.BlockSpec((per, LANES), lambda i, *_: (i, 0)),
                pl.BlockSpec((2 * per, LANES), lambda i, *_: (i, 0)),
                whole(cam_blocks, 16, CB),
                whole(3, 2 * point_blocks, LANES),
            ],
            out_specs=[
                pl.BlockSpec((2 * per, LANES), lambda i, *_: (i, 0)),
                whole(8, LANES),
            ],
            scratch_shapes=[pltpu.VMEM((point_blocks * 8, LANES), jnp.float32)]
            + [pltpu.VMEM((18 * PITCH, LANES), jnp.float32)] * SPREAD,
        ),
        out_shape=[
            jax.ShapeDtypeStruct((2 * rows, LANES), jnp.float32),
            jax.ShapeDtypeStruct((8, LANES), jnp.float32),
        ],
        compiler_params=params,
        name="project",
    )(tile_block, tile_points, oc, op, seen, cam_table, trial)
    residual = residual.reshape(rows, 2, LANES).transpose(1, 0, 2).reshape(2, obs_count)
    sums = pl.pallas_call(
        functools.partial(total_kernel, n_pts, n_cam),
        in_specs=[vmem],
        out_specs=vmem,
        out_shape=jax.ShapeDtypeStruct((8, LANES), jnp.float32),
        scratch_shapes=[
            pltpu.VMEM((n_cam, 8, LANES), jnp.float32),
            pltpu.VMEM((n_pts, 8, LANES), jnp.float32),
        ]
        + dma_sems(n_cam - 1, n_cam - 1, n_pts - 1, n_pts - 1),
        compiler_params=remote(2),
        name="total",
    )(partial)
    trial_cost = jnp.sum(sums) / (2.0 * obs_count * n_pts * n_cam)
    odd = jnp.remainder(accept, 2)
    accepted_points = jnp.where(odd == 1, trial.reshape(3, -1), points)
    return residual, trial_cost, accepted_points, cameras + odd.astype(jnp.float32) * increment


def solution(mesh):
    in_specs = (
        P(None, ("pts", "cam")),
        P(None, ("pts", "cam")),
        P(None, "pts"),
        P(None, "pts"),
        P(None, "pts"),
        P(None, ("pts", "cam")),
        P(None, ("pts", "cam")),
        P(None, ("pts", "cam")),
        P(("pts", "cam")),
        P(("pts", "cam")),
        P(("pts", "cam")),
        P(("pts", "cam")),
        P(),
    )
    out_specs = (P(None, ("pts", "cam")), P(), P(None, "pts"), P(None, ("pts", "cam")))
    return jax.shard_map(
        on_device, mesh=mesh, in_specs=in_specs, out_specs=out_specs, check_vma=False
    )
```

```python
import functools
import math

import jax
import jax.numpy as jnp
from jax import lax
from jax.experimental import pallas as pl
from jax.experimental.pallas import tpu as pltpu
from jax.sharding import PartitionSpec as P

CB = 128
PB = 256
TILE = 256
LANES = 128
PITCH = 9
FINE = 64
FINE_BITS = 6
COARSE_ROWS = 32
PAIRS = 8
TILES = 8
SPREAD = 8
BLOCKS_PER_STEP = 256
MESH = pl.DeviceIdType.MESH


LANE_GATHER = lax.GatherDimensionNumbers(
    offset_dims=(),
    collapsed_slice_dims=(1,),
    start_index_map=(1,),
    operand_batching_dims=(0,),
    start_indices_batching_dims=(0,),
)


def lane_take(slab, index):
    return lax.gather(
        slab, index[:, :, None], LANE_GATHER, (1, 1), mode=lax.GatherScatterMode.PROMISE_IN_BOUNDS
    )


def couple_kernel(
    tile_block, tile_points, cam_jac, point_jac, obs_cam, obs_point, table, out, total, packed, *scratch
):
    step = pl.program_id(0)
    tiles_per_step = obs_cam.shape[0] // 2
    buffers = [scratch[5 * u : 5 * u + 5] for u in range(PAIRS)]
    blocks = packed.shape[0] // 8

    @pl.when(step == 0)
    def _():
        total[...] = jnp.zeros_like(total)
        for _, _, _, low, high in buffers:
            low[...] = jnp.zeros_like(low)
            high[...] = jnp.zeros_like(high)

    wide = lax.broadcasted_iota(jnp.int32, (16, LANES), 0)
    fine = [(wide + 16 * k).astype(jnp.float32).astype(jnp.bfloat16) for k in range(FINE // 16)]
    half = (wide >= 8).astype(jnp.float32)
    coarse = [(half + 2.0 * k).astype(jnp.bfloat16) for k in range(PB // FINE // 2)]
    one = jnp.ones((16, LANES), jnp.bfloat16)
    zero = jnp.zeros((16, LANES), jnp.bfloat16)

    def twice(row):
        return jnp.broadcast_to(row, (16, LANES)).astype(jnp.bfloat16)

    def group(block, steps, *halves):
        jacs, sides = halves[:2], halves[2:]
        row = pl.multiple_of(block * 2 * TILES, 2 * TILES)
        tile = step * tiles_per_step + block * TILES
        for t in range(TILES):
            slab = table.at[tile_block[tile + t]]
            steps[pl.ds(t, 8, stride=PITCH), :] = slab[0:8, :]
            steps[pl.ds(8 * PITCH + t, 1), :] = slab[8:9, :]
            for h in range(2):
                lane = pl.ds(pl.multiple_of((row + 2 * t + h) * LANES, LANES), LANES)
                jac = cam_jac[:, lane].astype(jnp.float32)
                jacs[h][pl.ds(t, 8, stride=PITCH), :] = jac[0:8]
                jacs[h][pl.ds(8 * PITCH + t, 8, stride=PITCH), :] = jac[8:16]
                jacs[h][pl.ds(16 * PITCH + t, 2, stride=PITCH), :] = jac[16:18]
                jacs[h][pl.ds(18 * PITCH + t, 6, stride=PITCH), :] = point_jac[:, lane].astype(jnp.float32)
        sources = [steps[PITCH * m : PITCH * m + 8, :] for m in range(9)]
        for h in range(2):
            at = pl.ds(row + h, TILES, stride=2)
            index = obs_cam[at, :]
            moves = [lane_take(source, index) for source in sources]
            jac = [jacs[h][PITCH * m : PITCH * m + 8, :] for m in range(24)]
            first = sum((jac[m] * moves[m] for m in range(1, 9)), jac[0] * moves[0])
            second = sum((jac[9 + m] * moves[m] for m in range(1, 9)), jac[9] * moves[0])
            side = sides[h]
            for n in range(3):
                value = jac[18 + n] * first + jac[21 + n] * second
                head = value.astype(jnp.bfloat16).astype(jnp.float32)
                side[PITCH * n : PITCH * n + 8, :] = head
                side[PITCH * (n + 4) : PITCH * (n + 4) + 8, :] = value - head
            point = obs_point[at, :]
            side[PITCH * 8 : PITCH * 8 + 8, :] = (point & (FINE - 1)).astype(jnp.float32)
            side[PITCH * 9 : PITCH * 9 + 8, :] = (point >> FINE_BITS).astype(jnp.float32)
        for t in range(TILES):
            heads, hots = [], []
            for h in range(2):
                value = sides[h][pl.ds(t, 8, stride=PITCH), :]
                value = jnp.concatenate([value, value], axis=0).astype(jnp.bfloat16)
                low = twice(sides[h][pl.ds(8 * PITCH + t, 1), :])
                high = twice(sides[h][pl.ds(9 * PITCH + t, 1), :])
                heads.append(jnp.concatenate([jnp.where(k == high, value, zero) for k in coarse], axis=0))
                hots.append(jnp.concatenate([jnp.where(k == low, one, zero) for k in fine], axis=0))
            summed = lax.dot_general(
                jnp.concatenate(heads, axis=1),
                jnp.concatenate(hots, axis=1),
                (((1,), (1,)), ((), ())),
                preferred_element_type=jnp.float32,
            )
            place = pl.ds(pl.multiple_of(tile_points[tile + t] * COARSE_ROWS, COARSE_ROWS), COARSE_ROWS)
            total[place, :] = total[place, :] + summed

    def turn(i, carry):
        for u in range(PAIRS):
            group(i * PAIRS + u, *buffers[u])
        return carry

    lax.fori_loop(0, obs_cam.shape[0] // (2 * TILES * PAIRS), turn, 0)

    @pl.when(step == pl.num_programs(0) - 1)
    def _():
        top = lax.broadcasted_iota(jnp.int32, (8, LANES), 0) < 4

        def fold(i, carry):
            for u in range(8):
                k = i * 8 + u
                base = pl.multiple_of(k * COARSE_ROWS, COARSE_ROWS)
                parts = [total[pl.ds(base + 8 * j, 8), :] for j in range(4)]
                pair = [jnp.concatenate(parts[2 * j : 2 * j + 2], axis=1) for j in range(2)]
                pair = [value + pltpu.roll(value, 4, 0) for value in pair]
                packed[pl.ds(pl.multiple_of(k * 8, 8), 8), :] = jnp.where(top, *pair)
            return carry

        lax.fori_loop(0, blocks // 8, fold, 0)
        for n in range(3):
            out[n] = packed[pl.ds(n, out.shape[1], stride=4), :]


def project_kernel(
    tile_block, tile_points, obs_cam, obs_point, observed, cam_table, trial, residual, cost, point_table, *scratch
):
    step = pl.program_id(0)
    tiles_per_step = obs_cam.shape[0] // 2

    @pl.when(step == 0)
    def _():
        cost[...] = jnp.zeros_like(cost)
        for n in range(3):
            point_table[pl.ds(n, trial.shape[1], stride=4), :] = trial[n]
            point_table[pl.ds(3, trial.shape[1], stride=4), :] = jnp.zeros_like(trial[n])

    def group(block, buf):
        row = pl.multiple_of(block * 2 * TILES, 2 * TILES)
        tile = step * tiles_per_step + block * TILES
        for t in range(TILES):
            slab = cam_table.at[tile_block[tile + t]]
            buf[pl.ds(t, 8, stride=PITCH), :] = slab[0:8, :]
            buf[pl.ds(8 * PITCH + t, 2, stride=PITCH), :] = slab[8:10, :]
            place = pl.ds(pl.multiple_of(tile_points[tile + t] * 8, 8), 8)
            buf[pl.ds(10 * PITCH + t, 8, stride=PITCH), :] = point_table[place, :]
        sources = [buf[PITCH * m : PITCH * m + 8, :] for m in range(18)]
        total = None
        for h in range(2):
            at = pl.ds(row + h, TILES, stride=2)
            index = obs_cam[at, :]
            head, a, b, c, *shift, focal, k1, k2 = (lane_take(sources[m], index) for m in range(10))
            point = obs_point[at, :]
            local = point & (LANES - 1)
            upper = point >= LANES
            x, y, z = (
                jnp.where(upper, lane_take(sources[14 + n], local), lane_take(sources[10 + n], local))
                for n in range(3)
            )
            e, f, g = b * z - c * y, c * x - a * z, a * y - b * x
            px = x + shift[0] + (head * e + (b * g - c * f))
            py = y + shift[1] + (head * f + (c * e - a * g))
            pz = z + shift[2] + (head * g + (a * f - b * e))
            scale = 1.0 / jnp.maximum(-pz, 1.0)
            u, v = px * scale, py * scale
            q = u * u + v * v
            factor = focal * (1.0 + q * (k1 + k2 * q))
            at_u = pl.ds(2 * (row + h), TILES, stride=4)
            at_v = pl.ds(2 * (row + h) + 1, TILES, stride=4)
            ru = factor * u - observed[at_u, :]
            rv = factor * v - observed[at_v, :]
            residual[at_u, :] = ru
            residual[at_v, :] = rv
            square = ru * ru + rv * rv
            total = square if total is None else total + square
        return total

    def turn(i, carry):
        for u in range(SPREAD):
            carry = carry + group(i * SPREAD + u, scratch[u])
        return carry

    cost[...] += lax.fori_loop(
        0, obs_cam.shape[0] // (2 * TILES * SPREAD), turn, jnp.zeros((8, LANES), jnp.float32)
    )


def camera_rows(trial):
    w = trial[0:3]
    angle = jnp.sqrt(jnp.sum(w * w, axis=0, keepdims=True))
    head = math.sqrt(2.0) * jnp.cos(0.5 * angle)
    tail = math.sqrt(0.5) * jnp.sinc(angle / (2.0 * math.pi)) * w
    return jnp.concatenate([head, tail, trial[3:9]], axis=0)


def greet(axis, size, me):
    barrier = pltpu.get_barrier_semaphore()
    for d in range(1, size):
        pl.semaphore_signal(
            barrier, inc=1, device_id={axis: lax.rem(me + d, size)}, device_id_type=MESH
        )


def send_round(axis, size, me, source, target, send, recv):
    copies = []
    for d in range(1, size):
        peer = lax.rem(me + d, size)
        copies.append(
            pltpu.make_async_remote_copy(
                src_ref=source(peer, d),
                dst_ref=target(peer, d),
                send_sem=send.at[d - 1],
                recv_sem=recv.at[d - 1],
                device_id={axis: peer},
                device_id_type=MESH,
            )
        )
    for copy in copies:
        copy.start()
    return copies


def gather_kernel(n_pts, n_cam, own, out, local_sem, send_cam, recv_cam, send_pts, recv_pts):
    p, c = lax.axis_index("pts"), lax.axis_index("cam")
    greet("pts", n_pts, p)
    greet("cam", n_cam, c)
    pl.semaphore_wait(pltpu.get_barrier_semaphore(), n_pts + n_cam - 2)
    count = own.shape[0]
    mine = out.at[pl.ds((p * n_cam + c) * count, count)]
    local = pltpu.make_async_copy(own, mine, local_sem)
    local.start()
    copies = send_round("cam", n_cam, c, lambda *_: own, lambda *_: mine, send_cam, recv_cam)
    local.wait()
    for copy in copies:
        copy.wait()
    slab = out.at[pl.ds(p * n_cam * count, n_cam * count)]
    for copy in send_round("pts", n_pts, p, lambda *_: slab, lambda *_: slab, send_pts, recv_pts):
        copy.wait()


def solve_kernel(
    n_cam, planes, points, gradient, inverse, out,
    landed, own_points, own_gradient, own_inverse, work, in_sem, send_sum, recv_sum, send_out, recv_out,
):
    c = lax.axis_index("cam")
    rows = planes.shape[1] // n_cam
    span, pitch = rows * LANES, rows + 1
    own_lanes = pl.ds(pl.multiple_of(c * span, span), span)
    loads = [
        pltpu.make_async_copy(source.at[:, own_lanes], target, in_sem.at[i])
        for i, (source, target) in enumerate(
            ((points, own_points), (gradient, own_gradient), (inverse, own_inverse))
        )
    ]
    for load in loads:
        load.start()
    greet("cam", n_cam, c)
    pl.semaphore_wait(pltpu.get_barrier_semaphore(), n_cam - 1)

    def part(peer):
        return pl.ds(pl.multiple_of(peer * rows, 8), rows)

    copies = send_round(
        "cam", n_cam, c,
        lambda peer, d: planes.at[:, part(peer)], lambda peer, d: landed.at[d - 1], send_sum, recv_sum,
    )
    for load in loads:
        load.wait()

    def spread(i, carry):
        for u in range(8):
            k = i * 8 + u
            lanes = pl.ds(pl.multiple_of(k * LANES, LANES), LANES)
            work[pl.ds(k, 3, stride=pitch), :] = own_points[:, lanes]
            work[pl.ds(3 * pitch + k, 3, stride=pitch), :] = own_gradient[:, lanes]
            block = own_inverse[:, lanes]
            work[pl.ds(6 * pitch + k, 8, stride=pitch), :] = block[0:8]
            work[pl.ds(14 * pitch + k, 1), :] = block[8:9]
        return carry

    lax.fori_loop(0, rows // 8, spread, 0)
    for copy in copies:
        copy.wait()

    def solve(i, carry):
        at = pl.multiple_of(i * 8, 8)
        own = pl.multiple_of(c * rows + at, 8)

        def row(m):
            return work[pl.ds(m * pitch + at, 8), :]

        residue = []
        for n in range(3):
            value = planes[n, pl.ds(own, 8), :]
            for d in range(n_cam - 1):
                value = value + landed[d, n, pl.ds(at, 8), :]
            residue.append(row(3 + n) - value)
        for n in range(3):
            move = row(6 + 3 * n) * residue[0] + row(7 + 3 * n) * residue[1] + row(8 + 3 * n) * residue[2]
            out[n, pl.ds(own, 8), :] = row(n) + move
        return carry

    lax.fori_loop(0, rows // 8, solve, 0)
    mine = out.at[:, part(c)]
    for copy in send_round("cam", n_cam, c, lambda *_: mine, lambda *_: mine, send_out, recv_out):
        copy.wait()


def total_kernel(n_pts, n_cam, own, out, cam_slots, pts_slots, send_cam, recv_cam, send_pts, recv_pts):
    p, c = lax.axis_index("pts"), lax.axis_index("cam")
    greet("pts", n_pts, p)
    greet("cam", n_cam, c)
    cam_slots[c] = own[...]
    pl.semaphore_wait(pltpu.get_barrier_semaphore(), n_pts + n_cam - 2)
    slot = cam_slots.at[c]
    for copy in send_round("cam", n_cam, c, lambda *_: own, lambda *_: slot, send_cam, recv_cam):
        copy.wait()
    value = cam_slots[0]
    for i in range(1, n_cam):
        value = value + cam_slots[i]
    pts_slots[p] = value
    slot = pts_slots.at[p]
    for copy in send_round("pts", n_pts, p, lambda *_: slot, lambda *_: slot, send_pts, recv_pts):
        copy.wait()
    value = pts_slots[0]
    for i in range(1, n_pts):
        value = value + pts_slots[i]
    out[...] = value


def on_device(
    cameras, increment, points, point_gradient, point_inverse, cam_jacobian, point_jacobian,
    observed, tile_block, tile_points, obs_camera, obs_point, accept,
):
    own_blocks = cameras.shape[1] // CB
    own = jnp.concatenate(
        [increment, camera_rows(cameras + increment), jnp.zeros((5, cameras.shape[1]), jnp.float32)], axis=0
    )
    own = own.reshape(24, own_blocks, CB).transpose(1, 0, 2)
    n_pts, n_cam = lax.axis_size("pts"), lax.axis_size("cam")
    vmem = pl.BlockSpec(memory_space=pltpu.VMEM)

    def dma_sems(*counts):
        return [pltpu.SemaphoreType.DMA((count,)) for count in counts]

    def remote(ident):
        return pltpu.CompilerParams(
            collective_id=ident, has_side_effects=True, vmem_limit_bytes=50 * 2**20
        )

    every = pl.pallas_call(
        functools.partial(gather_kernel, n_pts, n_cam),
        in_specs=[vmem],
        out_specs=vmem,
        out_shape=jax.ShapeDtypeStruct((own_blocks * n_pts * n_cam, 24, CB), jnp.float32),
        scratch_shapes=[pltpu.SemaphoreType.DMA]
        + dma_sems(n_cam - 1, n_cam - 1, n_pts - 1, n_pts - 1),
        compiler_params=remote(0),
        name="cameras",
    )(own)
    cam_blocks = every.shape[0]
    step_table = jnp.concatenate([every[:, 0:9], jnp.zeros((cam_blocks, 7, CB), jnp.float32)], axis=1)
    cam_table = jnp.concatenate([every[:, 9:19], jnp.zeros((cam_blocks, 6, CB), jnp.float32)], axis=1)

    obs_count = obs_camera.shape[0]
    rows = obs_count // LANES
    per = math.gcd(rows, BLOCKS_PER_STEP)
    grid = (rows // per,)
    point_blocks = points.shape[1] // PB
    oc = obs_camera.reshape(rows, LANES)
    op = obs_point.reshape(rows, LANES)

    def whole(*shape):
        return pl.BlockSpec(shape, lambda i, *_: (0,) * len(shape))

    params = pltpu.CompilerParams(dimension_semantics=("arbitrary",), vmem_limit_bytes=50 * 2**20)
    planes = pl.pallas_call(
        couple_kernel,
        grid_spec=pltpu.PrefetchScalarGridSpec(
            num_scalar_prefetch=2,
            grid=grid,
            in_specs=[
                pl.BlockSpec((18, per * LANES), lambda i, *_: (0, i)),
                pl.BlockSpec((6, per * LANES), lambda i, *_: (0, i)),
                pl.BlockSpec((per, LANES), lambda i, *_: (i, 0)),
                pl.BlockSpec((per, LANES), lambda i, *_: (i, 0)),
                whole(cam_blocks, 16, CB),
            ],
            out_specs=whole(3, 2 * point_blocks, LANES),
            scratch_shapes=[
                pltpu.VMEM((point_blocks * COARSE_ROWS, FINE), jnp.float32),
                pltpu.VMEM((point_blocks * 8, LANES), jnp.float32),
            ]
            + [
                pltpu.VMEM((count * PITCH, LANES), jnp.float32) for count in (9, 24, 24, 10, 10)
            ]
            * PAIRS,
        ),
        out_shape=jax.ShapeDtypeStruct((3, 2 * point_blocks, LANES), jnp.float32),
        compiler_params=params,
        name="couple",
    )(tile_block, tile_points, cam_jacobian, point_jacobian, oc, op, step_table)

    own_rows = 2 * point_blocks // n_cam
    hbm = pl.BlockSpec(memory_space=pl.ANY)
    trial = pl.pallas_call(
        functools.partial(solve_kernel, n_cam),
        in_specs=[vmem, hbm, hbm, hbm],
        out_specs=vmem,
        out_shape=jax.ShapeDtypeStruct(planes.shape, jnp.float32),
        scratch_shapes=[
            pltpu.VMEM((n_cam - 1, 3, own_rows, LANES), jnp.float32),
            pltpu.VMEM((3, own_rows * LANES), jnp.float32),
            pltpu.VMEM((3, own_rows * LANES), jnp.float32),
            pltpu.VMEM((9, own_rows * LANES), jnp.float32),
            pltpu.VMEM((15 * (own_rows + 1), LANES), jnp.float32),
        ]
        + dma_sems(3, n_cam - 1, n_cam - 1, n_cam - 1, n_cam - 1),
        compiler_params=remote(1),
        name="solve",
    )(planes, points, point_gradient, point_inverse)

    seen = observed.reshape(2, rows, LANES).transpose(1, 0, 2).reshape(2 * rows, LANES)
    residual, partial = pl.pallas_call(
        project_kernel,
        grid_spec=pltpu.PrefetchScalarGridSpec(
            num_scalar_prefetch=2,
            grid=grid,
            in_specs=[
                pl.BlockSpec((per, LANES), lambda i, *_: (i, 0)),
                pl.BlockSpec((per, LANES), lambda i, *_: (i, 0)),
                pl.BlockSpec((2 * per, LANES), lambda i, *_: (i, 0)),
                whole(cam_blocks, 16, CB),
                whole(3, 2 * point_blocks, LANES),
            ],
            out_specs=[
                pl.BlockSpec((2 * per, LANES), lambda i, *_: (i, 0)),
                whole(8, LANES),
            ],
            scratch_shapes=[pltpu.VMEM((point_blocks * 8, LANES), jnp.float32)]
            + [pltpu.VMEM((18 * PITCH, LANES), jnp.float32)] * SPREAD,
        ),
        out_shape=[
            jax.ShapeDtypeStruct((2 * rows, LANES), jnp.float32),
            jax.ShapeDtypeStruct((8, LANES), jnp.float32),
        ],
        compiler_params=params,
        name="project",
    )(tile_block, tile_points, oc, op, seen, cam_table, trial)
    residual = residual.reshape(rows, 2, LANES).transpose(1, 0, 2).reshape(2, obs_count)
    sums = pl.pallas_call(
        functools.partial(total_kernel, n_pts, n_cam),
        in_specs=[vmem],
        out_specs=vmem,
        out_shape=jax.ShapeDtypeStruct((8, LANES), jnp.float32),
        scratch_shapes=[
            pltpu.VMEM((n_cam, 8, LANES), jnp.float32),
            pltpu.VMEM((n_pts, 8, LANES), jnp.float32),
        ]
        + dma_sems(n_cam - 1, n_cam - 1, n_pts - 1, n_pts - 1),
        compiler_params=remote(2),
        name="total",
    )(partial)
    trial_cost = jnp.sum(sums) / (2.0 * obs_count * n_pts * n_cam)
    odd = jnp.remainder(accept, 2)
    accepted_points = jnp.where(odd == 1, trial.reshape(3, -1), points)
    return residual, trial_cost, accepted_points, cameras + odd.astype(jnp.float32) * increment


def solution(mesh):
    in_specs = (
        P(None, ("pts", "cam")),
        P(None, ("pts", "cam")),
        P(None, "pts"),
        P(None, "pts"),
        P(None, "pts"),
        P(None, ("pts", "cam")),
        P(None, ("pts", "cam")),
        P(None, ("pts", "cam")),
        P(("pts", "cam")),
        P(("pts", "cam")),
        P(("pts", "cam")),
        P(("pts", "cam")),
        P(),
    )
    out_specs = (P(None, ("pts", "cam")), P(), P(None, "pts"), P(None, ("pts", "cam")))
    return jax.shard_map(
        on_device, mesh=mesh, in_specs=in_specs, out_specs=out_specs, check_vma=False
    )
```

```python
import functools
import math

import jax
import jax.numpy as jnp
from jax import lax
from jax.experimental import pallas as pl
from jax.experimental.pallas import tpu as pltpu
from jax.sharding import PartitionSpec as P

CB = 128
PB = 256
TILE = 256
LANES = 128
PITCH = 9
FINE = 64
FINE_BITS = 6
COARSE_ROWS = 32
PAIRS = 8
TILES = 8
SPREAD = 8
CHUNKS = 16
LAG = 4
BLOCKS_PER_STEP = 256
MESH = pl.DeviceIdType.MESH


LANE_GATHER = lax.GatherDimensionNumbers(
    offset_dims=(),
    collapsed_slice_dims=(1,),
    start_index_map=(1,),
    operand_batching_dims=(0,),
    start_indices_batching_dims=(0,),
)


def lane_take(slab, index):
    return lax.gather(
        slab, index[:, :, None], LANE_GATHER, (1, 1), mode=lax.GatherScatterMode.PROMISE_IN_BOUNDS
    )


def couple_kernel(
    tile_block, tile_points, cam_jac, point_jac, obs_cam, obs_point, table, out, total, packed, *scratch
):
    step = pl.program_id(0)
    tiles_per_step = obs_cam.shape[0] // 2
    buffers = [scratch[5 * u : 5 * u + 5] for u in range(PAIRS)]
    blocks = packed.shape[0] // 8

    @pl.when(step == 0)
    def _():
        total[...] = jnp.zeros_like(total)
        for _, _, _, low, high in buffers:
            low[...] = jnp.zeros_like(low)
            high[...] = jnp.zeros_like(high)

    wide = lax.broadcasted_iota(jnp.int32, (16, LANES), 0)
    fine = [(wide + 16 * k).astype(jnp.float32).astype(jnp.bfloat16) for k in range(FINE // 16)]
    half = (wide >= 8).astype(jnp.float32)
    coarse = [(half + 2.0 * k).astype(jnp.bfloat16) for k in range(PB // FINE // 2)]
    one = jnp.ones((16, LANES), jnp.bfloat16)
    zero = jnp.zeros((16, LANES), jnp.bfloat16)

    def twice(row):
        return jnp.broadcast_to(row, (16, LANES)).astype(jnp.bfloat16)

    def group(block, steps, *halves):
        jacs, sides = halves[:2], halves[2:]
        row = pl.multiple_of(block * 2 * TILES, 2 * TILES)
        tile = step * tiles_per_step + block * TILES
        for t in range(TILES):
            slab = table.at[tile_block[tile + t]]
            steps[pl.ds(t, 8, stride=PITCH), :] = slab[0:8, :]
            steps[pl.ds(8 * PITCH + t, 1), :] = slab[8:9, :]
            for h in range(2):
                lane = pl.ds(pl.multiple_of((row + 2 * t + h) * LANES, LANES), LANES)
                jac = cam_jac[:, lane].astype(jnp.float32)
                jacs[h][pl.ds(t, 8, stride=PITCH), :] = jac[0:8]
                jacs[h][pl.ds(8 * PITCH + t, 8, stride=PITCH), :] = jac[8:16]
                jacs[h][pl.ds(16 * PITCH + t, 2, stride=PITCH), :] = jac[16:18]
                jacs[h][pl.ds(18 * PITCH + t, 6, stride=PITCH), :] = point_jac[:, lane].astype(jnp.float32)
        sources = [steps[PITCH * m : PITCH * m + 8, :] for m in range(9)]
        for h in range(2):
            at = pl.ds(row + h, TILES, stride=2)
            index = obs_cam[at, :]
            moves = [lane_take(source, index) for source in sources]
            jac = [jacs[h][PITCH * m : PITCH * m + 8, :] for m in range(24)]
            first = sum((jac[m] * moves[m] for m in range(1, 9)), jac[0] * moves[0])
            second = sum((jac[9 + m] * moves[m] for m in range(1, 9)), jac[9] * moves[0])
            side = sides[h]
            for n in range(3):
                value = jac[18 + n] * first + jac[21 + n] * second
                head = value.astype(jnp.bfloat16).astype(jnp.float32)
                side[PITCH * n : PITCH * n + 8, :] = head
                side[PITCH * (n + 4) : PITCH * (n + 4) + 8, :] = value - head
            point = obs_point[at, :]
            side[PITCH * 8 : PITCH * 8 + 8, :] = (point & (FINE - 1)).astype(jnp.float32)
            side[PITCH * 9 : PITCH * 9 + 8, :] = (point >> FINE_BITS).astype(jnp.float32)
        for t in range(TILES):
            heads, hots = [], []
            for h in range(2):
                value = sides[h][pl.ds(t, 8, stride=PITCH), :]
                value = jnp.concatenate([value, value], axis=0).astype(jnp.bfloat16)
                low = twice(sides[h][pl.ds(8 * PITCH + t, 1), :])
                high = twice(sides[h][pl.ds(9 * PITCH + t, 1), :])
                heads.append(jnp.concatenate([jnp.where(k == high, value, zero) for k in coarse], axis=0))
                hots.append(jnp.concatenate([jnp.where(k == low, one, zero) for k in fine], axis=0))
            summed = lax.dot_general(
                jnp.concatenate(heads, axis=1),
                jnp.concatenate(hots, axis=1),
                (((1,), (1,)), ((), ())),
                preferred_element_type=jnp.float32,
            )
            place = pl.ds(pl.multiple_of(tile_points[tile + t] * COARSE_ROWS, COARSE_ROWS), COARSE_ROWS)
            total[place, :] = total[place, :] + summed

    def turn(i, carry):
        for u in range(PAIRS):
            group(i * PAIRS + u, *buffers[u])
        return carry

    lax.fori_loop(0, obs_cam.shape[0] // (2 * TILES * PAIRS), turn, 0)

    @pl.when(step == pl.num_programs(0) - 1)
    def _():
        top = lax.broadcasted_iota(jnp.int32, (8, LANES), 0) < 4

        def fold(i, carry):
            for u in range(8):
                k = i * 8 + u
                base = pl.multiple_of(k * COARSE_ROWS, COARSE_ROWS)
                parts = [total[pl.ds(base + 8 * j, 8), :] for j in range(4)]
                pair = [jnp.concatenate(parts[2 * j : 2 * j + 2], axis=1) for j in range(2)]
                pair = [value + pltpu.roll(value, 4, 0) for value in pair]
                packed[pl.ds(pl.multiple_of(k * 8, 8), 8), :] = jnp.where(top, *pair)
            return carry

        lax.fori_loop(0, blocks // 8, fold, 0)
        for n in range(3):
            out[n] = packed[pl.ds(n, out.shape[1], stride=4), :]


def project_kernel(
    tile_block, tile_points, obs_cam, obs_point, observed, cam_table, trial, residual, cost, point_table, *scratch
):
    step = pl.program_id(0)
    tiles_per_step = obs_cam.shape[0] // 2

    @pl.when(step == 0)
    def _():
        cost[...] = jnp.zeros_like(cost)
        for n in range(3):
            point_table[pl.ds(n, trial.shape[1], stride=4), :] = trial[n]
            point_table[pl.ds(3, trial.shape[1], stride=4), :] = jnp.zeros_like(trial[n])

    def group(block, buf):
        row = pl.multiple_of(block * 2 * TILES, 2 * TILES)
        tile = step * tiles_per_step + block * TILES
        for t in range(TILES):
            slab = cam_table.at[tile_block[tile + t]]
            buf[pl.ds(t, 8, stride=PITCH), :] = slab[0:8, :]
            buf[pl.ds(8 * PITCH + t, 2, stride=PITCH), :] = slab[8:10, :]
            place = pl.ds(pl.multiple_of(tile_points[tile + t] * 8, 8), 8)
            buf[pl.ds(10 * PITCH + t, 8, stride=PITCH), :] = point_table[place, :]
        sources = [buf[PITCH * m : PITCH * m + 8, :] for m in range(18)]
        total = None
        for h in range(2):
            at = pl.ds(row + h, TILES, stride=2)
            index = obs_cam[at, :]
            head, a, b, c, *shift, focal, k1, k2 = (lane_take(sources[m], index) for m in range(10))
            point = obs_point[at, :]
            local = point & (LANES - 1)
            upper = point >= LANES
            x, y, z = (
                jnp.where(upper, lane_take(sources[14 + n], local), lane_take(sources[10 + n], local))
                for n in range(3)
            )
            e, f, g = b * z - c * y, c * x - a * z, a * y - b * x
            px = x + shift[0] + (head * e + (b * g - c * f))
            py = y + shift[1] + (head * f + (c * e - a * g))
            pz = z + shift[2] + (head * g + (a * f - b * e))
            scale = 1.0 / jnp.maximum(-pz, 1.0)
            u, v = px * scale, py * scale
            q = u * u + v * v
            factor = focal * (1.0 + q * (k1 + k2 * q))
            at_u = pl.ds(2 * (row + h), TILES, stride=4)
            at_v = pl.ds(2 * (row + h) + 1, TILES, stride=4)
            ru = factor * u - observed[at_u, :]
            rv = factor * v - observed[at_v, :]
            residual[at_u, :] = ru
            residual[at_v, :] = rv
            square = ru * ru + rv * rv
            total = square if total is None else total + square
        return total

    def turn(i, carry):
        for u in range(SPREAD):
            carry = carry + group(i * SPREAD + u, scratch[u])
        return carry

    cost[...] += lax.fori_loop(
        0, obs_cam.shape[0] // (2 * TILES * SPREAD), turn, jnp.zeros((8, LANES), jnp.float32)
    )


def camera_rows(trial):
    w = trial[0:3]
    angle = jnp.sqrt(jnp.sum(w * w, axis=0, keepdims=True))
    head = math.sqrt(2.0) * jnp.cos(0.5 * angle)
    tail = math.sqrt(0.5) * jnp.sinc(angle / (2.0 * math.pi)) * w
    return jnp.concatenate([head, tail, trial[3:9]], axis=0)


def greet(axis, size, me):
    barrier = pltpu.get_barrier_semaphore()
    for d in range(1, size):
        pl.semaphore_signal(
            barrier, inc=1, device_id={axis: lax.rem(me + d, size)}, device_id_type=MESH
        )


def send_round(axis, size, me, source, target, send, recv):
    copies = []
    for d in range(1, size):
        peer = lax.rem(me + d, size)
        copies.append(
            pltpu.make_async_remote_copy(
                src_ref=source(peer, d),
                dst_ref=target(peer, d),
                send_sem=send.at[d - 1],
                recv_sem=recv.at[d - 1],
                device_id={axis: peer},
                device_id_type=MESH,
            )
        )
    for copy in copies:
        copy.start()
    return copies


def gather_kernel(n_pts, n_cam, own, out, local_sem, send_cam, recv_cam, send_pts, recv_pts):
    p, c = lax.axis_index("pts"), lax.axis_index("cam")
    greet("pts", n_pts, p)
    greet("cam", n_cam, c)
    pl.semaphore_wait(pltpu.get_barrier_semaphore(), n_pts + n_cam - 2)
    count = own.shape[0]
    mine = out.at[pl.ds((p * n_cam + c) * count, count)]
    local = pltpu.make_async_copy(own, mine, local_sem)
    local.start()
    copies = send_round("cam", n_cam, c, lambda *_: own, lambda *_: mine, send_cam, recv_cam)
    local.wait()
    for copy in copies:
        copy.wait()
    slab = out.at[pl.ds(p * n_cam * count, n_cam * count)]
    for copy in send_round("pts", n_pts, p, lambda *_: slab, lambda *_: slab, send_pts, recv_pts):
        copy.wait()


def solve_kernel(
    n_cam, planes, points, gradient, inverse, out,
    landed, own_points, own_gradient, own_inverse, work, in_sem, send_sum, recv_sum, send_out, recv_out,
):
    c = lax.axis_index("cam")
    last = n_cam - 1
    chunks = landed.shape[1]
    rows = planes.shape[1] // 2
    count = rows // chunks
    span, pitch = rows * LANES, rows + 1
    low_end, high_end = c == 0, c == last
    at_end = jnp.logical_or(low_end, high_end)
    own_base = jnp.where(low_end, 0, rows)
    loads = [
        pltpu.make_async_copy(
            source.at[:, pl.ds(pl.multiple_of(own_base * LANES, LANES), span)], target, in_sem.at[i]
        )
        for i, (source, target) in enumerate(
            ((points, own_points), (gradient, own_gradient), (inverse, own_inverse))
        )
    ]

    @pl.when(at_end)
    def _():
        for load in loads:
            load.start()

    barrier = pltpu.get_barrier_semaphore()

    def peer(step):
        return lax.rem(c + step + n_cam, n_cam)

    @pl.when(c > 0)
    def _():
        pl.semaphore_signal(barrier, inc=1, device_id={"cam": peer(-1)}, device_id_type=MESH)

    @pl.when(c < last)
    def _():
        pl.semaphore_signal(barrier, inc=1, device_id={"cam": peer(1)}, device_id_type=MESH)

    pl.semaphore_wait(barrier, jnp.where(at_end, 1, 2))

    def place(way, k):
        base = rows if way == 0 else 0
        return pl.ds(pl.multiple_of(base + k * count, 8), count)

    def toward(way):
        return peer(1) if way == 0 else peer(-1)

    def sum_copy(way, k, source):
        return pltpu.make_async_remote_copy(
            src_ref=source,
            dst_ref=landed.at[way, k],
            send_sem=send_sum.at[way, k],
            recv_sem=recv_sum.at[way, k],
            device_id={"cam": toward(way)},
            device_id_type=MESH,
        )

    def out_copy(way, k):
        part = out.at[:, place(way, k)]
        return pltpu.make_async_remote_copy(
            src_ref=part,
            dst_ref=part,
            send_sem=send_out.at[way, k],
            recv_sem=recv_out.at[way, k],
            device_id={"cam": toward(1 - way)},
            device_id_type=MESH,
        )

    for way, first in ((0, low_end), (1, high_end)):

        @pl.when(first)
        def _(way=way):
            def begin(k, carry):
                sum_copy(way, k, planes.at[:, place(way, k)]).start()
                return carry

            lax.fori_loop(0, chunks, begin, 0)

    @pl.when(at_end)
    def _():
        for load in loads:
            load.wait()

        def spread(i, carry):
            for u in range(8):
                k = i * 8 + u
                lanes = pl.ds(pl.multiple_of(k * LANES, LANES), LANES)
                work[pl.ds(k, 3, stride=pitch), :] = own_points[:, lanes]
                work[pl.ds(3 * pitch + k, 3, stride=pitch), :] = own_gradient[:, lanes]
                block = own_inverse[:, lanes]
                work[pl.ds(6 * pitch + k, 8, stride=pitch), :] = block[0:8]
                work[pl.ds(14 * pitch + k, 1), :] = block[8:9]
            return carry

        lax.fori_loop(0, rows // 8, spread, 0)

    def solved(way, k):
        def row(m):
            return work[pl.ds(m * pitch + k * count, count), :]

        total = landed[way, k] + planes[:, place(way, k), :]
        residue = [row(3 + n) - total[n] for n in range(3)]
        for n in range(3):
            move = row(6 + 3 * n) * residue[0] + row(7 + 3 * n) * residue[1] + row(8 + 3 * n) * residue[2]
            out[n, place(way, k), :] = row(n) + move

    def turn(s, carry):
        for way, hops in ((0, c), (1, last - c)):
            k = s - LAG * hops
            live = jnp.logical_and(hops > 0, jnp.logical_and(k >= 0, k < chunks))

            @pl.when(live)
            def _(way=way, k=k, hops=hops):
                sum_copy(way, k, landed.at[way, k]).wait_recv()

                @pl.when(hops < last)
                def _():
                    landed[way, k] = landed[way, k] + planes[:, place(way, k), :]
                    sum_copy(way, k, landed.at[way, k]).start()

                @pl.when(hops == last)
                def _():
                    solved(way, k)
                    out_copy(way, k).start()

        for way, hops in ((0, last - c), (1, c)):
            k = s - LAG * (last + hops)
            live = jnp.logical_and(hops > 0, jnp.logical_and(k >= 0, k < chunks))

            @pl.when(live)
            def _(way=way, k=k, hops=hops):
                out_copy(way, k).wait_recv()

                @pl.when(hops < last)
                def _():
                    out_copy(way, k).start()

        return carry

    lax.fori_loop(0, chunks + 2 * LAG * last, turn, 0)

    def finish(k, carry):
        for way, first, end in ((0, low_end, high_end), (1, high_end, low_end)):

            @pl.when(jnp.logical_not(end))
            def _(way=way):
                sum_copy(way, k, landed.at[way, k]).wait_send()

            @pl.when(jnp.logical_not(first))
            def _(way=way):
                out_copy(way, k).wait_send()

        return carry

    lax.fori_loop(0, chunks, finish, 0)


def total_kernel(n_pts, n_cam, own, out, cam_slots, pts_slots, send_cam, recv_cam, send_pts, recv_pts):
    p, c = lax.axis_index("pts"), lax.axis_index("cam")
    greet("pts", n_pts, p)
    greet("cam", n_cam, c)
    cam_slots[c] = own[...]
    pl.semaphore_wait(pltpu.get_barrier_semaphore(), n_pts + n_cam - 2)
    slot = cam_slots.at[c]
    for copy in send_round("cam", n_cam, c, lambda *_: own, lambda *_: slot, send_cam, recv_cam):
        copy.wait()
    value = cam_slots[0]
    for i in range(1, n_cam):
        value = value + cam_slots[i]
    pts_slots[p] = value
    slot = pts_slots.at[p]
    for copy in send_round("pts", n_pts, p, lambda *_: slot, lambda *_: slot, send_pts, recv_pts):
        copy.wait()
    value = pts_slots[0]
    for i in range(1, n_pts):
        value = value + pts_slots[i]
    out[...] = value


def on_device(
    cameras, increment, points, point_gradient, point_inverse, cam_jacobian, point_jacobian,
    observed, tile_block, tile_points, obs_camera, obs_point, accept,
):
    own_blocks = cameras.shape[1] // CB
    own = jnp.concatenate(
        [increment, camera_rows(cameras + increment), jnp.zeros((5, cameras.shape[1]), jnp.float32)], axis=0
    )
    own = own.reshape(24, own_blocks, CB).transpose(1, 0, 2)
    n_pts, n_cam = lax.axis_size("pts"), lax.axis_size("cam")
    vmem = pl.BlockSpec(memory_space=pltpu.VMEM)

    def dma_sems(*counts):
        return [pltpu.SemaphoreType.DMA((count,)) for count in counts]

    def remote(ident):
        return pltpu.CompilerParams(
            collective_id=ident, has_side_effects=True, vmem_limit_bytes=50 * 2**20
        )

    every = pl.pallas_call(
        functools.partial(gather_kernel, n_pts, n_cam),
        in_specs=[vmem],
        out_specs=vmem,
        out_shape=jax.ShapeDtypeStruct((own_blocks * n_pts * n_cam, 24, CB), jnp.float32),
        scratch_shapes=[pltpu.SemaphoreType.DMA]
        + dma_sems(n_cam - 1, n_cam - 1, n_pts - 1, n_pts - 1),
        compiler_params=remote(0),
        name="cameras",
    )(own)
    cam_blocks = every.shape[0]
    step_table = jnp.concatenate([every[:, 0:9], jnp.zeros((cam_blocks, 7, CB), jnp.float32)], axis=1)
    cam_table = jnp.concatenate([every[:, 9:19], jnp.zeros((cam_blocks, 6, CB), jnp.float32)], axis=1)

    obs_count = obs_camera.shape[0]
    rows = obs_count // LANES
    per = math.gcd(rows, BLOCKS_PER_STEP)
    grid = (rows // per,)
    point_blocks = points.shape[1] // PB
    oc = obs_camera.reshape(rows, LANES)
    op = obs_point.reshape(rows, LANES)

    def whole(*shape):
        return pl.BlockSpec(shape, lambda i, *_: (0,) * len(shape))

    params = pltpu.CompilerParams(dimension_semantics=("arbitrary",), vmem_limit_bytes=50 * 2**20)
    planes = pl.pallas_call(
        couple_kernel,
        grid_spec=pltpu.PrefetchScalarGridSpec(
            num_scalar_prefetch=2,
            grid=grid,
            in_specs=[
                pl.BlockSpec((18, per * LANES), lambda i, *_: (0, i)),
                pl.BlockSpec((6, per * LANES), lambda i, *_: (0, i)),
                pl.BlockSpec((per, LANES), lambda i, *_: (i, 0)),
                pl.BlockSpec((per, LANES), lambda i, *_: (i, 0)),
                whole(cam_blocks, 16, CB),
            ],
            out_specs=whole(3, 2 * point_blocks, LANES),
            scratch_shapes=[
                pltpu.VMEM((point_blocks * COARSE_ROWS, FINE), jnp.float32),
                pltpu.VMEM((point_blocks * 8, LANES), jnp.float32),
            ]
            + [
                pltpu.VMEM((count * PITCH, LANES), jnp.float32) for count in (9, 24, 24, 10, 10)
            ]
            * PAIRS,
        ),
        out_shape=jax.ShapeDtypeStruct((3, 2 * point_blocks, LANES), jnp.float32),
        compiler_params=params,
        name="couple",
    )(tile_block, tile_points, cam_jacobian, point_jacobian, oc, op, step_table)

    own_rows = point_blocks
    chunks = math.gcd(own_rows // 8, CHUNKS)
    hbm = pl.BlockSpec(memory_space=pl.ANY)
    trial = pl.pallas_call(
        functools.partial(solve_kernel, n_cam),
        in_specs=[vmem, hbm, hbm, hbm],
        out_specs=vmem,
        out_shape=jax.ShapeDtypeStruct(planes.shape, jnp.float32),
        scratch_shapes=[
            pltpu.VMEM((2, chunks, 3, own_rows // chunks, LANES), jnp.float32),
            pltpu.VMEM((3, own_rows * LANES), jnp.float32),
            pltpu.VMEM((3, own_rows * LANES), jnp.float32),
            pltpu.VMEM((9, own_rows * LANES), jnp.float32),
            pltpu.VMEM((15 * (own_rows + 1), LANES), jnp.float32),
            pltpu.SemaphoreType.DMA((3,)),
        ]
        + [pltpu.SemaphoreType.DMA((2, chunks))] * 4,
        compiler_params=remote(1),
        name="solve",
    )(planes, points, point_gradient, point_inverse)

    seen = observed.reshape(2, rows, LANES).transpose(1, 0, 2).reshape(2 * rows, LANES)
    residual, partial = pl.pallas_call(
        project_kernel,
        grid_spec=pltpu.PrefetchScalarGridSpec(
            num_scalar_prefetch=2,
            grid=grid,
            in_specs=[
                pl.BlockSpec((per, LANES), lambda i, *_: (i, 0)),
                pl.BlockSpec((per, LANES), lambda i, *_: (i, 0)),
                pl.BlockSpec((2 * per, LANES), lambda i, *_: (i, 0)),
                whole(cam_blocks, 16, CB),
                whole(3, 2 * point_blocks, LANES),
            ],
            out_specs=[
                pl.BlockSpec((2 * per, LANES), lambda i, *_: (i, 0)),
                whole(8, LANES),
            ],
            scratch_shapes=[pltpu.VMEM((point_blocks * 8, LANES), jnp.float32)]
            + [pltpu.VMEM((18 * PITCH, LANES), jnp.float32)] * SPREAD,
        ),
        out_shape=[
            jax.ShapeDtypeStruct((2 * rows, LANES), jnp.float32),
            jax.ShapeDtypeStruct((8, LANES), jnp.float32),
        ],
        compiler_params=params,
        name="project",
    )(tile_block, tile_points, oc, op, seen, cam_table, trial)
    residual = residual.reshape(rows, 2, LANES).transpose(1, 0, 2).reshape(2, obs_count)
    sums = pl.pallas_call(
        functools.partial(total_kernel, n_pts, n_cam),
        in_specs=[vmem],
        out_specs=vmem,
        out_shape=jax.ShapeDtypeStruct((8, LANES), jnp.float32),
        scratch_shapes=[
            pltpu.VMEM((n_cam, 8, LANES), jnp.float32),
            pltpu.VMEM((n_pts, 8, LANES), jnp.float32),
        ]
        + dma_sems(n_cam - 1, n_cam - 1, n_pts - 1, n_pts - 1),
        compiler_params=remote(2),
        name="total",
    )(partial)
    trial_cost = jnp.sum(sums) / (2.0 * obs_count * n_pts * n_cam)
    odd = jnp.remainder(accept, 2)
    accepted_points = jnp.where(odd == 1, trial.reshape(3, -1), points)
    return residual, trial_cost, accepted_points, cameras + odd.astype(jnp.float32) * increment


def solution(mesh):
    in_specs = (
        P(None, ("pts", "cam")),
        P(None, ("pts", "cam")),
        P(None, "pts"),
        P(None, "pts"),
        P(None, "pts"),
        P(None, ("pts", "cam")),
        P(None, ("pts", "cam")),
        P(None, ("pts", "cam")),
        P(("pts", "cam")),
        P(("pts", "cam")),
        P(("pts", "cam")),
        P(("pts", "cam")),
        P(),
    )
    out_specs = (P(None, ("pts", "cam")), P(), P(None, "pts"), P(None, ("pts", "cam")))
    return jax.shard_map(
        on_device, mesh=mesh, in_specs=in_specs, out_specs=out_specs, check_vma=False
    )
```

```python
import functools
import math

import jax
import jax.numpy as jnp
from jax import lax
from jax.experimental import pallas as pl
from jax.experimental.pallas import tpu as pltpu
from jax.sharding import PartitionSpec as P

CB = 128
PB = 256
TILE = 256
LANES = 128
PITCH = 9
FINE = 64
FINE_BITS = 6
COARSE_ROWS = 32
PAIRS = 8
TILES = 8
SPREAD = 8
CHUNKS = 16
LAG = 5
BLOCKS_PER_STEP = 256
MESH = pl.DeviceIdType.MESH


LANE_GATHER = lax.GatherDimensionNumbers(
    offset_dims=(),
    collapsed_slice_dims=(1,),
    start_index_map=(1,),
    operand_batching_dims=(0,),
    start_indices_batching_dims=(0,),
)


def lane_take(slab, index):
    return lax.gather(
        slab, index[:, :, None], LANE_GATHER, (1, 1), mode=lax.GatherScatterMode.PROMISE_IN_BOUNDS
    )


def couple_kernel(
    tile_block, tile_points, cam_jac, point_jac, obs_cam, obs_point, table, out, total, packed, *scratch
):
    step = pl.program_id(0)
    tiles_per_step = obs_cam.shape[0] // 2
    buffers = [scratch[5 * u : 5 * u + 5] for u in range(PAIRS)]
    blocks = packed.shape[0] // 8

    @pl.when(step == 0)
    def _():
        total[...] = jnp.zeros_like(total)
        for _, _, _, low, high in buffers:
            low[...] = jnp.zeros_like(low)
            high[...] = jnp.zeros_like(high)

    wide = lax.broadcasted_iota(jnp.int32, (16, LANES), 0)
    fine = [(wide + 16 * k).astype(jnp.float32).astype(jnp.bfloat16) for k in range(FINE // 16)]
    half = (wide >= 8).astype(jnp.float32)
    coarse = [(half + 2.0 * k).astype(jnp.bfloat16) for k in range(PB // FINE // 2)]
    one = jnp.ones((16, LANES), jnp.bfloat16)
    zero = jnp.zeros((16, LANES), jnp.bfloat16)

    def twice(row):
        return jnp.broadcast_to(row, (16, LANES)).astype(jnp.bfloat16)

    def group(block, steps, *halves):
        jacs, sides = halves[:2], halves[2:]
        row = pl.multiple_of(block * 2 * TILES, 2 * TILES)
        tile = step * tiles_per_step + block * TILES
        for t in range(TILES):
            slab = table.at[tile_block[tile + t]]
            steps[pl.ds(t, 8, stride=PITCH), :] = slab[0:8, :]
            steps[pl.ds(8 * PITCH + t, 1), :] = slab[8:9, :]
            for h in range(2):
                lane = pl.ds(pl.multiple_of((row + 2 * t + h) * LANES, LANES), LANES)
                jac = cam_jac[:, lane].astype(jnp.float32)
                jacs[h][pl.ds(t, 8, stride=PITCH), :] = jac[0:8]
                jacs[h][pl.ds(8 * PITCH + t, 8, stride=PITCH), :] = jac[8:16]
                jacs[h][pl.ds(16 * PITCH + t, 2, stride=PITCH), :] = jac[16:18]
                jacs[h][pl.ds(18 * PITCH + t, 6, stride=PITCH), :] = point_jac[:, lane].astype(jnp.float32)
        sources = [steps[PITCH * m : PITCH * m + 8, :] for m in range(9)]
        for h in range(2):
            at = pl.ds(row + h, TILES, stride=2)
            index = obs_cam[at, :]
            moves = [lane_take(source, index) for source in sources]
            jac = [jacs[h][PITCH * m : PITCH * m + 8, :] for m in range(24)]
            first = sum((jac[m] * moves[m] for m in range(1, 9)), jac[0] * moves[0])
            second = sum((jac[9 + m] * moves[m] for m in range(1, 9)), jac[9] * moves[0])
            side = sides[h]
            for n in range(3):
                value = jac[18 + n] * first + jac[21 + n] * second
                head = value.astype(jnp.bfloat16).astype(jnp.float32)
                side[PITCH * n : PITCH * n + 8, :] = head
                side[PITCH * (n + 4) : PITCH * (n + 4) + 8, :] = value - head
            point = obs_point[at, :]
            side[PITCH * 8 : PITCH * 8 + 8, :] = (point & (FINE - 1)).astype(jnp.float32)
            side[PITCH * 9 : PITCH * 9 + 8, :] = (point >> FINE_BITS).astype(jnp.float32)
        for t in range(TILES):
            heads, hots = [], []
            for h in range(2):
                value = sides[h][pl.ds(t, 8, stride=PITCH), :]
                value = jnp.concatenate([value, value], axis=0).astype(jnp.bfloat16)
                low = twice(sides[h][pl.ds(8 * PITCH + t, 1), :])
                high = twice(sides[h][pl.ds(9 * PITCH + t, 1), :])
                heads.append(jnp.concatenate([jnp.where(k == high, value, zero) for k in coarse], axis=0))
                hots.append(jnp.concatenate([jnp.where(k == low, one, zero) for k in fine], axis=0))
            summed = lax.dot_general(
                jnp.concatenate(heads, axis=1),
                jnp.concatenate(hots, axis=1),
                (((1,), (1,)), ((), ())),
                preferred_element_type=jnp.float32,
            )
            place = pl.ds(pl.multiple_of(tile_points[tile + t] * COARSE_ROWS, COARSE_ROWS), COARSE_ROWS)
            total[place, :] = total[place, :] + summed

    def turn(i, carry):
        for u in range(PAIRS):
            group(i * PAIRS + u, *buffers[u])
        return carry

    lax.fori_loop(0, obs_cam.shape[0] // (2 * TILES * PAIRS), turn, 0)

    @pl.when(step == pl.num_programs(0) - 1)
    def _():
        top = lax.broadcasted_iota(jnp.int32, (8, LANES), 0) < 4

        def fold(i, carry):
            for u in range(8):
                k = i * 8 + u
                base = pl.multiple_of(k * COARSE_ROWS, COARSE_ROWS)
                parts = [total[pl.ds(base + 8 * j, 8), :] for j in range(4)]
                pair = [jnp.concatenate(parts[2 * j : 2 * j + 2], axis=1) for j in range(2)]
                pair = [value + pltpu.roll(value, 4, 0) for value in pair]
                packed[pl.ds(pl.multiple_of(k * 8, 8), 8), :] = jnp.where(top, *pair)
            return carry

        lax.fori_loop(0, blocks // 8, fold, 0)
        for n in range(3):
            out[n] = packed[pl.ds(n, out.shape[1], stride=4), :]


def camera_rows(trial):
    w = trial[0:3]
    angle = jnp.sqrt(jnp.sum(w * w, axis=0, keepdims=True))
    head = math.sqrt(2.0) * jnp.cos(0.5 * angle)
    tail = math.sqrt(0.5) * jnp.sinc(angle / (2.0 * math.pi)) * w
    return jnp.concatenate([head, tail, trial[3:9]], axis=0)


def greet(axis, size, me):
    barrier = pltpu.get_barrier_semaphore()
    for d in range(1, size):
        pl.semaphore_signal(
            barrier, inc=1, device_id={axis: lax.rem(me + d, size)}, device_id_type=MESH
        )


def send_round(axis, size, me, source, target, send, recv):
    copies = []
    for d in range(1, size):
        peer = lax.rem(me + d, size)
        copies.append(
            pltpu.make_async_remote_copy(
                src_ref=source(peer, d),
                dst_ref=target(peer, d),
                send_sem=send.at[d - 1],
                recv_sem=recv.at[d - 1],
                device_id={axis: peer},
                device_id_type=MESH,
            )
        )
    for copy in copies:
        copy.start()
    return copies


def gather_kernel(n_pts, n_cam, own, out, local_sem, send_cam, recv_cam, send_pts, recv_pts):
    p, c = lax.axis_index("pts"), lax.axis_index("cam")
    greet("pts", n_pts, p)
    greet("cam", n_cam, c)
    pl.semaphore_wait(pltpu.get_barrier_semaphore(), n_pts + n_cam - 2)
    count = own.shape[0]
    mine = out.at[pl.ds((p * n_cam + c) * count, count)]
    local = pltpu.make_async_copy(own, mine, local_sem)
    local.start()
    copies = send_round("cam", n_cam, c, lambda *_: own, lambda *_: mine, send_cam, recv_cam)
    local.wait()
    for copy in copies:
        copy.wait()
    slab = out.at[pl.ds(p * n_cam * count, n_cam * count)]
    for copy in send_round("pts", n_pts, p, lambda *_: slab, lambda *_: slab, send_pts, recv_pts):
        copy.wait()


def finish_kernel(
    n_pts, n_cam, tile_block, tile_points, planes, cam_table, points, gradient, inverse, hbm_cam, hbm_point,
    hbm_seen, residual, out, sums, landed, own_points, own_gradient, own_inverse, work, obs_cam, obs_point,
    observed, cam_store, point_table, partial, cam_slots, pts_slots, in_sem, send_sum, recv_sum, send_out,
    recv_out, send_cam, recv_cam, send_pts, recv_pts, *buffers,
):
    p, c = lax.axis_index("pts"), lax.axis_index("cam")
    streams = [
        pltpu.make_async_copy(source, target, in_sem.at[3 + i])
        for i, (source, target) in enumerate(
            ((hbm_cam, obs_cam), (hbm_point, obs_point), (hbm_seen, observed))
        )
    ]
    for stream in streams:
        stream.start()
    last = n_cam - 1
    chunks = landed.shape[1]
    rows = planes.shape[1] // 2
    count = rows // chunks
    span, pitch = rows * LANES, rows + 1
    low_end, high_end = c == 0, c == last
    at_end = jnp.logical_or(low_end, high_end)
    own_base = jnp.where(low_end, 0, rows)
    loads = [
        pltpu.make_async_copy(
            source.at[:, pl.ds(pl.multiple_of(own_base * LANES, LANES), span)], target, in_sem.at[i]
        )
        for i, (source, target) in enumerate(
            ((points, own_points), (gradient, own_gradient), (inverse, own_inverse))
        )
    ]

    @pl.when(at_end)
    def _():
        for load in loads:
            load.start()

    greet("pts", n_pts, p)
    greet("cam", n_cam, c)

    def take_cameras(i, carry):
        for u in range(SPREAD):
            block = i * SPREAD + u
            row = pl.multiple_of(block * 2 * TILES, 2 * TILES)
            buf = buffers[u]
            for t in range(TILES):
                slab = cam_table[tile_block[block * TILES + t]]
                buf[pl.ds(t, 8, stride=PITCH), :] = slab[0:8]
                buf[pl.ds(8 * PITCH + t, 2, stride=PITCH), :] = slab[8:10]
            sources = [buf[PITCH * m : PITCH * m + 8, :] for m in range(10)]
            for h in range(2):
                index = obs_cam[pl.ds(row + h, TILES, stride=2), :]
                for m in range(10):
                    cam_store[m, pl.ds(row + TILES * h, TILES), :] = lane_take(sources[m], index)
        return carry

    turns = obs_cam.shape[0] // (2 * TILES * SPREAD)
    early = turns // 4
    streams[0].wait()
    lax.fori_loop(0, early, take_cameras, 0)
    pl.semaphore_wait(pltpu.get_barrier_semaphore(), n_pts + n_cam - 2)

    def peer(step):
        return lax.rem(c + step + n_cam, n_cam)

    def place(way, k):
        base = rows if way == 0 else 0
        return pl.ds(pl.multiple_of(base + k * count, 8), count)

    def toward(way):
        return peer(1) if way == 0 else peer(-1)

    def sum_copy(way, k, source):
        return pltpu.make_async_remote_copy(
            src_ref=source,
            dst_ref=landed.at[way, k],
            send_sem=send_sum.at[way, k],
            recv_sem=recv_sum.at[way, k],
            device_id={"cam": toward(way)},
            device_id_type=MESH,
        )

    def out_copy(way, k):
        part = out.at[:, place(way, k)]
        return pltpu.make_async_remote_copy(
            src_ref=part,
            dst_ref=part,
            send_sem=send_out.at[way, k],
            recv_sem=recv_out.at[way, k],
            device_id={"cam": toward(1 - way)},
            device_id_type=MESH,
        )

    for way, first in ((0, low_end), (1, high_end)):

        @pl.when(first)
        def _(way=way):
            def begin(k, carry):
                sum_copy(way, k, planes.at[:, place(way, k)]).start()
                return carry

            lax.fori_loop(0, chunks, begin, 0)

    lax.fori_loop(early, turns, take_cameras, 0)

    @pl.when(at_end)
    def _():
        for load in loads:
            load.wait()

        def spread(i, carry):
            for u in range(8):
                k = i * 8 + u
                lanes = pl.ds(pl.multiple_of(k * LANES, LANES), LANES)
                work[pl.ds(k, 3, stride=pitch), :] = own_points[:, lanes]
                work[pl.ds(3 * pitch + k, 3, stride=pitch), :] = own_gradient[:, lanes]
                block = own_inverse[:, lanes]
                work[pl.ds(6 * pitch + k, 8, stride=pitch), :] = block[0:8]
                work[pl.ds(14 * pitch + k, 1), :] = block[8:9]
            return carry

        lax.fori_loop(0, rows // 8, spread, 0)

    def solved(way, k):
        def row(m):
            return work[pl.ds(m * pitch + k * count, count), :]

        total = landed[way, k] + planes[:, place(way, k), :]
        residue = [row(3 + n) - total[n] for n in range(3)]
        for n in range(3):
            move = row(6 + 3 * n) * residue[0] + row(7 + 3 * n) * residue[1] + row(8 + 3 * n) * residue[2]
            out[n, place(way, k), :] = row(n) + move

    def turn(s, carry):
        for way, hops in ((0, c), (1, last - c)):
            k = s - LAG * hops
            live = jnp.logical_and(hops > 0, jnp.logical_and(k >= 0, k < chunks))

            @pl.when(live)
            def _(way=way, k=k, hops=hops):
                sum_copy(way, k, landed.at[way, k]).wait_recv()

                @pl.when(hops < last)
                def _():
                    landed[way, k] = landed[way, k] + planes[:, place(way, k), :]
                    sum_copy(way, k, landed.at[way, k]).start()

                @pl.when(hops == last)
                def _():
                    solved(way, k)
                    out_copy(way, k).start()

        for way, hops in ((0, last - c), (1, c)):
            k = s - LAG * (last + hops)
            live = jnp.logical_and(hops > 0, jnp.logical_and(k >= 0, k < chunks))

            @pl.when(live)
            def _(way=way, k=k, hops=hops):
                out_copy(way, k).wait_recv()

                @pl.when(hops < last)
                def _():
                    out_copy(way, k).start()

        return carry

    lax.fori_loop(0, chunks + 2 * LAG * last, turn, 0)

    def finish(k, carry):
        for way, first, end in ((0, low_end, high_end), (1, high_end, low_end)):

            @pl.when(jnp.logical_not(end))
            def _(way=way):
                sum_copy(way, k, landed.at[way, k]).wait_send()

            @pl.when(jnp.logical_not(first))
            def _(way=way):
                out_copy(way, k).wait_send()

        return carry

    lax.fori_loop(0, chunks, finish, 0)
    for n in range(3):
        point_table[pl.ds(n, out.shape[1], stride=4), :] = out[n]
    point_table[pl.ds(3, out.shape[1], stride=4), :] = jnp.zeros_like(out[0])
    point_slabs = point_table.reshape(point_table.shape[0] // 8, 8, LANES)
    for stream in streams[1:]:
        stream.wait()

    def project(i, carry):
        for u in range(SPREAD):
            block = i * SPREAD + u
            row = pl.multiple_of(block * 2 * TILES, 2 * TILES)
            buf = buffers[u]
            for t in range(TILES):
                buf[pl.ds(t, 8, stride=PITCH), :] = point_slabs[tile_points[block * TILES + t]]
            sources = [buf[PITCH * m : PITCH * m + 8, :] for m in range(8)]
            for h in range(2):
                point = obs_point[pl.ds(row + h, TILES, stride=2), :]
                local = point & (LANES - 1)
                upper = point >= LANES
                x, y, z = (
                    jnp.where(upper, lane_take(sources[4 + n], local), lane_take(sources[n], local))
                    for n in range(3)
                )
                head, a, b, c, *shift, focal, k1, k2 = (
                    cam_store[m, pl.ds(row + TILES * h, TILES), :] for m in range(10)
                )
                e, f, g = b * z - c * y, c * x - a * z, a * y - b * x
                px = x + shift[0] + (head * e + (b * g - c * f))
                py = y + shift[1] + (head * f + (c * e - a * g))
                pz = z + shift[2] + (head * g + (a * f - b * e))
                scale = 1.0 / jnp.maximum(-pz, 1.0)
                fu, fv = px * scale, py * scale
                q = fu * fu + fv * fv
                factor = focal * (1.0 + q * (k1 + k2 * q))
                at_u = pl.ds(2 * (row + h), TILES, stride=4)
                at_v = pl.ds(2 * (row + h) + 1, TILES, stride=4)
                ru = factor * fu - observed[at_u, :]
                rv = factor * fv - observed[at_v, :]
                residual[at_u, :] = ru
                residual[at_v, :] = rv
                carry = carry + (ru * ru + rv * rv)
        return carry

    partial[...] = lax.fori_loop(0, turns, project, jnp.zeros((8, LANES), jnp.float32))
    slot = cam_slots.at[c]
    exchange = send_round("cam", n_cam, c, lambda *_: partial, lambda *_: slot, send_cam, recv_cam)
    cam_slots[c] = partial[...]
    for copy in exchange:
        copy.wait()
    value = cam_slots[0]
    for i in range(1, n_cam):
        value = value + cam_slots[i]
    pts_slots[p] = value
    slot = pts_slots.at[p]
    for copy in send_round("pts", n_pts, p, lambda *_: slot, lambda *_: slot, send_pts, recv_pts):
        copy.wait()
    value = pts_slots[0]
    for i in range(1, n_pts):
        value = value + pts_slots[i]
    sums[...] = value


def on_device(
    cameras, increment, points, point_gradient, point_inverse, cam_jacobian, point_jacobian,
    observed, tile_block, tile_points, obs_camera, obs_point, accept,
):
    own_blocks = cameras.shape[1] // CB
    own = jnp.concatenate(
        [increment, camera_rows(cameras + increment), jnp.zeros((5, cameras.shape[1]), jnp.float32)], axis=0
    )
    own = own.reshape(24, own_blocks, CB).transpose(1, 0, 2)
    n_pts, n_cam = lax.axis_size("pts"), lax.axis_size("cam")
    vmem = pl.BlockSpec(memory_space=pltpu.VMEM)

    def dma_sems(*counts):
        return [pltpu.SemaphoreType.DMA((count,)) for count in counts]

    def remote(ident):
        return pltpu.CompilerParams(
            collective_id=ident, has_side_effects=True, vmem_limit_bytes=50 * 2**20
        )

    every = pl.pallas_call(
        functools.partial(gather_kernel, n_pts, n_cam),
        in_specs=[vmem],
        out_specs=vmem,
        out_shape=jax.ShapeDtypeStruct((own_blocks * n_pts * n_cam, 24, CB), jnp.float32),
        scratch_shapes=[pltpu.SemaphoreType.DMA]
        + dma_sems(n_cam - 1, n_cam - 1, n_pts - 1, n_pts - 1),
        compiler_params=remote(0),
        name="cameras",
    )(own)
    cam_blocks = every.shape[0]
    step_table = jnp.concatenate([every[:, 0:9], jnp.zeros((cam_blocks, 7, CB), jnp.float32)], axis=1)
    cam_table = jnp.concatenate([every[:, 9:19], jnp.zeros((cam_blocks, 6, CB), jnp.float32)], axis=1)

    obs_count = obs_camera.shape[0]
    rows = obs_count // LANES
    per = math.gcd(rows, BLOCKS_PER_STEP)
    grid = (rows // per,)
    point_blocks = points.shape[1] // PB
    oc = obs_camera.reshape(rows, LANES)
    op = obs_point.reshape(rows, LANES)

    def whole(*shape):
        return pl.BlockSpec(shape, lambda i, *_: (0,) * len(shape))

    params = pltpu.CompilerParams(dimension_semantics=("arbitrary",), vmem_limit_bytes=50 * 2**20)
    planes = pl.pallas_call(
        couple_kernel,
        grid_spec=pltpu.PrefetchScalarGridSpec(
            num_scalar_prefetch=2,
            grid=grid,
            in_specs=[
                pl.BlockSpec((18, per * LANES), lambda i, *_: (0, i)),
                pl.BlockSpec((6, per * LANES), lambda i, *_: (0, i)),
                pl.BlockSpec((per, LANES), lambda i, *_: (i, 0)),
                pl.BlockSpec((per, LANES), lambda i, *_: (i, 0)),
                whole(cam_blocks, 16, CB),
            ],
            out_specs=whole(3, 2 * point_blocks, LANES),
            scratch_shapes=[
                pltpu.VMEM((point_blocks * COARSE_ROWS, FINE), jnp.float32),
                pltpu.VMEM((point_blocks * 8, LANES), jnp.float32),
            ]
            + [
                pltpu.VMEM((count * PITCH, LANES), jnp.float32) for count in (9, 24, 24, 10, 10)
            ]
            * PAIRS,
        ),
        out_shape=jax.ShapeDtypeStruct((3, 2 * point_blocks, LANES), jnp.float32),
        compiler_params=params,
        name="couple",
    )(tile_block, tile_points, cam_jacobian, point_jacobian, oc, op, step_table)

    own_rows = point_blocks
    chunks = math.gcd(own_rows // 8, CHUNKS)
    anywhere = pl.BlockSpec(memory_space=pl.ANY)
    smem = pl.BlockSpec(memory_space=pltpu.SMEM)
    seen = observed.reshape(2, rows, LANES).transpose(1, 0, 2).reshape(2 * rows, LANES)
    residual, trial, sums = pl.pallas_call(
        functools.partial(finish_kernel, n_pts, n_cam),
        in_specs=[smem, smem, vmem, vmem] + [anywhere] * 6,
        out_specs=[vmem, vmem, vmem],
        out_shape=[
            jax.ShapeDtypeStruct((2 * rows, LANES), jnp.float32),
            jax.ShapeDtypeStruct(planes.shape, jnp.float32),
            jax.ShapeDtypeStruct((8, LANES), jnp.float32),
        ],
        scratch_shapes=[
            pltpu.VMEM((2, chunks, 3, own_rows // chunks, LANES), jnp.float32),
            pltpu.VMEM((3, own_rows * LANES), jnp.float32),
            pltpu.VMEM((3, own_rows * LANES), jnp.float32),
            pltpu.VMEM((9, own_rows * LANES), jnp.float32),
            pltpu.VMEM((15 * (own_rows + 1), LANES), jnp.float32),
            pltpu.VMEM((rows, LANES), jnp.int32),
            pltpu.VMEM((rows, LANES), jnp.int32),
            pltpu.VMEM((2 * rows, LANES), jnp.float32),
            pltpu.VMEM((10, rows, LANES), jnp.float32),
            pltpu.VMEM((point_blocks * 8, LANES), jnp.float32),
            pltpu.VMEM((8, LANES), jnp.float32),
            pltpu.VMEM((n_cam, 8, LANES), jnp.float32),
            pltpu.VMEM((n_pts, 8, LANES), jnp.float32),
            pltpu.SemaphoreType.DMA((6,)),
        ]
        + [pltpu.SemaphoreType.DMA((2, chunks))] * 4
        + dma_sems(n_cam - 1, n_cam - 1, n_pts - 1, n_pts - 1)
        + [pltpu.VMEM((10 * PITCH, LANES), jnp.float32)] * SPREAD,
        compiler_params=remote(1),
        name="finish",
    )(
        tile_block, tile_points, planes, cam_table, points, point_gradient,
        point_inverse, oc, op, seen,
    )
    residual = residual.reshape(rows, 2, LANES).transpose(1, 0, 2).reshape(2, obs_count)
    trial_cost = jnp.sum(sums) / (2.0 * obs_count * n_pts * n_cam)
    odd = jnp.remainder(accept, 2)
    accepted_points = jnp.where(odd == 1, trial.reshape(3, -1), points)
    return residual, trial_cost, accepted_points, cameras + odd.astype(jnp.float32) * increment


def solution(mesh):
    in_specs = (
        P(None, ("pts", "cam")),
        P(None, ("pts", "cam")),
        P(None, "pts"),
        P(None, "pts"),
        P(None, "pts"),
        P(None, ("pts", "cam")),
        P(None, ("pts", "cam")),
        P(None, ("pts", "cam")),
        P(("pts", "cam")),
        P(("pts", "cam")),
        P(("pts", "cam")),
        P(("pts", "cam")),
        P(),
    )
    out_specs = (P(None, ("pts", "cam")), P(), P(None, "pts"), P(None, ("pts", "cam")))
    return jax.shard_map(
        on_device, mesh=mesh, in_specs=in_specs, out_specs=out_specs, check_vma=False
    )
```

```python
import functools
import math

import jax
import jax.numpy as jnp
from jax import lax
from jax.experimental import pallas as pl
from jax.experimental.pallas import tpu as pltpu
from jax.sharding import PartitionSpec as P

CB = 128
PB = 256
TILE = 256
LANES = 128
PITCH = 9
FINE = 64
FINE_BITS = 6
COARSE_ROWS = 32
PAIRS = 8
TILES = 8
SPREAD = 8
CHUNKS = 16
LAG = 5
BLOCKS_PER_STEP = 256
MESH = pl.DeviceIdType.MESH


LANE_GATHER = lax.GatherDimensionNumbers(
    offset_dims=(),
    collapsed_slice_dims=(1,),
    start_index_map=(1,),
    operand_batching_dims=(0,),
    start_indices_batching_dims=(0,),
)


def lane_take(slab, index):
    return lax.gather(
        slab, index[:, :, None], LANE_GATHER, (1, 1), mode=lax.GatherScatterMode.PROMISE_IN_BOUNDS
    )


def couple_kernel(
    tile_block, tile_points, cam_jac, point_jac, obs_cam, obs_point, table, out, total, packed, *scratch
):
    step = pl.program_id(0)
    tiles_per_step = obs_cam.shape[0] // 2
    buffers = [scratch[5 * u : 5 * u + 5] for u in range(PAIRS)]
    blocks = packed.shape[0] // 8

    @pl.when(step == 0)
    def _():
        total[...] = jnp.zeros_like(total)
        for _, _, _, low, high in buffers:
            low[...] = jnp.zeros_like(low)
            high[...] = jnp.zeros_like(high)

    wide = lax.broadcasted_iota(jnp.int32, (16, LANES), 0)
    fine = [(wide + 16 * k).astype(jnp.float32).astype(jnp.bfloat16) for k in range(FINE // 16)]
    half = (wide >= 8).astype(jnp.float32)
    coarse = [(half + 2.0 * k).astype(jnp.bfloat16) for k in range(PB // FINE // 2)]
    one = jnp.ones((16, LANES), jnp.bfloat16)
    zero = jnp.zeros((16, LANES), jnp.bfloat16)

    def twice(row):
        return jnp.broadcast_to(row, (16, LANES)).astype(jnp.bfloat16)

    def group(block, steps, *halves):
        jacs, sides = halves[:2], halves[2:]
        row = pl.multiple_of(block * 2 * TILES, 2 * TILES)
        tile = step * tiles_per_step + block * TILES
        for t in range(TILES):
            slab = table.at[tile_block[tile + t]]
            steps[pl.ds(t, 8, stride=PITCH), :] = slab[0:8, :]
            steps[pl.ds(8 * PITCH + t, 1), :] = slab[8:9, :]
            for h in range(2):
                lane = pl.ds(pl.multiple_of((row + 2 * t + h) * LANES, LANES), LANES)
                jac = cam_jac[:, lane].astype(jnp.float32)
                jacs[h][pl.ds(t, 8, stride=PITCH), :] = jac[0:8]
                jacs[h][pl.ds(8 * PITCH + t, 8, stride=PITCH), :] = jac[8:16]
                jacs[h][pl.ds(16 * PITCH + t, 2, stride=PITCH), :] = jac[16:18]
                jacs[h][pl.ds(18 * PITCH + t, 6, stride=PITCH), :] = point_jac[:, lane].astype(jnp.float32)
        sources = [steps[PITCH * m : PITCH * m + 8, :] for m in range(9)]
        for h in range(2):
            at = pl.ds(row + h, TILES, stride=2)
            index = obs_cam[at, :]
            moves = [lane_take(source, index) for source in sources]
            jac = [jacs[h][PITCH * m : PITCH * m + 8, :] for m in range(24)]
            first = sum((jac[m] * moves[m] for m in range(1, 9)), jac[0] * moves[0])
            second = sum((jac[9 + m] * moves[m] for m in range(1, 9)), jac[9] * moves[0])
            side = sides[h]
            for n in range(3):
                value = jac[18 + n] * first + jac[21 + n] * second
                head = value.astype(jnp.bfloat16).astype(jnp.float32)
                side[PITCH * n : PITCH * n + 8, :] = head
                side[PITCH * (n + 4) : PITCH * (n + 4) + 8, :] = value - head
            point = obs_point[at, :]
            side[PITCH * 8 : PITCH * 8 + 8, :] = (point & (FINE - 1)).astype(jnp.float32)
            side[PITCH * 9 : PITCH * 9 + 8, :] = (point >> FINE_BITS).astype(jnp.float32)
        for t in range(TILES):
            heads, hots = [], []
            for h in range(2):
                value = sides[h][pl.ds(t, 8, stride=PITCH), :]
                value = jnp.concatenate([value, value], axis=0).astype(jnp.bfloat16)
                low = twice(sides[h][pl.ds(8 * PITCH + t, 1), :])
                high = twice(sides[h][pl.ds(9 * PITCH + t, 1), :])
                heads.append(jnp.concatenate([jnp.where(k == high, value, zero) for k in coarse], axis=0))
                hots.append(jnp.concatenate([jnp.where(k == low, one, zero) for k in fine], axis=0))
            summed = lax.dot_general(
                jnp.concatenate(heads, axis=1),
                jnp.concatenate(hots, axis=1),
                (((1,), (1,)), ((), ())),
                preferred_element_type=jnp.float32,
            )
            place = pl.ds(pl.multiple_of(tile_points[tile + t] * COARSE_ROWS, COARSE_ROWS), COARSE_ROWS)
            total[place, :] = total[place, :] + summed

    def turn(i, carry):
        for u in range(PAIRS):
            group(i * PAIRS + u, *buffers[u])
        return carry

    lax.fori_loop(0, obs_cam.shape[0] // (2 * TILES * PAIRS), turn, 0)

    @pl.when(step == pl.num_programs(0) - 1)
    def _():
        top = lax.broadcasted_iota(jnp.int32, (8, LANES), 0) < 4

        def fold(i, carry):
            for u in range(32):
                k = i * 32 + u
                base = pl.multiple_of(k * COARSE_ROWS, COARSE_ROWS)
                parts = [total[pl.ds(base + 8 * j, 8), :] for j in range(4)]
                pair = [jnp.concatenate(parts[2 * j : 2 * j + 2], axis=1) for j in range(2)]
                pair = [value + pltpu.roll(value, 4, 0) for value in pair]
                packed[pl.ds(pl.multiple_of(k * 8, 8), 8), :] = jnp.where(top, *pair)
            return carry

        lax.fori_loop(0, blocks // 32, fold, 0)
        for n in range(3):
            out[n] = packed[pl.ds(n, out.shape[1], stride=4), :]


def camera_rows(trial):
    w = trial[0:3]
    angle = jnp.sqrt(w[0:1] * w[0:1] + w[1:2] * w[1:2] + w[2:3] * w[2:3])
    head = math.sqrt(2.0) * jnp.cos(0.5 * angle)
    still = angle == 0.0
    ratio = jnp.where(still, 0.5, jnp.sin(0.5 * angle) / jnp.where(still, 1.0, angle))
    tail = math.sqrt(2.0) * ratio * w
    return jnp.concatenate([head, tail, trial[3:9]], axis=0)


def greet(axis, size, me):
    barrier = pltpu.get_barrier_semaphore()
    for d in range(1, size):
        pl.semaphore_signal(
            barrier, inc=1, device_id={axis: lax.rem(me + d, size)}, device_id_type=MESH
        )


def send_round(axis, size, me, source, target, send, recv):
    copies = []
    for d in range(1, size):
        peer = lax.rem(me + d, size)
        copies.append(
            pltpu.make_async_remote_copy(
                src_ref=source(peer, d),
                dst_ref=target(peer, d),
                send_sem=send.at[d - 1],
                recv_sem=recv.at[d - 1],
                device_id={axis: peer},
                device_id_type=MESH,
            )
        )
    for copy in copies:
        copy.start()
    return copies


def gather_kernel(
    n_pts, n_cam, hbm_cameras, hbm_increment, out, cameras, increment, in_sem, send_cam, recv_cam, send_pts, recv_pts
):
    p, c = lax.axis_index("pts"), lax.axis_index("cam")
    loads = [
        pltpu.make_async_copy(source, target, in_sem.at[i])
        for i, (source, target) in enumerate(((hbm_cameras, cameras), (hbm_increment, increment)))
    ]
    for load in loads:
        load.start()
    greet("pts", n_pts, p)
    greet("cam", n_cam, c)
    count = cameras.shape[1] // CB
    base = (p * n_cam + c) * count
    for load in loads:
        load.wait()
    for i in range(count):
        lanes = slice(i * CB, (i + 1) * CB)
        move = increment[:, lanes]
        trial = cameras[:, lanes] + move
        out[base + i, 0:9, :] = move
        out[base + i, 9:19, :] = camera_rows(trial)
    pl.semaphore_wait(pltpu.get_barrier_semaphore(), n_pts + n_cam - 2)

    def blocks(j):
        owner = p * n_cam + lax.rem(c - j + n_cam, n_cam)
        return out.at[pl.ds(owner * count, count), 0:19]

    def forward(j):
        return send_round("pts", n_pts, p, lambda *_: blocks(j), lambda *_: blocks(j), send_pts.at[j], recv_pts.at[j])

    copies = send_round("cam", n_cam, c, lambda *_: blocks(0), lambda *_: blocks(0), send_cam, recv_cam)
    forwarded = forward(0)
    for j in sorted(range(1, n_cam), key=lambda j: min(j, n_cam - j)):
        copies[j - 1].wait_recv()
        forwarded += forward(j)
    for copy in copies:
        copy.wait_send()
    for copy in forwarded:
        copy.wait()


def finish_kernel(
    n_pts, n_cam, tile_block, tile_points, planes, cam_table, points, gradient, inverse, hbm_cam, hbm_point,
    hbm_seen, residual, point_table, sums, out, landed, own_points, own_gradient, own_inverse, work, obs_cam, obs_point,
    observed, cam_store, partial, cam_slots, pts_slots, in_sem, send_sum, recv_sum, send_out,
    recv_out, send_cam, recv_cam, send_pts, recv_pts, *buffers,
):
    p, c = lax.axis_index("pts"), lax.axis_index("cam")
    streams = [
        pltpu.make_async_copy(source, target, in_sem.at[3 + i])
        for i, (source, target) in enumerate(
            ((hbm_cam, obs_cam), (hbm_point, obs_point), (hbm_seen, observed))
        )
    ]
    for stream in streams:
        stream.start()
    last = n_cam - 1
    chunks = landed.shape[1]
    rows = planes.shape[1] // 2
    count = rows // chunks
    span, pitch = rows * LANES, rows + 1
    low_end, high_end = c == 0, c == last
    at_end = jnp.logical_or(low_end, high_end)
    own_base = jnp.where(low_end, 0, rows)
    loads = [
        pltpu.make_async_copy(
            source.at[:, pl.ds(pl.multiple_of(own_base * LANES, LANES), span)], target, in_sem.at[i]
        )
        for i, (source, target) in enumerate(
            ((points, own_points), (gradient, own_gradient), (inverse, own_inverse))
        )
    ]

    @pl.when(at_end)
    def _():
        for load in loads:
            load.start()

    greet("pts", n_pts, p)
    greet("cam", n_cam, c)

    def take_cameras(i, carry):
        for u in range(SPREAD):
            block = i * SPREAD + u
            row = pl.multiple_of(block * 2 * TILES, 2 * TILES)
            buf = buffers[u]
            for t in range(TILES):
                slab = cam_table[tile_block[block * TILES + t]]
                buf[pl.ds(t, 8, stride=PITCH), :] = slab[0:8]
                buf[pl.ds(8 * PITCH + t, 2, stride=PITCH), :] = slab[8:10]
            sources = [buf[PITCH * m : PITCH * m + 8, :] for m in range(10)]
            for h in range(2):
                index = obs_cam[pl.ds(row + h, TILES, stride=2), :]
                for m in range(10):
                    cam_store[m, pl.ds(row + TILES * h, TILES), :] = lane_take(sources[m], index)
        return carry

    turns = obs_cam.shape[0] // (2 * TILES * SPREAD)
    early = turns // 4
    streams[0].wait()
    lax.fori_loop(0, early, take_cameras, 0)
    pl.semaphore_wait(pltpu.get_barrier_semaphore(), n_pts + n_cam - 2)

    def peer(step):
        return lax.rem(c + step + n_cam, n_cam)

    def place(way, k):
        base = rows if way == 0 else 0
        return pl.ds(pl.multiple_of(base + k * count, 8), count)

    def toward(way):
        return peer(1) if way == 0 else peer(-1)

    def sum_copy(way, k, source):
        return pltpu.make_async_remote_copy(
            src_ref=source,
            dst_ref=landed.at[way, k],
            send_sem=send_sum.at[way, k],
            recv_sem=recv_sum.at[way, k],
            device_id={"cam": toward(way)},
            device_id_type=MESH,
        )

    def out_copy(way, k):
        part = out.at[:, place(way, k)]
        return pltpu.make_async_remote_copy(
            src_ref=part,
            dst_ref=part,
            send_sem=send_out.at[way, k],
            recv_sem=recv_out.at[way, k],
            device_id={"cam": toward(1 - way)},
            device_id_type=MESH,
        )

    for way, first in ((0, low_end), (1, high_end)):

        @pl.when(first)
        def _(way=way):
            def begin(k, carry):
                sum_copy(way, k, planes.at[:, place(way, k)]).start()
                return carry

            lax.fori_loop(0, chunks, begin, 0)

    lax.fori_loop(early, turns, take_cameras, 0)

    @pl.when(at_end)
    def _():
        for load in loads:
            load.wait()

        def spread(i, carry):
            for u in range(8):
                k = i * 8 + u
                lanes = pl.ds(pl.multiple_of(k * LANES, LANES), LANES)
                work[pl.ds(k, 3, stride=pitch), :] = own_points[:, lanes]
                work[pl.ds(3 * pitch + k, 3, stride=pitch), :] = own_gradient[:, lanes]
                block = own_inverse[:, lanes]
                work[pl.ds(6 * pitch + k, 8, stride=pitch), :] = block[0:8]
                work[pl.ds(14 * pitch + k, 1), :] = block[8:9]
            return carry

        lax.fori_loop(0, rows // 8, spread, 0)

    def solved(way, k):
        def row(m):
            return work[pl.ds(m * pitch + k * count, count), :]

        total = landed[way, k] + planes[:, place(way, k), :]
        residue = [row(3 + n) - total[n] for n in range(3)]
        for n in range(3):
            move = row(6 + 3 * n) * residue[0] + row(7 + 3 * n) * residue[1] + row(8 + 3 * n) * residue[2]
            out[n, place(way, k), :] = row(n) + move

    def turn(s, carry):
        for way, hops in ((0, c), (1, last - c)):
            k = s - LAG * hops
            live = jnp.logical_and(hops > 0, jnp.logical_and(k >= 0, k < chunks))

            @pl.when(live)
            def _(way=way, k=k, hops=hops):
                sum_copy(way, k, landed.at[way, k]).wait_recv()

                @pl.when(hops < last)
                def _():
                    landed[way, k] = landed[way, k] + planes[:, place(way, k), :]
                    sum_copy(way, k, landed.at[way, k]).start()

                @pl.when(hops == last)
                def _():
                    solved(way, k)
                    out_copy(way, k).start()

        for way, hops in ((0, last - c), (1, c)):
            k = s - LAG * (last + hops)
            live = jnp.logical_and(hops > 0, jnp.logical_and(k >= 0, k < chunks))

            @pl.when(live)
            def _(way=way, k=k, hops=hops):
                out_copy(way, k).wait_recv()

                @pl.when(hops < last)
                def _():
                    out_copy(way, k).start()

        return carry

    lax.fori_loop(0, chunks + 2 * LAG * last, turn, 0)

    def finish(k, carry):
        for way, first, end in ((0, low_end, high_end), (1, high_end, low_end)):

            @pl.when(jnp.logical_not(end))
            def _(way=way):
                sum_copy(way, k, landed.at[way, k]).wait_send()

            @pl.when(jnp.logical_not(first))
            def _(way=way):
                out_copy(way, k).wait_send()

        return carry

    lax.fori_loop(0, chunks, finish, 0)
    for n in range(3):
        point_table[pl.ds(n, out.shape[1], stride=4), :] = out[n]
    point_table[pl.ds(3, out.shape[1], stride=4), :] = jnp.zeros_like(out[0])
    point_slabs = point_table.reshape(point_table.shape[0] // 8, 8, LANES)
    for stream in streams[1:]:
        stream.wait()

    def project(i, carry):
        for u in range(SPREAD):
            block = i * SPREAD + u
            row = pl.multiple_of(block * 2 * TILES, 2 * TILES)
            buf = buffers[u]
            for t in range(TILES):
                buf[pl.ds(t, 8, stride=PITCH), :] = point_slabs[tile_points[block * TILES + t]]
            sources = [buf[PITCH * m : PITCH * m + 8, :] for m in range(8)]
            for h in range(2):
                point = obs_point[pl.ds(row + h, TILES, stride=2), :]
                local = point & (LANES - 1)
                upper = point >= LANES
                x, y, z = (
                    jnp.where(upper, lane_take(sources[4 + n], local), lane_take(sources[n], local))
                    for n in range(3)
                )
                head, a, b, c, *shift, focal, k1, k2 = (
                    cam_store[m, pl.ds(row + TILES * h, TILES), :] for m in range(10)
                )
                e, f, g = b * z - c * y, c * x - a * z, a * y - b * x
                px = x + shift[0] + (head * e + (b * g - c * f))
                py = y + shift[1] + (head * f + (c * e - a * g))
                pz = z + shift[2] + (head * g + (a * f - b * e))
                scale = 1.0 / jnp.maximum(-pz, 1.0)
                fu, fv = px * scale, py * scale
                q = fu * fu + fv * fv
                factor = focal * (1.0 + q * (k1 + k2 * q))
                at_u = pl.ds(2 * (row + h), TILES, stride=4)
                at_v = pl.ds(2 * (row + h) + 1, TILES, stride=4)
                ru = factor * fu - observed[at_u, :]
                rv = factor * fv - observed[at_v, :]
                residual[at_u, :] = ru
                residual[at_v, :] = rv
                carry = carry + (ru * ru + rv * rv)
        return carry

    partial[...] = lax.fori_loop(0, turns, project, jnp.zeros((8, LANES), jnp.float32))
    slot = cam_slots.at[c]
    exchange = send_round("cam", n_cam, c, lambda *_: partial, lambda *_: slot, send_cam, recv_cam)
    cam_slots[c] = partial[...]
    for copy in exchange:
        copy.wait()
    value = cam_slots[0]
    for i in range(1, n_cam):
        value = value + cam_slots[i]
    pts_slots[p] = value
    slot = pts_slots.at[p]
    for copy in send_round("pts", n_pts, p, lambda *_: slot, lambda *_: slot, send_pts, recv_pts):
        copy.wait()
    value = pts_slots[0]
    for i in range(1, n_pts):
        value = value + pts_slots[i]
    sums[...] = value


def emit_kernel(
    scale, accept, sums, seen, table, points, cameras, increment, residual, cost, accepted_points, accepted_cameras, sem
):
    copy = pltpu.make_async_copy(seen, residual, sem)
    copy.start()
    odd = (accept[0] & 1) == 1
    accepted_cameras[...] = cameras[...] + odd.astype(jnp.float32) * increment[...]
    total = jnp.sum(sums[...], axis=1, keepdims=True)
    cost[0] = jnp.sum(total) * scale

    def turn(i, carry):
        for u in range(16):
            k = i * 16 + u
            lanes = pl.ds(pl.multiple_of(k * LANES, LANES), LANES)
            accepted_points[:, lanes] = jnp.where(odd, table[pl.ds(4 * k, 3), :], points[:, lanes])
        return carry

    lax.fori_loop(0, table.shape[0] // 64, turn, 0)
    copy.wait()


def on_device(
    cameras, increment, points, point_gradient, point_inverse, cam_jacobian, point_jacobian,
    observed, tile_block, tile_points, obs_camera, obs_point, accept,
):
    own_blocks = cameras.shape[1] // CB
    n_pts, n_cam = lax.axis_size("pts"), lax.axis_size("cam")
    vmem = pl.BlockSpec(memory_space=pltpu.VMEM)
    hbm = pl.BlockSpec(memory_space=pltpu.HBM)

    def dma_sems(*counts):
        return [pltpu.SemaphoreType.DMA((count,)) for count in counts]

    def remote(ident):
        return pltpu.CompilerParams(
            collective_id=ident, has_side_effects=True, vmem_limit_bytes=36 * 2**20
        )

    every = pl.pallas_call(
        functools.partial(gather_kernel, n_pts, n_cam),
        in_specs=[hbm, hbm],
        out_specs=vmem,
        out_shape=jax.ShapeDtypeStruct((own_blocks * n_pts * n_cam, 24, CB), jnp.float32),
        scratch_shapes=[pltpu.VMEM(cameras.shape, jnp.float32)] * 2
        + dma_sems(2, n_cam - 1, n_cam - 1)
        + [pltpu.SemaphoreType.DMA((n_cam, n_pts - 1))] * 2,
        compiler_params=remote(0),
        cost_estimate=pl.CostEstimate(flops=2**30, bytes_accessed=2**20, transcendentals=0),
        name="cameras",
    )(cameras, increment)
    cam_blocks = every.shape[0]
    cam_table = jnp.concatenate([every[:, 9:19], jnp.zeros((cam_blocks, 6, CB), jnp.float32)], axis=1)

    obs_count = obs_camera.shape[0]
    rows = obs_count // LANES
    per = math.gcd(rows, BLOCKS_PER_STEP)
    grid = (rows // per,)
    point_blocks = points.shape[1] // PB
    oc = obs_camera.reshape(rows, LANES)
    op = obs_point.reshape(rows, LANES)

    def whole(*shape):
        return pl.BlockSpec(shape, lambda i, *_: (0,) * len(shape))

    params = pltpu.CompilerParams(dimension_semantics=("arbitrary",), vmem_limit_bytes=50 * 2**20)
    planes = pl.pallas_call(
        couple_kernel,
        grid_spec=pltpu.PrefetchScalarGridSpec(
            num_scalar_prefetch=2,
            grid=grid,
            in_specs=[
                pl.BlockSpec((18, per * LANES), lambda i, *_: (0, i)),
                pl.BlockSpec((6, per * LANES), lambda i, *_: (0, i)),
                pl.BlockSpec((per, LANES), lambda i, *_: (i, 0)),
                pl.BlockSpec((per, LANES), lambda i, *_: (i, 0)),
                whole(cam_blocks, 24, CB),
            ],
            out_specs=whole(3, 2 * point_blocks, LANES),
            scratch_shapes=[
                pltpu.VMEM((point_blocks * COARSE_ROWS, FINE), jnp.float32),
                pltpu.VMEM((point_blocks * 8, LANES), jnp.float32),
            ]
            + [
                pltpu.VMEM((count * PITCH, LANES), jnp.float32) for count in (9, 24, 24, 10, 10)
            ]
            * PAIRS,
        ),
        out_shape=jax.ShapeDtypeStruct((3, 2 * point_blocks, LANES), jnp.float32),
        compiler_params=params,
        name="couple",
    )(tile_block, tile_points, cam_jacobian, point_jacobian, oc, op, every)

    own_rows = point_blocks
    chunks = math.gcd(own_rows // 8, CHUNKS)
    anywhere = pl.BlockSpec(memory_space=pl.ANY)
    smem = pl.BlockSpec(memory_space=pltpu.SMEM)
    seen = observed.reshape(2, rows, LANES).transpose(1, 0, 2).reshape(2 * rows, LANES)
    residual, point_table, sums = pl.pallas_call(
        functools.partial(finish_kernel, n_pts, n_cam),
        in_specs=[smem, smem, vmem, vmem] + [anywhere] * 6,
        out_specs=[vmem, vmem, vmem],
        out_shape=[
            jax.ShapeDtypeStruct((2 * rows, LANES), jnp.float32),
            jax.ShapeDtypeStruct((point_blocks * 8, LANES), jnp.float32),
            jax.ShapeDtypeStruct((8, LANES), jnp.float32),
        ],
        scratch_shapes=[
            pltpu.VMEM(planes.shape, jnp.float32),
            pltpu.VMEM((2, chunks, 3, own_rows // chunks, LANES), jnp.float32),
            pltpu.VMEM((3, own_rows * LANES), jnp.float32),
            pltpu.VMEM((3, own_rows * LANES), jnp.float32),
            pltpu.VMEM((9, own_rows * LANES), jnp.float32),
            pltpu.VMEM((15 * (own_rows + 1), LANES), jnp.float32),
            pltpu.VMEM((rows, LANES), jnp.int32),
            pltpu.VMEM((rows, LANES), jnp.int32),
            pltpu.VMEM((2 * rows, LANES), jnp.float32),
            pltpu.VMEM((10, rows, LANES), jnp.float32),
            pltpu.VMEM((8, LANES), jnp.float32),
            pltpu.VMEM((n_cam, 8, LANES), jnp.float32),
            pltpu.VMEM((n_pts, 8, LANES), jnp.float32),
            pltpu.SemaphoreType.DMA((6,)),
        ]
        + [pltpu.SemaphoreType.DMA((2, chunks))] * 4
        + dma_sems(n_cam - 1, n_cam - 1, n_pts - 1, n_pts - 1)
        + [pltpu.VMEM((10 * PITCH, LANES), jnp.float32)] * SPREAD,
        compiler_params=remote(1),
        name="finish",
    )(
        tile_block, tile_points, planes, cam_table, points, point_gradient,
        point_inverse, oc, op, seen,
    )
    residual, cost, accepted_points, accepted_cameras = pl.pallas_call(
        functools.partial(emit_kernel, 1.0 / (2.0 * obs_count * n_pts * n_cam)),
        in_specs=[smem] + [vmem] * 6,
        out_specs=[anywhere, smem, vmem, vmem],
        out_shape=[
            jax.ShapeDtypeStruct((2 * rows, LANES), jnp.float32),
            jax.ShapeDtypeStruct((1,), jnp.float32),
            jax.ShapeDtypeStruct(points.shape, jnp.float32),
            jax.ShapeDtypeStruct(cameras.shape, jnp.float32),
        ],
        scratch_shapes=[pltpu.SemaphoreType.DMA],
        compiler_params=pltpu.CompilerParams(vmem_limit_bytes=16 * 2**20),
        name="emit",
    )(accept.reshape(1), sums, residual, point_table, points, cameras, increment)
    residual = residual.reshape(rows, 2, LANES).transpose(1, 0, 2).reshape(2, obs_count)
    return residual, cost.reshape(()), accepted_points, accepted_cameras


def solution(mesh):
    in_specs = (
        P(None, ("pts", "cam")),
        P(None, ("pts", "cam")),
        P(None, "pts"),
        P(None, "pts"),
        P(None, "pts"),
        P(None, ("pts", "cam")),
        P(None, ("pts", "cam")),
        P(None, ("pts", "cam")),
        P(("pts", "cam")),
        P(("pts", "cam")),
        P(("pts", "cam")),
        P(("pts", "cam")),
        P(),
    )
    out_specs = (P(None, ("pts", "cam")), P(), P(None, "pts"), P(None, ("pts", "cam")))
    return jax.shard_map(
        on_device, mesh=mesh, in_specs=in_specs, out_specs=out_specs, check_vma=False
    )
```

```python
import functools
import math

import jax
import jax.numpy as jnp
from jax import lax
from jax.experimental import pallas as pl
from jax.experimental.pallas import tpu as pltpu
from jax.sharding import PartitionSpec as P

CB = 128
PB = 256
TILE = 256
LANES = 128
PITCH = 9
FINE = 64
FINE_BITS = 6
COARSE_ROWS = 32
PAIRS = 8
TILES = 8
SPREAD = 16
CHUNKS = 16
LAG = 5
BLOCKS_PER_STEP = 256
MESH = pl.DeviceIdType.MESH


LANE_GATHER = lax.GatherDimensionNumbers(
    offset_dims=(),
    collapsed_slice_dims=(1,),
    start_index_map=(1,),
    operand_batching_dims=(0,),
    start_indices_batching_dims=(0,),
)


def lane_take(slab, index):
    return lax.gather(
        slab, index[:, :, None], LANE_GATHER, (1, 1), mode=lax.GatherScatterMode.PROMISE_IN_BOUNDS
    )


def couple_kernel(
    tile_block, tile_points, cam_jac, point_jac, obs_cam, obs_point, table, out, total, packed, *scratch
):
    step = pl.program_id(0)
    tiles_per_step = obs_cam.shape[0] // 2
    buffers = [scratch[5 * u : 5 * u + 5] for u in range(PAIRS)]
    blocks = packed.shape[0] // 8

    @pl.when(step == 0)
    def _():
        total[...] = jnp.zeros_like(total)
        for _, _, _, low, high in buffers:
            low[...] = jnp.zeros_like(low)
            high[...] = jnp.zeros_like(high)

    wide = lax.broadcasted_iota(jnp.int32, (16, LANES), 0)
    fine = [(wide + 16 * k).astype(jnp.float32).astype(jnp.bfloat16) for k in range(FINE // 16)]
    half = (wide >= 8).astype(jnp.float32)
    coarse = [(half + 2.0 * k).astype(jnp.bfloat16) for k in range(PB // FINE // 2)]
    one = jnp.ones((16, LANES), jnp.bfloat16)
    zero = jnp.zeros((16, LANES), jnp.bfloat16)

    def twice(row):
        return jnp.broadcast_to(row, (16, LANES)).astype(jnp.bfloat16)

    def group(block, steps, *halves):
        jacs, sides = halves[:2], halves[2:]
        row = pl.multiple_of(block * 2 * TILES, 2 * TILES)
        tile = step * tiles_per_step + block * TILES
        for t in range(TILES):
            slab = table.at[tile_block[tile + t]]
            steps[pl.ds(t, 8, stride=PITCH), :] = slab[0:8, :]
            steps[pl.ds(8 * PITCH + t, 1), :] = slab[8:9, :]
            for h in range(2):
                lane = pl.ds(pl.multiple_of((row + 2 * t + h) * LANES, LANES), LANES)
                jac = cam_jac[:, lane].astype(jnp.float32)
                jacs[h][pl.ds(t, 8, stride=PITCH), :] = jac[0:8]
                jacs[h][pl.ds(8 * PITCH + t, 8, stride=PITCH), :] = jac[8:16]
                jacs[h][pl.ds(16 * PITCH + t, 2, stride=PITCH), :] = jac[16:18]
                jacs[h][pl.ds(18 * PITCH + t, 6, stride=PITCH), :] = point_jac[:, lane].astype(jnp.float32)
        sources = [steps[PITCH * m : PITCH * m + 8, :] for m in range(9)]
        for h in range(2):
            at = pl.ds(row + h, TILES, stride=2)
            index = obs_cam[at, :]
            moves = [lane_take(source, index) for source in sources]
            jac = [jacs[h][PITCH * m : PITCH * m + 8, :] for m in range(24)]
            first = sum((jac[m] * moves[m] for m in range(1, 9)), jac[0] * moves[0])
            second = sum((jac[9 + m] * moves[m] for m in range(1, 9)), jac[9] * moves[0])
            side = sides[h]
            for n in range(3):
                value = jac[18 + n] * first + jac[21 + n] * second
                head = value.astype(jnp.bfloat16).astype(jnp.float32)
                side[PITCH * n : PITCH * n + 8, :] = head
                side[PITCH * (n + 4) : PITCH * (n + 4) + 8, :] = value - head
            point = obs_point[at, :]
            side[PITCH * 8 : PITCH * 8 + 8, :] = (point & (FINE - 1)).astype(jnp.float32)
            side[PITCH * 9 : PITCH * 9 + 8, :] = (point >> FINE_BITS).astype(jnp.float32)
        for t in range(TILES):
            heads, hots = [], []
            for h in range(2):
                value = sides[h][pl.ds(t, 8, stride=PITCH), :]
                value = jnp.concatenate([value, value], axis=0).astype(jnp.bfloat16)
                low = twice(sides[h][pl.ds(8 * PITCH + t, 1), :])
                high = twice(sides[h][pl.ds(9 * PITCH + t, 1), :])
                heads.append(jnp.concatenate([jnp.where(k == high, value, zero) for k in coarse], axis=0))
                hots.append(jnp.concatenate([jnp.where(k == low, one, zero) for k in fine], axis=0))
            summed = lax.dot_general(
                jnp.concatenate(heads, axis=1),
                jnp.concatenate(hots, axis=1),
                (((1,), (1,)), ((), ())),
                preferred_element_type=jnp.float32,
            )
            place = pl.ds(pl.multiple_of(tile_points[tile + t] * COARSE_ROWS, COARSE_ROWS), COARSE_ROWS)
            total[place, :] = total[place, :] + summed

    def turn(i, carry):
        for u in range(PAIRS):
            group(i * PAIRS + u, *buffers[u])
        return carry

    lax.fori_loop(0, obs_cam.shape[0] // (2 * TILES * PAIRS), turn, 0)

    @pl.when(step == pl.num_programs(0) - 1)
    def _():
        top = lax.broadcasted_iota(jnp.int32, (8, LANES), 0) < 4

        def fold(i, carry):
            for u in range(32):
                k = i * 32 + u
                base = pl.multiple_of(k * COARSE_ROWS, COARSE_ROWS)
                parts = [total[pl.ds(base + 8 * j, 8), :] for j in range(4)]
                pair = [jnp.concatenate(parts[2 * j : 2 * j + 2], axis=1) for j in range(2)]
                pair = [value + pltpu.roll(value, 4, 0) for value in pair]
                packed[pl.ds(pl.multiple_of(k * 8, 8), 8), :] = jnp.where(top, *pair)
            return carry

        lax.fori_loop(0, blocks // 32, fold, 0)
        count = out.shape[2]
        for i in range(out.shape[0]):
            for n in range(3):
                out[i, n] = packed[pl.ds(4 * count * i + n, count, stride=4), :]


def camera_rows(trial):
    w = trial[0:3]
    angle = jnp.sqrt(w[0:1] * w[0:1] + w[1:2] * w[1:2] + w[2:3] * w[2:3])
    head = math.sqrt(2.0) * jnp.cos(0.5 * angle)
    still = angle == 0.0
    ratio = jnp.where(still, 0.5, jnp.sin(0.5 * angle) / jnp.where(still, 1.0, angle))
    tail = math.sqrt(2.0) * ratio * w
    return jnp.concatenate([head, tail, trial[3:9]], axis=0)


def greet(axis, size, me):
    barrier = pltpu.get_barrier_semaphore()
    for d in range(1, size):
        pl.semaphore_signal(
            barrier, inc=1, device_id={axis: lax.rem(me + d, size)}, device_id_type=MESH
        )


def send_round(axis, size, me, source, target, send, recv):
    copies = []
    for d in range(1, size):
        peer = lax.rem(me + d, size)
        copies.append(
            pltpu.make_async_remote_copy(
                src_ref=source(peer, d),
                dst_ref=target(peer, d),
                send_sem=send.at[d - 1],
                recv_sem=recv.at[d - 1],
                device_id={axis: peer},
                device_id_type=MESH,
            )
        )
    for copy in copies:
        copy.start()
    return copies


def gather_kernel(
    n_pts, n_cam, hbm_cameras, hbm_increment, out, cameras, increment, in_sem, send_cam, recv_cam, send_pts, recv_pts
):
    p, c = lax.axis_index("pts"), lax.axis_index("cam")
    loads = [
        pltpu.make_async_copy(source, target, in_sem.at[i])
        for i, (source, target) in enumerate(((hbm_cameras, cameras), (hbm_increment, increment)))
    ]
    for load in loads:
        load.start()
    greet("pts", n_pts, p)
    greet("cam", n_cam, c)
    count = cameras.shape[1] // CB
    base = (p * n_cam + c) * count
    for load in loads:
        load.wait()
    for i in range(count):
        lanes = slice(i * CB, (i + 1) * CB)
        move = increment[:, lanes]
        trial = cameras[:, lanes] + move
        out[base + i, 0:9, :] = move
        out[base + i, 9:19, :] = camera_rows(trial)
    pl.semaphore_wait(pltpu.get_barrier_semaphore(), n_pts + n_cam - 2)

    def blocks(j):
        owner = p * n_cam + lax.rem(c - j + n_cam, n_cam)
        return out.at[pl.ds(owner * count, count), 0:19]

    def forward(j):
        return send_round("pts", n_pts, p, lambda *_: blocks(j), lambda *_: blocks(j), send_pts.at[j], recv_pts.at[j])

    copies = send_round("cam", n_cam, c, lambda *_: blocks(0), lambda *_: blocks(0), send_cam, recv_cam)
    forwarded = forward(0)
    for j in sorted(range(1, n_cam), key=lambda j: min(j, n_cam - j)):
        copies[j - 1].wait_recv()
        forwarded += forward(j)
    for copy in copies:
        copy.wait_send()
    for copy in forwarded:
        copy.wait()


def finish_kernel(
    n_pts, n_cam, tile_block, tile_points, planes, cam_table, points, gradient, inverse, hbm_cam, hbm_point,
    hbm_seen, residual, point_table, sums, out, landed, own_points, own_gradient, own_inverse, work, obs_cam, obs_point,
    observed, cam_store, slots, in_sem, send_sum, recv_sum, send_out,
    recv_out, send_cost, recv_cost, *buffers,
):
    p, c = lax.axis_index("pts"), lax.axis_index("cam")
    streams = [
        pltpu.make_async_copy(source, target, in_sem.at[3 + i])
        for i, (source, target) in enumerate(
            ((hbm_cam, obs_cam), (hbm_point, obs_point), (hbm_seen, observed))
        )
    ]
    for stream in streams:
        stream.start()
    last = n_cam - 1
    chunks = landed.shape[1]
    count = planes.shape[2]
    rows = count * chunks
    span, pitch = rows * LANES, rows + 1
    low_end, high_end = c == 0, c == last
    at_end = jnp.logical_or(low_end, high_end)
    own_base = jnp.where(low_end, 0, rows)
    loads = [
        pltpu.make_async_copy(
            source.at[:, pl.ds(pl.multiple_of(own_base * LANES, LANES), span)], target, in_sem.at[i]
        )
        for i, (source, target) in enumerate(
            ((points, own_points), (gradient, own_gradient), (inverse, own_inverse))
        )
    ]

    @pl.when(at_end)
    def _():
        for load in loads:
            load.start()

    greet("pts", n_pts, p)
    barrier = pltpu.get_barrier_semaphore()

    def peer(step):
        return lax.rem(c + step + n_cam, n_cam)

    @pl.when(c > 0)
    def _():
        pl.semaphore_signal(barrier, inc=1, device_id={"cam": peer(-1)}, device_id_type=MESH)

    @pl.when(c < last)
    def _():
        pl.semaphore_signal(barrier, inc=1, device_id={"cam": peer(1)}, device_id_type=MESH)

    def take_cameras(i, carry):
        for u in range(SPREAD):
            block = i * SPREAD + u
            row = pl.multiple_of(block * 2 * TILES, 2 * TILES)
            buf = buffers[u]
            for t in range(TILES):
                slab = cam_table[tile_block[block * TILES + t]]
                buf[pl.ds(t, 8, stride=PITCH), :] = slab[0:8]
                buf[pl.ds(8 * PITCH + t, 2, stride=PITCH), :] = slab[8:10]
            sources = [buf[PITCH * m : PITCH * m + 8, :] for m in range(10)]
            for h in range(2):
                index = obs_cam[pl.ds(row + h, TILES, stride=2), :]
                for m in range(10):
                    cam_store[m, pl.ds(row + TILES * h, TILES), :] = lane_take(sources[m], index)
        return carry

    turns = obs_cam.shape[0] // (2 * TILES * SPREAD)
    early = turns // 4
    streams[0].wait()
    lax.fori_loop(0, early, take_cameras, 0)
    pl.semaphore_wait(barrier, n_pts - 1 + jnp.where(at_end, 1, 2))

    def place(way, k):
        return k + chunks if way == 0 else k

    def toward(way):
        return peer(1) if way == 0 else peer(-1)

    def sum_copy(way, k, source):
        return pltpu.make_async_remote_copy(
            src_ref=source,
            dst_ref=landed.at[way, k],
            send_sem=send_sum.at[way, k],
            recv_sem=recv_sum.at[way, k],
            device_id={"cam": toward(way)},
            device_id_type=MESH,
        )

    def out_copy(way, k):
        part = out.at[place(way, k)]
        return pltpu.make_async_remote_copy(
            src_ref=part,
            dst_ref=part,
            send_sem=send_out.at[way, k],
            recv_sem=recv_out.at[way, k],
            device_id={"cam": toward(1 - way)},
            device_id_type=MESH,
        )

    for way, first in ((0, low_end), (1, high_end)):

        @pl.when(first)
        def _(way=way):
            def begin(k, carry):
                sum_copy(way, k, planes.at[place(way, k)]).start()
                return carry

            lax.fori_loop(0, chunks, begin, 0)

    lax.fori_loop(early, turns, take_cameras, 0)

    @pl.when(at_end)
    def _():
        for load in loads:
            load.wait()

        def spread(i, carry):
            for u in range(8):
                k = i * 8 + u
                lanes = pl.ds(pl.multiple_of(k * LANES, LANES), LANES)
                work[pl.ds(k, 3, stride=pitch), :] = own_points[:, lanes]
                work[pl.ds(3 * pitch + k, 3, stride=pitch), :] = own_gradient[:, lanes]
                block = own_inverse[:, lanes]
                work[pl.ds(6 * pitch + k, 8, stride=pitch), :] = block[0:8]
                work[pl.ds(14 * pitch + k, 1), :] = block[8:9]
            return carry

        lax.fori_loop(0, rows // 8, spread, 0)

    def solved(way, k):
        def row(m):
            return work[pl.ds(m * pitch + k * count, count), :]

        total = landed[way, k] + planes[place(way, k)]
        residue = [row(3 + n) - total[n] for n in range(3)]
        for n in range(3):
            move = row(6 + 3 * n) * residue[0] + row(7 + 3 * n) * residue[1] + row(8 + 3 * n) * residue[2]
            out[place(way, k), n] = row(n) + move

    def turn(s, carry):
        for way, hops in ((0, c), (1, last - c)):
            k = s - LAG * hops
            live = jnp.logical_and(hops > 0, jnp.logical_and(k >= 0, k < chunks))

            @pl.when(live)
            def _(way=way, k=k, hops=hops):
                sum_copy(way, k, landed.at[way, k]).wait_recv()

                @pl.when(hops < last)
                def _():
                    landed[way, k] = landed[way, k] + planes[place(way, k)]
                    sum_copy(way, k, landed.at[way, k]).start()

                @pl.when(hops == last)
                def _():
                    solved(way, k)
                    out_copy(way, k).start()

        for way, hops in ((0, last - c), (1, c)):
            k = s - LAG * (last + hops)
            live = jnp.logical_and(hops > 0, jnp.logical_and(k >= 0, k < chunks))

            @pl.when(live)
            def _(way=way, k=k, hops=hops):
                out_copy(way, k).wait_recv()

                @pl.when(hops < last)
                def _():
                    out_copy(way, k).start()

        return carry

    lax.fori_loop(0, chunks + 2 * LAG * last, turn, 0)

    def finish(k, carry):
        for way, first, end in ((0, low_end, high_end), (1, high_end, low_end)):

            @pl.when(jnp.logical_not(end))
            def _(way=way):
                sum_copy(way, k, landed.at[way, k]).wait_send()

            @pl.when(jnp.logical_not(first))
            def _(way=way):
                out_copy(way, k).wait_send()

        return carry

    lax.fori_loop(0, chunks, finish, 0)
    point_table[...] = jnp.zeros_like(point_table)
    for i in range(2 * chunks):
        for n in range(3):
            point_table[pl.ds(4 * count * i + n, count, stride=4), :] = out[i, n]
    point_slabs = point_table.reshape(point_table.shape[0] // 8, 8, LANES)
    for stream in streams[1:]:
        stream.wait()

    def project(i, carry):
        for u in range(SPREAD):
            block = i * SPREAD + u
            row = pl.multiple_of(block * 2 * TILES, 2 * TILES)
            buf = buffers[u]
            for t in range(TILES):
                buf[pl.ds(t, 8, stride=PITCH), :] = point_slabs[tile_points[block * TILES + t]]
            sources = [buf[PITCH * m : PITCH * m + 8, :] for m in range(8)]
            for h in range(2):
                point = obs_point[pl.ds(row + h, TILES, stride=2), :]
                local = point & (LANES - 1)
                upper = point >= LANES
                x, y, z = (
                    jnp.where(upper, lane_take(sources[4 + n], local), lane_take(sources[n], local))
                    for n in range(3)
                )
                head, a, b, c, *shift, focal, k1, k2 = (
                    cam_store[m, pl.ds(row + TILES * h, TILES), :] for m in range(10)
                )
                e, f, g = b * z - c * y, c * x - a * z, a * y - b * x
                px = x + shift[0] + (head * e + (b * g - c * f))
                py = y + shift[1] + (head * f + (c * e - a * g))
                pz = z + shift[2] + (head * g + (a * f - b * e))
                scale = 1.0 / jnp.maximum(-pz, 1.0)
                fu, fv = px * scale, py * scale
                q = fu * fu + fv * fv
                factor = focal * (1.0 + q * (k1 + k2 * q))
                at_u = pl.ds(2 * (row + h), TILES, stride=4)
                at_v = pl.ds(2 * (row + h) + 1, TILES, stride=4)
                ru = factor * fu - observed[at_u, :]
                rv = factor * fv - observed[at_v, :]
                residual[at_u, :] = ru
                residual[at_v, :] = rv
                carry = carry + (ru * ru + rv * rv)
        return carry

    cost = lax.fori_loop(0, turns, project, jnp.zeros((8, LANES), jnp.float32))
    me = p * n_cam + c
    slots[pl.ds(me, 1), :] = jnp.sum(cost, axis=0, keepdims=True)
    mine = slots.at[pl.ds(me, 1)]
    copies = []
    for j in range(1, n_pts * n_cam):
        step_p, step_c = j // n_cam, j % n_cam
        copies.append(
            pltpu.make_async_remote_copy(
                src_ref=mine,
                dst_ref=mine,
                send_sem=send_cost.at[j],
                recv_sem=recv_cost.at[j],
                device_id={"pts": lax.rem(p + step_p, n_pts), "cam": lax.rem(c + step_c, n_cam)},
                device_id_type=MESH,
            )
        )
    for copy in copies:
        copy.start()
    for copy in copies:
        copy.wait()
    sums[...] = jnp.sum(slots[...], axis=0, keepdims=True)


def emit_kernel(
    scale, accept, sums, seen, table, points, cameras, increment, residual, cost, accepted_points, accepted_cameras, sem
):
    copy = pltpu.make_async_copy(seen, residual, sem)
    copy.start()
    odd = (accept[0] & 1) == 1
    accepted_cameras[...] = cameras[...] + odd.astype(jnp.float32) * increment[...]
    cost[0] = jnp.sum(sums[...]) * scale

    def turn(i, carry):
        for u in range(16):
            k = i * 16 + u
            lanes = pl.ds(pl.multiple_of(k * LANES, LANES), LANES)
            accepted_points[:, lanes] = jnp.where(odd, table[pl.ds(4 * k, 3), :], points[:, lanes])
        return carry

    lax.fori_loop(0, table.shape[0] // 64, turn, 0)
    copy.wait()


def on_device(
    cameras, increment, points, point_gradient, point_inverse, cam_jacobian, point_jacobian,
    observed, tile_block, tile_points, obs_camera, obs_point, accept,
):
    own_blocks = cameras.shape[1] // CB
    n_pts, n_cam = lax.axis_size("pts"), lax.axis_size("cam")
    vmem = pl.BlockSpec(memory_space=pltpu.VMEM)
    hbm = pl.BlockSpec(memory_space=pltpu.HBM)

    def dma_sems(*counts):
        return [pltpu.SemaphoreType.DMA((count,)) for count in counts]

    def remote(ident):
        return pltpu.CompilerParams(
            collective_id=ident, has_side_effects=True, vmem_limit_bytes=36 * 2**20
        )

    every = pl.pallas_call(
        functools.partial(gather_kernel, n_pts, n_cam),
        in_specs=[hbm, hbm],
        out_specs=vmem,
        out_shape=jax.ShapeDtypeStruct((own_blocks * n_pts * n_cam, 24, CB), jnp.float32),
        scratch_shapes=[pltpu.VMEM(cameras.shape, jnp.float32)] * 2
        + dma_sems(2, n_cam - 1, n_cam - 1)
        + [pltpu.SemaphoreType.DMA((n_cam, n_pts - 1))] * 2,
        compiler_params=remote(0),
        cost_estimate=pl.CostEstimate(flops=2**30, bytes_accessed=2**20, transcendentals=0),
        name="cameras",
    )(cameras, increment)
    cam_blocks = every.shape[0]
    cam_table = jnp.concatenate([every[:, 9:19], jnp.zeros((cam_blocks, 6, CB), jnp.float32)], axis=1)

    obs_count = obs_camera.shape[0]
    rows = obs_count // LANES
    per = math.gcd(rows, BLOCKS_PER_STEP)
    grid = (rows // per,)
    point_blocks = points.shape[1] // PB
    chunks = math.gcd(point_blocks // 8, CHUNKS)
    oc = obs_camera.reshape(rows, LANES)
    op = obs_point.reshape(rows, LANES)

    def whole(*shape):
        return pl.BlockSpec(shape, lambda i, *_: (0,) * len(shape))

    params = pltpu.CompilerParams(dimension_semantics=("arbitrary",), vmem_limit_bytes=50 * 2**20)
    planes = pl.pallas_call(
        couple_kernel,
        grid_spec=pltpu.PrefetchScalarGridSpec(
            num_scalar_prefetch=2,
            grid=grid,
            in_specs=[
                pl.BlockSpec((18, per * LANES), lambda i, *_: (0, i)),
                pl.BlockSpec((6, per * LANES), lambda i, *_: (0, i)),
                pl.BlockSpec((per, LANES), lambda i, *_: (i, 0)),
                pl.BlockSpec((per, LANES), lambda i, *_: (i, 0)),
                whole(cam_blocks, 24, CB),
            ],
            out_specs=whole(2 * chunks, 3, point_blocks // chunks, LANES),
            scratch_shapes=[
                pltpu.VMEM((point_blocks * COARSE_ROWS, FINE), jnp.float32),
                pltpu.VMEM((point_blocks * 8, LANES), jnp.float32),
            ]
            + [
                pltpu.VMEM((count * PITCH, LANES), jnp.float32) for count in (9, 24, 24, 10, 10)
            ]
            * PAIRS,
        ),
        out_shape=jax.ShapeDtypeStruct((2 * chunks, 3, point_blocks // chunks, LANES), jnp.float32),
        compiler_params=params,
        name="couple",
    )(tile_block, tile_points, cam_jacobian, point_jacobian, oc, op, every)

    own_rows = point_blocks
    anywhere = pl.BlockSpec(memory_space=pl.ANY)
    smem = pl.BlockSpec(memory_space=pltpu.SMEM)
    seen = observed.reshape(2, rows, LANES).transpose(1, 0, 2).reshape(2 * rows, LANES)
    residual, point_table, sums = pl.pallas_call(
        functools.partial(finish_kernel, n_pts, n_cam),
        in_specs=[smem, smem, vmem, vmem] + [anywhere] * 6,
        out_specs=[vmem, vmem, vmem],
        out_shape=[
            jax.ShapeDtypeStruct((2 * rows, LANES), jnp.float32),
            jax.ShapeDtypeStruct((point_blocks * 8, LANES), jnp.float32),
            jax.ShapeDtypeStruct((1, LANES), jnp.float32),
        ],
        scratch_shapes=[
            pltpu.VMEM(planes.shape, jnp.float32),
            pltpu.VMEM((2, chunks, 3, own_rows // chunks, LANES), jnp.float32),
            pltpu.VMEM((3, own_rows * LANES), jnp.float32),
            pltpu.VMEM((3, own_rows * LANES), jnp.float32),
            pltpu.VMEM((9, own_rows * LANES), jnp.float32),
            pltpu.VMEM((15 * (own_rows + 1), LANES), jnp.float32),
            pltpu.VMEM((rows, LANES), jnp.int32),
            pltpu.VMEM((rows, LANES), jnp.int32),
            pltpu.VMEM((2 * rows, LANES), jnp.float32),
            pltpu.VMEM((10, rows, LANES), jnp.float32),
            pltpu.VMEM((n_pts * n_cam, LANES), jnp.float32),
            pltpu.SemaphoreType.DMA((6,)),
        ]
        + [pltpu.SemaphoreType.DMA((2, chunks))] * 4
        + dma_sems(n_pts * n_cam, n_pts * n_cam)
        + [pltpu.VMEM((10 * PITCH, LANES), jnp.float32)] * SPREAD,
        compiler_params=remote(1),
        name="finish",
    )(
        tile_block, tile_points, planes, cam_table, points, point_gradient,
        point_inverse, oc, op, seen,
    )
    residual, cost, accepted_points, accepted_cameras = pl.pallas_call(
        functools.partial(emit_kernel, 1.0 / (2.0 * obs_count * n_pts * n_cam)),
        in_specs=[smem] + [vmem] * 6,
        out_specs=[anywhere, smem, vmem, vmem],
        out_shape=[
            jax.ShapeDtypeStruct((2 * rows, LANES), jnp.float32),
            jax.ShapeDtypeStruct((1,), jnp.float32),
            jax.ShapeDtypeStruct(points.shape, jnp.float32),
            jax.ShapeDtypeStruct(cameras.shape, jnp.float32),
        ],
        scratch_shapes=[pltpu.SemaphoreType.DMA],
        compiler_params=pltpu.CompilerParams(vmem_limit_bytes=16 * 2**20),
        name="emit",
    )(accept.reshape(1), sums, residual, point_table, points, cameras, increment)
    residual = residual.reshape(rows, 2, LANES).transpose(1, 0, 2).reshape(2, obs_count)
    return residual, cost.reshape(()), accepted_points, accepted_cameras


def solution(mesh):
    in_specs = (
        P(None, ("pts", "cam")),
        P(None, ("pts", "cam")),
        P(None, "pts"),
        P(None, "pts"),
        P(None, "pts"),
        P(None, ("pts", "cam")),
        P(None, ("pts", "cam")),
        P(None, ("pts", "cam")),
        P(("pts", "cam")),
        P(("pts", "cam")),
        P(("pts", "cam")),
        P(("pts", "cam")),
        P(),
    )
    out_specs = (P(None, ("pts", "cam")), P(), P(None, "pts"), P(None, ("pts", "cam")))
    return jax.shard_map(
        on_device, mesh=mesh, in_specs=in_specs, out_specs=out_specs, check_vma=False
    )
```

```python
import functools
import math

import jax
import jax.numpy as jnp
from jax import lax
from jax.experimental import pallas as pl
from jax.experimental.pallas import tpu as pltpu
from jax.sharding import PartitionSpec as P

CB = 128
PB = 256
TILE = 256
LANES = 128
PITCH = 9
FINE = 64
FINE_BITS = 6
COARSE_ROWS = 32
PAIRS = 8
SPLIT = 2
TILES = 8
SPREAD = 32
CHUNKS = 16
LAG = 5
BLOCKS_PER_STEP = 256
MESH = pl.DeviceIdType.MESH


LANE_GATHER = lax.GatherDimensionNumbers(
    offset_dims=(),
    collapsed_slice_dims=(1,),
    start_index_map=(1,),
    operand_batching_dims=(0,),
    start_indices_batching_dims=(0,),
)


def lane_take(slab, index):
    return lax.gather(
        slab, index[:, :, None], LANE_GATHER, (1, 1), mode=lax.GatherScatterMode.PROMISE_IN_BOUNDS
    )


def couple_kernel(
    tile_block, tile_points, cam_jac, point_jac, obs_cam, obs_point, table, out, packed, *scratch
):
    step = pl.program_id(0)
    tiles_per_step = obs_cam.shape[0] // 2
    totals, scratch = scratch[:SPLIT], scratch[SPLIT:]
    buffers = [scratch[5 * u : 5 * u + 5] for u in range(PAIRS)]
    blocks = packed.shape[0] // 8

    @pl.when(step == 0)
    def _():
        for total in totals:
            total[...] = jnp.zeros_like(total)
        for _, _, _, low, high in buffers:
            low[...] = jnp.zeros_like(low)
            high[...] = jnp.zeros_like(high)

    wide = lax.broadcasted_iota(jnp.int32, (16, LANES), 0)
    fine = [(wide + 16 * k).astype(jnp.float32).astype(jnp.bfloat16) for k in range(FINE // 16)]
    half = (wide >= 8).astype(jnp.float32)
    coarse = [(half + 2.0 * k).astype(jnp.bfloat16) for k in range(PB // FINE // 2)]
    one = jnp.ones((16, LANES), jnp.bfloat16)
    zero = jnp.zeros((16, LANES), jnp.bfloat16)

    def twice(row):
        return jnp.broadcast_to(row, (16, LANES)).astype(jnp.bfloat16)

    def group(block, steps, *halves):
        jacs, sides = halves[:2], halves[2:]
        row = pl.multiple_of(block * 2 * TILES, 2 * TILES)
        tile = step * tiles_per_step + block * TILES
        for t in range(TILES):
            slab = table.at[tile_block[tile + t]]
            steps[pl.ds(t, 8, stride=PITCH), :] = slab[0:8, :]
            steps[pl.ds(8 * PITCH + t, 1), :] = slab[8:9, :]
            for h in range(2):
                lane = pl.ds(pl.multiple_of((row + 2 * t + h) * LANES, LANES), LANES)
                jac = cam_jac[:, lane].astype(jnp.float32)
                jacs[h][pl.ds(t, 8, stride=PITCH), :] = jac[0:8]
                jacs[h][pl.ds(8 * PITCH + t, 8, stride=PITCH), :] = jac[8:16]
                jacs[h][pl.ds(16 * PITCH + t, 2, stride=PITCH), :] = jac[16:18]
                jacs[h][pl.ds(18 * PITCH + t, 6, stride=PITCH), :] = point_jac[:, lane].astype(jnp.float32)
        sources = [steps[PITCH * m : PITCH * m + 8, :] for m in range(9)]
        for h in range(2):
            at = pl.ds(row + h, TILES, stride=2)
            index = obs_cam[at, :]
            moves = [lane_take(source, index) for source in sources]
            jac = [jacs[h][PITCH * m : PITCH * m + 8, :] for m in range(24)]
            first = sum((jac[m] * moves[m] for m in range(1, 9)), jac[0] * moves[0])
            second = sum((jac[9 + m] * moves[m] for m in range(1, 9)), jac[9] * moves[0])
            side = sides[h]
            for n in range(3):
                value = jac[18 + n] * first + jac[21 + n] * second
                head = value.astype(jnp.bfloat16).astype(jnp.float32)
                side[PITCH * n : PITCH * n + 8, :] = head
                side[PITCH * (n + 4) : PITCH * (n + 4) + 8, :] = value - head
            point = obs_point[at, :]
            side[PITCH * 8 : PITCH * 8 + 8, :] = (point & (FINE - 1)).astype(jnp.float32)
            side[PITCH * 9 : PITCH * 9 + 8, :] = (point >> FINE_BITS).astype(jnp.float32)
        for t in range(TILES):
            heads, hots = [], []
            for h in range(2):
                value = sides[h][pl.ds(t, 8, stride=PITCH), :]
                value = jnp.concatenate([value, value], axis=0).astype(jnp.bfloat16)
                low = twice(sides[h][pl.ds(8 * PITCH + t, 1), :])
                high = twice(sides[h][pl.ds(9 * PITCH + t, 1), :])
                heads.append(jnp.concatenate([jnp.where(k == high, value, zero) for k in coarse], axis=0))
                hots.append(jnp.concatenate([jnp.where(k == low, one, zero) for k in fine], axis=0))
            summed = lax.dot_general(
                jnp.concatenate(heads, axis=1),
                jnp.concatenate(hots, axis=1),
                (((1,), (1,)), ((), ())),
                preferred_element_type=jnp.float32,
            )
            place = pl.ds(pl.multiple_of(tile_points[tile + t] * COARSE_ROWS, COARSE_ROWS), COARSE_ROWS)
            total = totals[t % SPLIT]
            total[place, :] = total[place, :] + summed

    def turn(i, carry):
        for u in range(PAIRS):
            group(i * PAIRS + u, *buffers[u])
        return carry

    lax.fori_loop(0, obs_cam.shape[0] // (2 * TILES * PAIRS), turn, 0)

    @pl.when(step == pl.num_programs(0) - 1)
    def _():
        top = lax.broadcasted_iota(jnp.int32, (8, LANES), 0) < 4

        def fold(i, carry):
            for u in range(32):
                k = i * 32 + u
                base = pl.multiple_of(k * COARSE_ROWS, COARSE_ROWS)
                parts = [sum(total[pl.ds(base + 8 * j, 8), :] for total in totals) for j in range(4)]
                pair = [jnp.concatenate(parts[2 * j : 2 * j + 2], axis=1) for j in range(2)]
                pair = [value + pltpu.roll(value, 4, 0) for value in pair]
                packed[pl.ds(pl.multiple_of(k * 8, 8), 8), :] = jnp.where(top, *pair)
            return carry

        lax.fori_loop(0, blocks // 32, fold, 0)
        count = out.shape[2]
        for i in range(out.shape[0]):
            for n in range(3):
                out[i, n] = packed[pl.ds(4 * count * i + n, count, stride=4), :]


def camera_rows(trial):
    w = trial[0:3]
    angle = jnp.sqrt(w[0:1] * w[0:1] + w[1:2] * w[1:2] + w[2:3] * w[2:3])
    head = math.sqrt(2.0) * jnp.cos(0.5 * angle)
    still = angle == 0.0
    ratio = jnp.where(still, 0.5, jnp.sin(0.5 * angle) / jnp.where(still, 1.0, angle))
    tail = math.sqrt(2.0) * ratio * w
    return jnp.concatenate([head, tail, trial[3:9]], axis=0)


def greet(axis, size, me):
    barrier = pltpu.get_barrier_semaphore()
    for d in range(1, size):
        pl.semaphore_signal(
            barrier, inc=1, device_id={axis: lax.rem(me + d, size)}, device_id_type=MESH
        )


def send_round(axis, size, me, source, target, send, recv):
    copies = []
    for d in range(1, size):
        peer = lax.rem(me + d, size)
        copies.append(
            pltpu.make_async_remote_copy(
                src_ref=source(peer, d),
                dst_ref=target(peer, d),
                send_sem=send.at[d - 1],
                recv_sem=recv.at[d - 1],
                device_id={axis: peer},
                device_id_type=MESH,
            )
        )
    for copy in copies:
        copy.start()
    return copies


def gather_kernel(
    n_pts, n_cam, hbm_cameras, hbm_increment, out, cameras, increment, in_sem, send_cam, recv_cam, send_pts, recv_pts
):
    p, c = lax.axis_index("pts"), lax.axis_index("cam")
    loads = [
        pltpu.make_async_copy(source, target, in_sem.at[i])
        for i, (source, target) in enumerate(((hbm_cameras, cameras), (hbm_increment, increment)))
    ]
    for load in loads:
        load.start()
    greet("pts", n_pts, p)
    greet("cam", n_cam, c)
    count = cameras.shape[1] // CB
    base = (p * n_cam + c) * count
    for load in loads:
        load.wait()
    for i in range(count):
        lanes = slice(i * CB, (i + 1) * CB)
        move = increment[:, lanes]
        trial = cameras[:, lanes] + move
        out[base + i, 0:9, :] = move
        out[base + i, 9:19, :] = camera_rows(trial)
    pl.semaphore_wait(pltpu.get_barrier_semaphore(), n_pts + n_cam - 2)

    def blocks(j):
        owner = p * n_cam + lax.rem(c - j + n_cam, n_cam)
        return out.at[pl.ds(owner * count, count), 0:19]

    def forward(j):
        return send_round("pts", n_pts, p, lambda *_: blocks(j), lambda *_: blocks(j), send_pts.at[j], recv_pts.at[j])

    copies = send_round("cam", n_cam, c, lambda *_: blocks(0), lambda *_: blocks(0), send_cam, recv_cam)
    forwarded = forward(0)
    for j in sorted(range(1, n_cam), key=lambda j: min(j, n_cam - j)):
        copies[j - 1].wait_recv()
        forwarded += forward(j)
    for copy in copies:
        copy.wait_send()
    for copy in forwarded:
        copy.wait()


def finish_kernel(
    n_pts, n_cam, tile_block, tile_points, planes, cam_table, points, gradient, inverse, hbm_cam, hbm_point,
    hbm_seen, residual, point_table, sums, out, landed, own_points, own_gradient, own_inverse, work, obs_cam, obs_point,
    observed, cam_store, slots, in_sem, send_sum, recv_sum, send_out,
    recv_out, send_cost, recv_cost, *buffers,
):
    p, c = lax.axis_index("pts"), lax.axis_index("cam")
    streams = [
        pltpu.make_async_copy(source, target, in_sem.at[3 + i])
        for i, (source, target) in enumerate(
            ((hbm_cam, obs_cam), (hbm_point, obs_point), (hbm_seen, observed))
        )
    ]
    for stream in streams:
        stream.start()
    last = n_cam - 1
    chunks = landed.shape[1]
    count = planes.shape[2]
    rows = count * chunks
    span, pitch = rows * LANES, rows + 1
    low_end, high_end = c == 0, c == last
    at_end = jnp.logical_or(low_end, high_end)
    own_base = jnp.where(low_end, 0, rows)
    loads = [
        pltpu.make_async_copy(
            source.at[:, pl.ds(pl.multiple_of(own_base * LANES, LANES), span)], target, in_sem.at[i]
        )
        for i, (source, target) in enumerate(
            ((points, own_points), (gradient, own_gradient), (inverse, own_inverse))
        )
    ]

    @pl.when(at_end)
    def _():
        for load in loads:
            load.start()

    greet("pts", n_pts, p)
    barrier = pltpu.get_barrier_semaphore()

    def peer(step):
        return lax.rem(c + step + n_cam, n_cam)

    @pl.when(c > 0)
    def _():
        pl.semaphore_signal(barrier, inc=1, device_id={"cam": peer(-1)}, device_id_type=MESH)

    @pl.when(c < last)
    def _():
        pl.semaphore_signal(barrier, inc=1, device_id={"cam": peer(1)}, device_id_type=MESH)

    def take_cameras(i, carry):
        for u in range(SPREAD):
            block = i * SPREAD + u
            row = pl.multiple_of(block * 2 * TILES, 2 * TILES)
            buf = buffers[u]
            for t in range(TILES):
                slab = cam_table[tile_block[block * TILES + t]]
                buf[pl.ds(t, 8, stride=PITCH), :] = slab[0:8]
                buf[pl.ds(8 * PITCH + t, 2, stride=PITCH), :] = slab[8:10]
            sources = [buf[PITCH * m : PITCH * m + 8, :] for m in range(10)]
            for h in range(2):
                index = obs_cam[pl.ds(row + h, TILES, stride=2), :]
                for m in range(10):
                    cam_store[m, pl.ds(row + TILES * h, TILES), :] = lane_take(sources[m], index)
        return carry

    turns = obs_cam.shape[0] // (2 * TILES * SPREAD)
    early = turns // 4
    streams[0].wait()
    lax.fori_loop(0, early, take_cameras, 0)
    pl.semaphore_wait(barrier, n_pts - 1 + jnp.where(at_end, 1, 2))

    def place(way, k):
        return k + chunks if way == 0 else k

    def toward(way):
        return peer(1) if way == 0 else peer(-1)

    def sum_copy(way, k, source):
        return pltpu.make_async_remote_copy(
            src_ref=source,
            dst_ref=landed.at[way, k],
            send_sem=send_sum.at[way, k],
            recv_sem=recv_sum.at[way, k],
            device_id={"cam": toward(way)},
            device_id_type=MESH,
        )

    def out_copy(way, k):
        part = out.at[place(way, k)]
        return pltpu.make_async_remote_copy(
            src_ref=part,
            dst_ref=part,
            send_sem=send_out.at[way, k],
            recv_sem=recv_out.at[way, k],
            device_id={"cam": toward(1 - way)},
            device_id_type=MESH,
        )

    for way, first in ((0, low_end), (1, high_end)):

        @pl.when(first)
        def _(way=way):
            def begin(k, carry):
                sum_copy(way, k, planes.at[place(way, k)]).start()
                return carry

            lax.fori_loop(0, chunks, begin, 0)

    lax.fori_loop(early, turns, take_cameras, 0)

    @pl.when(at_end)
    def _():
        for load in loads:
            load.wait()

        def spread(i, carry):
            for u in range(8):
                k = i * 8 + u
                lanes = pl.ds(pl.multiple_of(k * LANES, LANES), LANES)
                work[pl.ds(k, 3, stride=pitch), :] = own_points[:, lanes]
                work[pl.ds(3 * pitch + k, 3, stride=pitch), :] = own_gradient[:, lanes]
                block = own_inverse[:, lanes]
                work[pl.ds(6 * pitch + k, 8, stride=pitch), :] = block[0:8]
                work[pl.ds(14 * pitch + k, 1), :] = block[8:9]
            return carry

        lax.fori_loop(0, rows // 8, spread, 0)

    def solved(way, k):
        def row(m):
            return work[pl.ds(m * pitch + k * count, count), :]

        total = landed[way, k] + planes[place(way, k)]
        residue = [row(3 + n) - total[n] for n in range(3)]
        for n in range(3):
            move = row(6 + 3 * n) * residue[0] + row(7 + 3 * n) * residue[1] + row(8 + 3 * n) * residue[2]
            out[place(way, k), n] = row(n) + move

    def turn(s, carry):
        for way, hops in ((0, c), (1, last - c)):
            k = s - LAG * hops
            live = jnp.logical_and(hops > 0, jnp.logical_and(k >= 0, k < chunks))

            @pl.when(live)
            def _(way=way, k=k, hops=hops):
                sum_copy(way, k, landed.at[way, k]).wait_recv()

                @pl.when(hops < last)
                def _():
                    landed[way, k] = landed[way, k] + planes[place(way, k)]
                    sum_copy(way, k, landed.at[way, k]).start()

                @pl.when(hops == last)
                def _():
                    solved(way, k)
                    out_copy(way, k).start()

        for way, hops in ((0, last - c), (1, c)):
            k = s - LAG * (last + hops)
            live = jnp.logical_and(hops > 0, jnp.logical_and(k >= 0, k < chunks))

            @pl.when(live)
            def _(way=way, k=k, hops=hops):
                out_copy(way, k).wait_recv()

                @pl.when(hops < last)
                def _():
                    out_copy(way, k).start()

        return carry

    lax.fori_loop(0, chunks + 2 * LAG * last, turn, 0)

    def finish(k, carry):
        for way, first, end in ((0, low_end, high_end), (1, high_end, low_end)):

            @pl.when(jnp.logical_not(end))
            def _(way=way):
                sum_copy(way, k, landed.at[way, k]).wait_send()

            @pl.when(jnp.logical_not(first))
            def _(way=way):
                out_copy(way, k).wait_send()

        return carry

    lax.fori_loop(0, chunks, finish, 0)
    point_table[...] = jnp.zeros_like(point_table)
    for i in range(2 * chunks):
        for n in range(3):
            point_table[pl.ds(4 * count * i + n, count, stride=4), :] = out[i, n]
    point_slabs = point_table.reshape(point_table.shape[0] // 8, 8, LANES)
    for stream in streams[1:]:
        stream.wait()

    def project(i, carry):
        for u in range(SPREAD):
            block = i * SPREAD + u
            row = pl.multiple_of(block * 2 * TILES, 2 * TILES)
            buf = buffers[u]
            for t in range(TILES):
                buf[pl.ds(t, 8, stride=PITCH), :] = point_slabs[tile_points[block * TILES + t]]
            sources = [buf[PITCH * m : PITCH * m + 8, :] for m in range(8)]
            for h in range(2):
                point = obs_point[pl.ds(row + h, TILES, stride=2), :]
                local = point & (LANES - 1)
                upper = point >= LANES
                x, y, z = (
                    jnp.where(upper, lane_take(sources[4 + n], local), lane_take(sources[n], local))
                    for n in range(3)
                )
                head, a, b, c, *shift, focal, k1, k2 = (
                    cam_store[m, pl.ds(row + TILES * h, TILES), :] for m in range(10)
                )
                e, f, g = b * z - c * y, c * x - a * z, a * y - b * x
                px = x + shift[0] + (head * e + (b * g - c * f))
                py = y + shift[1] + (head * f + (c * e - a * g))
                pz = z + shift[2] + (head * g + (a * f - b * e))
                scale = 1.0 / jnp.maximum(-pz, 1.0)
                fu, fv = px * scale, py * scale
                q = fu * fu + fv * fv
                factor = focal * (1.0 + q * (k1 + k2 * q))
                at_u = pl.ds(2 * (row + h), TILES, stride=4)
                at_v = pl.ds(2 * (row + h) + 1, TILES, stride=4)
                ru = factor * fu - observed[at_u, :]
                rv = factor * fv - observed[at_v, :]
                residual[at_u, :] = ru
                residual[at_v, :] = rv
                carry = carry + (ru * ru + rv * rv)
        return carry

    cost = lax.fori_loop(0, turns, project, jnp.zeros((8, LANES), jnp.float32))
    me = p * n_cam + c
    slots[pl.ds(me, 1), :] = jnp.sum(cost, axis=0, keepdims=True)
    mine = slots.at[pl.ds(me, 1)]
    copies = []
    for j in range(1, n_pts * n_cam):
        step_p, step_c = j // n_cam, j % n_cam
        copies.append(
            pltpu.make_async_remote_copy(
                src_ref=mine,
                dst_ref=mine,
                send_sem=send_cost.at[j],
                recv_sem=recv_cost.at[j],
                device_id={"pts": lax.rem(p + step_p, n_pts), "cam": lax.rem(c + step_c, n_cam)},
                device_id_type=MESH,
            )
        )
    for copy in copies:
        copy.start()
    for copy in copies:
        copy.wait()
    sums[...] = jnp.sum(slots[...], axis=0, keepdims=True)


def emit_kernel(
    scale, accept, sums, seen, table, points, cameras, increment, residual, cost, accepted_points, accepted_cameras, sem
):
    copy = pltpu.make_async_copy(seen, residual, sem)
    copy.start()
    odd = (accept[0] & 1) == 1
    accepted_cameras[...] = cameras[...] + odd.astype(jnp.float32) * increment[...]
    cost[0] = jnp.sum(sums[...]) * scale

    def turn(i, carry):
        for u in range(16):
            k = i * 16 + u
            lanes = pl.ds(pl.multiple_of(k * LANES, LANES), LANES)
            accepted_points[:, lanes] = jnp.where(odd, table[pl.ds(4 * k, 3), :], points[:, lanes])
        return carry

    lax.fori_loop(0, table.shape[0] // 64, turn, 0)
    copy.wait()


def on_device(
    cameras, increment, points, point_gradient, point_inverse, cam_jacobian, point_jacobian,
    observed, tile_block, tile_points, obs_camera, obs_point, accept,
):
    own_blocks = cameras.shape[1] // CB
    n_pts, n_cam = lax.axis_size("pts"), lax.axis_size("cam")
    vmem = pl.BlockSpec(memory_space=pltpu.VMEM)
    hbm = pl.BlockSpec(memory_space=pltpu.HBM)

    def dma_sems(*counts):
        return [pltpu.SemaphoreType.DMA((count,)) for count in counts]

    def remote(ident):
        return pltpu.CompilerParams(
            collective_id=ident, has_side_effects=True, vmem_limit_bytes=36 * 2**20
        )

    every = pl.pallas_call(
        functools.partial(gather_kernel, n_pts, n_cam),
        in_specs=[hbm, hbm],
        out_specs=vmem,
        out_shape=jax.ShapeDtypeStruct((own_blocks * n_pts * n_cam, 24, CB), jnp.float32),
        scratch_shapes=[pltpu.VMEM(cameras.shape, jnp.float32)] * 2
        + dma_sems(2, n_cam - 1, n_cam - 1)
        + [pltpu.SemaphoreType.DMA((n_cam, n_pts - 1))] * 2,
        compiler_params=remote(0),
        cost_estimate=pl.CostEstimate(flops=2**30, bytes_accessed=2**20, transcendentals=0),
        name="cameras",
    )(cameras, increment)
    cam_blocks = every.shape[0]
    cam_table = jnp.concatenate([every[:, 9:19], jnp.zeros((cam_blocks, 6, CB), jnp.float32)], axis=1)

    obs_count = obs_camera.shape[0]
    rows = obs_count // LANES
    per = math.gcd(rows, BLOCKS_PER_STEP)
    grid = (rows // per,)
    point_blocks = points.shape[1] // PB
    chunks = math.gcd(point_blocks // 8, CHUNKS)
    oc = obs_camera.reshape(rows, LANES)
    op = obs_point.reshape(rows, LANES)

    def whole(*shape):
        return pl.BlockSpec(shape, lambda i, *_: (0,) * len(shape))

    params = pltpu.CompilerParams(dimension_semantics=("arbitrary",), vmem_limit_bytes=50 * 2**20)
    planes = pl.pallas_call(
        couple_kernel,
        grid_spec=pltpu.PrefetchScalarGridSpec(
            num_scalar_prefetch=2,
            grid=grid,
            in_specs=[
                pl.BlockSpec((18, per * LANES), lambda i, *_: (0, i)),
                pl.BlockSpec((6, per * LANES), lambda i, *_: (0, i)),
                pl.BlockSpec((per, LANES), lambda i, *_: (i, 0)),
                pl.BlockSpec((per, LANES), lambda i, *_: (i, 0)),
                whole(cam_blocks, 24, CB),
            ],
            out_specs=whole(2 * chunks, 3, point_blocks // chunks, LANES),
            scratch_shapes=[
                pltpu.VMEM((point_blocks * 8, LANES), jnp.float32),
            ]
            + [pltpu.VMEM((point_blocks * COARSE_ROWS, FINE), jnp.float32)] * SPLIT
            + [
                pltpu.VMEM((count * PITCH, LANES), jnp.float32) for count in (9, 24, 24, 10, 10)
            ]
            * PAIRS,
        ),
        out_shape=jax.ShapeDtypeStruct((2 * chunks, 3, point_blocks // chunks, LANES), jnp.float32),
        compiler_params=params,
        name="couple",
    )(tile_block, tile_points, cam_jacobian, point_jacobian, oc, op, every)

    own_rows = point_blocks
    anywhere = pl.BlockSpec(memory_space=pl.ANY)
    smem = pl.BlockSpec(memory_space=pltpu.SMEM)
    seen = observed.reshape(2, rows, LANES).transpose(1, 0, 2).reshape(2 * rows, LANES)
    residual, point_table, sums = pl.pallas_call(
        functools.partial(finish_kernel, n_pts, n_cam),
        in_specs=[smem, smem, vmem, vmem] + [anywhere] * 6,
        out_specs=[vmem, vmem, vmem],
        out_shape=[
            jax.ShapeDtypeStruct((2 * rows, LANES), jnp.float32),
            jax.ShapeDtypeStruct((point_blocks * 8, LANES), jnp.float32),
            jax.ShapeDtypeStruct((1, LANES), jnp.float32),
        ],
        scratch_shapes=[
            pltpu.VMEM(planes.shape, jnp.float32),
            pltpu.VMEM((2, chunks, 3, own_rows // chunks, LANES), jnp.float32),
            pltpu.VMEM((3, own_rows * LANES), jnp.float32),
            pltpu.VMEM((3, own_rows * LANES), jnp.float32),
            pltpu.VMEM((9, own_rows * LANES), jnp.float32),
            pltpu.VMEM((15 * (own_rows + 1), LANES), jnp.float32),
            pltpu.VMEM((rows, LANES), jnp.int32),
            pltpu.VMEM((rows, LANES), jnp.int32),
            pltpu.VMEM((2 * rows, LANES), jnp.float32),
            pltpu.VMEM((10, rows, LANES), jnp.float32),
            pltpu.VMEM((n_pts * n_cam, LANES), jnp.float32),
            pltpu.SemaphoreType.DMA((6,)),
        ]
        + [pltpu.SemaphoreType.DMA((2, chunks))] * 4
        + dma_sems(n_pts * n_cam, n_pts * n_cam)
        + [pltpu.VMEM((10 * PITCH, LANES), jnp.float32)] * SPREAD,
        compiler_params=remote(1),
        name="finish",
    )(
        tile_block, tile_points, planes, cam_table, points, point_gradient,
        point_inverse, oc, op, seen,
    )
    residual, cost, accepted_points, accepted_cameras = pl.pallas_call(
        functools.partial(emit_kernel, 1.0 / (2.0 * obs_count * n_pts * n_cam)),
        in_specs=[smem] + [vmem] * 6,
        out_specs=[anywhere, smem, vmem, vmem],
        out_shape=[
            jax.ShapeDtypeStruct((2 * rows, LANES), jnp.float32),
            jax.ShapeDtypeStruct((1,), jnp.float32),
            jax.ShapeDtypeStruct(points.shape, jnp.float32),
            jax.ShapeDtypeStruct(cameras.shape, jnp.float32),
        ],
        scratch_shapes=[pltpu.SemaphoreType.DMA],
        compiler_params=pltpu.CompilerParams(vmem_limit_bytes=16 * 2**20),
        name="emit",
    )(accept.reshape(1), sums, residual, point_table, points, cameras, increment)
    residual = residual.reshape(rows, 2, LANES).transpose(1, 0, 2).reshape(2, obs_count)
    return residual, cost.reshape(()), accepted_points, accepted_cameras


def solution(mesh):
    in_specs = (
        P(None, ("pts", "cam")),
        P(None, ("pts", "cam")),
        P(None, "pts"),
        P(None, "pts"),
        P(None, "pts"),
        P(None, ("pts", "cam")),
        P(None, ("pts", "cam")),
        P(None, ("pts", "cam")),
        P(("pts", "cam")),
        P(("pts", "cam")),
        P(("pts", "cam")),
        P(("pts", "cam")),
        P(),
    )
    out_specs = (P(None, ("pts", "cam")), P(), P(None, "pts"), P(None, ("pts", "cam")))
    return jax.shard_map(
        on_device, mesh=mesh, in_specs=in_specs, out_specs=out_specs, check_vma=False
    )
```

```python
import functools
import math

import jax
import jax.numpy as jnp
from jax import lax
from jax.experimental import pallas as pl
from jax.experimental.pallas import tpu as pltpu
from jax.sharding import PartitionSpec as P

CB = 128
PB = 256
TILE = 256
LANES = 128
PITCH = 9
FINE = 64
FINE_BITS = 6
COARSE_ROWS = 32
PAIRS = 16
SPLIT = 2
TILES = 8
SPREAD = 32
CHUNKS = 16
LAG = 5
BLOCKS_PER_STEP = 256
MESH = pl.DeviceIdType.MESH


LANE_GATHER = lax.GatherDimensionNumbers(
    offset_dims=(),
    collapsed_slice_dims=(1,),
    start_index_map=(1,),
    operand_batching_dims=(0,),
    start_indices_batching_dims=(0,),
)


def lane_take(slab, index):
    return lax.gather(
        slab, index[:, :, None], LANE_GATHER, (1, 1), mode=lax.GatherScatterMode.PROMISE_IN_BOUNDS
    )


def couple_kernel(
    tile_block, tile_points, cam_jac, point_jac, obs_cam, obs_point, table, out, packed, *scratch
):
    step = pl.program_id(0)
    tiles_per_step = obs_cam.shape[0] // 2
    totals, scratch = scratch[:SPLIT], scratch[SPLIT:]
    buffers = [scratch[5 * u : 5 * u + 5] for u in range(PAIRS)]
    blocks = packed.shape[0] // 8

    @pl.when(step == 0)
    def _():
        for total in totals:
            total[...] = jnp.zeros_like(total)
        for _, _, _, low, high in buffers:
            low[...] = jnp.zeros_like(low)
            high[...] = jnp.zeros_like(high)

    wide = lax.broadcasted_iota(jnp.int32, (16, LANES), 0)
    fine = [(wide + 16 * k).astype(jnp.float32).astype(jnp.bfloat16) for k in range(FINE // 16)]
    half = (wide >= 8).astype(jnp.float32)
    coarse = [(half + 2.0 * k).astype(jnp.bfloat16) for k in range(PB // FINE // 2)]
    one = jnp.ones((16, LANES), jnp.bfloat16)
    zero = jnp.zeros((16, LANES), jnp.bfloat16)

    def twice(row):
        return jnp.broadcast_to(row, (16, LANES)).astype(jnp.bfloat16)

    def group(block, steps, *halves):
        jacs, sides = halves[:2], halves[2:]
        row = pl.multiple_of(block * 2 * TILES, 2 * TILES)
        tile = step * tiles_per_step + block * TILES
        for t in range(TILES):
            slab = table.at[tile_block[tile + t]]
            steps[pl.ds(t, 8, stride=PITCH), :] = slab[0:8, :]
            steps[pl.ds(8 * PITCH + t, 1), :] = slab[8:9, :]
            for h in range(2):
                lane = pl.ds(pl.multiple_of((row + 2 * t + h) * LANES, LANES), LANES)
                jac = cam_jac[:, lane].astype(jnp.float32)
                jacs[h][pl.ds(t, 8, stride=PITCH), :] = jac[0:8]
                jacs[h][pl.ds(8 * PITCH + t, 8, stride=PITCH), :] = jac[8:16]
                jacs[h][pl.ds(16 * PITCH + t, 2, stride=PITCH), :] = jac[16:18]
                jacs[h][pl.ds(18 * PITCH + t, 6, stride=PITCH), :] = point_jac[:, lane].astype(jnp.float32)
        sources = [steps[PITCH * m : PITCH * m + 8, :] for m in range(9)]
        for h in range(2):
            at = pl.ds(row + h, TILES, stride=2)
            index = obs_cam[at, :]
            moves = [lane_take(source, index) for source in sources]
            jac = [jacs[h][PITCH * m : PITCH * m + 8, :] for m in range(24)]
            first = sum((jac[m] * moves[m] for m in range(1, 9)), jac[0] * moves[0])
            second = sum((jac[9 + m] * moves[m] for m in range(1, 9)), jac[9] * moves[0])
            side = sides[h]
            for n in range(3):
                value = jac[18 + n] * first + jac[21 + n] * second
                head = value.astype(jnp.bfloat16).astype(jnp.float32)
                side[PITCH * n : PITCH * n + 8, :] = head
                side[PITCH * (n + 4) : PITCH * (n + 4) + 8, :] = value - head
            point = obs_point[at, :]
            side[PITCH * 8 : PITCH * 8 + 8, :] = (point & (FINE - 1)).astype(jnp.float32)
            side[PITCH * 9 : PITCH * 9 + 8, :] = (point >> FINE_BITS).astype(jnp.float32)
        for t in range(TILES):
            heads, hots = [], []
            for h in range(2):
                value = sides[h][pl.ds(t, 8, stride=PITCH), :]
                value = jnp.concatenate([value, value], axis=0).astype(jnp.bfloat16)
                low = twice(sides[h][pl.ds(8 * PITCH + t, 1), :])
                high = twice(sides[h][pl.ds(9 * PITCH + t, 1), :])
                heads.append(jnp.concatenate([jnp.where(k == high, value, zero) for k in coarse], axis=0))
                hots.append(jnp.concatenate([jnp.where(k == low, one, zero) for k in fine], axis=0))
            summed = lax.dot_general(
                jnp.concatenate(heads, axis=1),
                jnp.concatenate(hots, axis=1),
                (((1,), (1,)), ((), ())),
                preferred_element_type=jnp.float32,
            )
            place = pl.ds(pl.multiple_of(tile_points[tile + t] * COARSE_ROWS, COARSE_ROWS), COARSE_ROWS)
            total = totals[t % SPLIT]
            total[place, :] = total[place, :] + summed

    def turn(i, carry):
        for u in range(PAIRS):
            group(i * PAIRS + u, *buffers[u])
        return carry

    lax.fori_loop(0, obs_cam.shape[0] // (2 * TILES * PAIRS), turn, 0)

    @pl.when(step == pl.num_programs(0) - 1)
    def _():
        top = lax.broadcasted_iota(jnp.int32, (8, LANES), 0) < 4

        def fold(i, carry):
            for u in range(32):
                k = i * 32 + u
                base = pl.multiple_of(k * COARSE_ROWS, COARSE_ROWS)
                parts = [sum(total[pl.ds(base + 8 * j, 8), :] for total in totals) for j in range(4)]
                pair = [jnp.concatenate(parts[2 * j : 2 * j + 2], axis=1) for j in range(2)]
                pair = [value + pltpu.roll(value, 4, 0) for value in pair]
                packed[pl.ds(pl.multiple_of(k * 8, 8), 8), :] = jnp.where(top, *pair)
            return carry

        lax.fori_loop(0, blocks // 32, fold, 0)
        count = out.shape[2]
        for i in range(out.shape[0]):
            for n in range(3):
                out[i, n] = packed[pl.ds(4 * count * i + n, count, stride=4), :]


def camera_rows(trial):
    w = trial[0:3]
    angle = jnp.sqrt(w[0:1] * w[0:1] + w[1:2] * w[1:2] + w[2:3] * w[2:3])
    head = math.sqrt(2.0) * jnp.cos(0.5 * angle)
    still = angle == 0.0
    ratio = jnp.where(still, 0.5, jnp.sin(0.5 * angle) / jnp.where(still, 1.0, angle))
    tail = math.sqrt(2.0) * ratio * w
    return jnp.concatenate([head, tail, trial[3:9]], axis=0)


def greet(axis, size, me):
    barrier = pltpu.get_barrier_semaphore()
    for d in range(1, size):
        pl.semaphore_signal(
            barrier, inc=1, device_id={axis: lax.rem(me + d, size)}, device_id_type=MESH
        )


def send_round(axis, size, me, source, target, send, recv):
    copies = []
    for d in range(1, size):
        peer = lax.rem(me + d, size)
        copies.append(
            pltpu.make_async_remote_copy(
                src_ref=source(peer, d),
                dst_ref=target(peer, d),
                send_sem=send.at[d - 1],
                recv_sem=recv.at[d - 1],
                device_id={axis: peer},
                device_id_type=MESH,
            )
        )
    for copy in copies:
        copy.start()
    return copies


def gather_kernel(n_pts, n_cam, own, out, send_cam, recv_cam, send_pts, recv_pts):
    p, c = lax.axis_index("pts"), lax.axis_index("cam")
    greet("pts", n_pts, p)
    greet("cam", n_cam, c)
    count = own.shape[2] // CB
    base = (p * n_cam + c) * count
    for i in range(count):
        lanes = slice(i * CB, (i + 1) * CB)
        move = own[1, :, lanes]
        trial = own[0, :, lanes] + move
        out[base + i, 0:9, :] = move
        out[base + i, 9:19, :] = camera_rows(trial)
    pl.semaphore_wait(pltpu.get_barrier_semaphore(), n_pts + n_cam - 2)

    def blocks(j):
        owner = p * n_cam + lax.rem(c - j + n_cam, n_cam)
        return out.at[pl.ds(owner * count, count), 0:19]

    def forward(j):
        return send_round("pts", n_pts, p, lambda *_: blocks(j), lambda *_: blocks(j), send_pts.at[j], recv_pts.at[j])

    copies = send_round("cam", n_cam, c, lambda *_: blocks(0), lambda *_: blocks(0), send_cam, recv_cam)
    forwarded = forward(0)
    for j in sorted(range(1, n_cam), key=lambda j: min(j, n_cam - j)):
        copies[j - 1].wait_recv()
        forwarded += forward(j)
    for copy in copies:
        copy.wait_send()
    for copy in forwarded:
        copy.wait()


def finish_kernel(
    n_pts, n_cam, tile_block, tile_points, planes, cam_table, points, gradient, inverse, hbm_cam, hbm_point,
    hbm_seen, residual, point_table, sums, out, landed, own_points, own_gradient, own_inverse, work, obs_cam, obs_point,
    observed, cam_store, slots, in_sem, send_sum, recv_sum, send_out,
    recv_out, send_cost, recv_cost, *buffers,
):
    p, c = lax.axis_index("pts"), lax.axis_index("cam")
    streams = [
        pltpu.make_async_copy(source, target, in_sem.at[3 + i])
        for i, (source, target) in enumerate(
            ((hbm_cam, obs_cam), (hbm_point, obs_point), (hbm_seen, observed))
        )
    ]
    for stream in streams:
        stream.start()
    last = n_cam - 1
    chunks = landed.shape[1]
    count = planes.shape[2]
    rows = count * chunks
    span, pitch = rows * LANES, rows + 1
    low_end, high_end = c == 0, c == last
    at_end = jnp.logical_or(low_end, high_end)
    own_base = jnp.where(low_end, 0, rows)
    loads = [
        pltpu.make_async_copy(
            source.at[:, pl.ds(pl.multiple_of(own_base * LANES, LANES), span)], target, in_sem.at[i]
        )
        for i, (source, target) in enumerate(
            ((points, own_points), (gradient, own_gradient), (inverse, own_inverse))
        )
    ]

    @pl.when(at_end)
    def _():
        for load in loads:
            load.start()

    greet("pts", n_pts, p)
    barrier = pltpu.get_barrier_semaphore()

    def peer(step):
        return lax.rem(c + step + n_cam, n_cam)

    @pl.when(c > 0)
    def _():
        pl.semaphore_signal(barrier, inc=1, device_id={"cam": peer(-1)}, device_id_type=MESH)

    @pl.when(c < last)
    def _():
        pl.semaphore_signal(barrier, inc=1, device_id={"cam": peer(1)}, device_id_type=MESH)

    def take_cameras(i, carry):
        for u in range(SPREAD):
            block = i * SPREAD + u
            row = pl.multiple_of(block * 2 * TILES, 2 * TILES)
            buf = buffers[u]
            for t in range(TILES):
                slab = cam_table[tile_block[block * TILES + t]]
                buf[pl.ds(t, 8, stride=PITCH), :] = slab[0:8]
                buf[pl.ds(8 * PITCH + t, 2, stride=PITCH), :] = slab[8:10]
            sources = [buf[PITCH * m : PITCH * m + 8, :] for m in range(10)]
            for h in range(2):
                index = obs_cam[pl.ds(row + h, TILES, stride=2), :]
                for m in range(10):
                    cam_store[m, pl.ds(row + TILES * h, TILES), :] = lane_take(sources[m], index)
        return carry

    turns = obs_cam.shape[0] // (2 * TILES * SPREAD)
    early = turns // 4
    streams[0].wait()
    lax.fori_loop(0, early, take_cameras, 0)
    pl.semaphore_wait(barrier, n_pts - 1 + jnp.where(at_end, 1, 2))

    def place(way, k):
        return k + chunks if way == 0 else k

    def toward(way):
        return peer(1) if way == 0 else peer(-1)

    def sum_copy(way, k, source):
        return pltpu.make_async_remote_copy(
            src_ref=source,
            dst_ref=landed.at[way, k],
            send_sem=send_sum.at[way, k],
            recv_sem=recv_sum.at[way, k],
            device_id={"cam": toward(way)},
            device_id_type=MESH,
        )

    def out_copy(way, k):
        part = out.at[place(way, k)]
        return pltpu.make_async_remote_copy(
            src_ref=part,
            dst_ref=part,
            send_sem=send_out.at[way, k],
            recv_sem=recv_out.at[way, k],
            device_id={"cam": toward(1 - way)},
            device_id_type=MESH,
        )

    for way, first in ((0, low_end), (1, high_end)):

        @pl.when(first)
        def _(way=way):
            def begin(k, carry):
                sum_copy(way, k, planes.at[place(way, k)]).start()
                return carry

            lax.fori_loop(0, chunks, begin, 0)

    lax.fori_loop(early, turns, take_cameras, 0)

    @pl.when(at_end)
    def _():
        for load in loads:
            load.wait()

        def spread(i, carry):
            for u in range(8):
                k = i * 8 + u
                lanes = pl.ds(pl.multiple_of(k * LANES, LANES), LANES)
                work[pl.ds(k, 3, stride=pitch), :] = own_points[:, lanes]
                work[pl.ds(3 * pitch + k, 3, stride=pitch), :] = own_gradient[:, lanes]
                block = own_inverse[:, lanes]
                work[pl.ds(6 * pitch + k, 8, stride=pitch), :] = block[0:8]
                work[pl.ds(14 * pitch + k, 1), :] = block[8:9]
            return carry

        lax.fori_loop(0, rows // 8, spread, 0)

    def solved(way, k):
        def row(m):
            return work[pl.ds(m * pitch + k * count, count), :]

        total = landed[way, k] + planes[place(way, k)]
        residue = [row(3 + n) - total[n] for n in range(3)]
        for n in range(3):
            move = row(6 + 3 * n) * residue[0] + row(7 + 3 * n) * residue[1] + row(8 + 3 * n) * residue[2]
            out[place(way, k), n] = row(n) + move

    def turn(s, carry):
        for way, hops in ((0, c), (1, last - c)):
            k = s - LAG * hops
            live = jnp.logical_and(hops > 0, jnp.logical_and(k >= 0, k < chunks))

            @pl.when(live)
            def _(way=way, k=k, hops=hops):
                sum_copy(way, k, landed.at[way, k]).wait_recv()

                @pl.when(hops < last)
                def _():
                    landed[way, k] = landed[way, k] + planes[place(way, k)]
                    sum_copy(way, k, landed.at[way, k]).start()

                @pl.when(hops == last)
                def _():
                    solved(way, k)
                    out_copy(way, k).start()

        for way, hops in ((0, last - c), (1, c)):
            k = s - LAG * (last + hops)
            live = jnp.logical_and(hops > 0, jnp.logical_and(k >= 0, k < chunks))

            @pl.when(live)
            def _(way=way, k=k, hops=hops):
                out_copy(way, k).wait_recv()

                @pl.when(hops < last)
                def _():
                    out_copy(way, k).start()

        return carry

    lax.fori_loop(0, chunks + 2 * LAG * last, turn, 0)

    def finish(k, carry):
        for way, first, end in ((0, low_end, high_end), (1, high_end, low_end)):

            @pl.when(jnp.logical_not(end))
            def _(way=way):
                sum_copy(way, k, landed.at[way, k]).wait_send()

            @pl.when(jnp.logical_not(first))
            def _(way=way):
                out_copy(way, k).wait_send()

        return carry

    lax.fori_loop(0, chunks, finish, 0)
    point_table[...] = jnp.zeros_like(point_table)
    for i in range(2 * chunks):
        for n in range(3):
            point_table[pl.ds(4 * count * i + n, count, stride=4), :] = out[i, n]
    point_slabs = point_table.reshape(point_table.shape[0] // 8, 8, LANES)
    for stream in streams[1:]:
        stream.wait()

    def project(i, carry):
        for u in range(SPREAD):
            block = i * SPREAD + u
            row = pl.multiple_of(block * 2 * TILES, 2 * TILES)
            buf = buffers[u]
            for t in range(TILES):
                buf[pl.ds(t, 8, stride=PITCH), :] = point_slabs[tile_points[block * TILES + t]]
            sources = [buf[PITCH * m : PITCH * m + 8, :] for m in range(8)]
            for h in range(2):
                point = obs_point[pl.ds(row + h, TILES, stride=2), :]
                local = point & (LANES - 1)
                upper = point >= LANES
                x, y, z = (
                    jnp.where(upper, lane_take(sources[4 + n], local), lane_take(sources[n], local))
                    for n in range(3)
                )
                head, a, b, c, *shift, focal, k1, k2 = (
                    cam_store[m, pl.ds(row + TILES * h, TILES), :] for m in range(10)
                )
                e, f, g = b * z - c * y, c * x - a * z, a * y - b * x
                px = x + shift[0] + (head * e + (b * g - c * f))
                py = y + shift[1] + (head * f + (c * e - a * g))
                pz = z + shift[2] + (head * g + (a * f - b * e))
                scale = 1.0 / jnp.maximum(-pz, 1.0)
                fu, fv = px * scale, py * scale
                q = fu * fu + fv * fv
                factor = focal * (1.0 + q * (k1 + k2 * q))
                at_u = pl.ds(2 * (row + h), TILES, stride=4)
                at_v = pl.ds(2 * (row + h) + 1, TILES, stride=4)
                ru = factor * fu - observed[at_u, :]
                rv = factor * fv - observed[at_v, :]
                residual[at_u, :] = ru
                residual[at_v, :] = rv
                carry = carry + (ru * ru + rv * rv)
        return carry

    cost = lax.fori_loop(0, turns, project, jnp.zeros((8, LANES), jnp.float32))
    me = p * n_cam + c
    slots[pl.ds(me, 1), :] = jnp.sum(cost, axis=0, keepdims=True)
    mine = slots.at[pl.ds(me, 1)]
    copies = []
    for j in range(1, n_pts * n_cam):
        step_p, step_c = j // n_cam, j % n_cam
        copies.append(
            pltpu.make_async_remote_copy(
                src_ref=mine,
                dst_ref=mine,
                send_sem=send_cost.at[j],
                recv_sem=recv_cost.at[j],
                device_id={"pts": lax.rem(p + step_p, n_pts), "cam": lax.rem(c + step_c, n_cam)},
                device_id_type=MESH,
            )
        )
    for copy in copies:
        copy.start()
    for copy in copies:
        copy.wait()
    sums[...] = jnp.sum(slots[...], axis=0, keepdims=True)


def emit_kernel(
    scale, accept, sums, seen, table, points, cameras, increment, residual, cost, accepted_points, accepted_cameras, sem
):
    copy = pltpu.make_async_copy(seen, residual, sem)
    copy.start()
    odd = (accept[0] & 1) == 1
    accepted_cameras[...] = cameras[...] + odd.astype(jnp.float32) * increment[...]
    cost[0] = jnp.sum(sums[...]) * scale

    def turn(i, carry):
        for u in range(16):
            k = i * 16 + u
            lanes = pl.ds(pl.multiple_of(k * LANES, LANES), LANES)
            accepted_points[:, lanes] = jnp.where(odd, table[pl.ds(4 * k, 3), :], points[:, lanes])
        return carry

    lax.fori_loop(0, table.shape[0] // 64, turn, 0)
    copy.wait()


def on_device(
    cameras, increment, points, point_gradient, point_inverse, cam_jacobian, point_jacobian,
    observed, tile_block, tile_points, obs_camera, obs_point, accept,
):
    own_blocks = cameras.shape[1] // CB
    n_pts, n_cam = lax.axis_size("pts"), lax.axis_size("cam")
    vmem = pl.BlockSpec(memory_space=pltpu.VMEM)
    hbm = pl.BlockSpec(memory_space=pltpu.HBM)

    def dma_sems(*counts):
        return [pltpu.SemaphoreType.DMA((count,)) for count in counts]

    def remote(ident):
        return pltpu.CompilerParams(
            collective_id=ident, has_side_effects=True, vmem_limit_bytes=36 * 2**20
        )

    every = pl.pallas_call(
        functools.partial(gather_kernel, n_pts, n_cam),
        in_specs=[vmem],
        out_specs=vmem,
        out_shape=jax.ShapeDtypeStruct((own_blocks * n_pts * n_cam, 24, CB), jnp.float32),
        scratch_shapes=dma_sems(n_cam - 1, n_cam - 1)
        + [pltpu.SemaphoreType.DMA((n_cam, n_pts - 1))] * 2,
        compiler_params=remote(0),
        cost_estimate=pl.CostEstimate(flops=2**30, bytes_accessed=2**20, transcendentals=0),
        name="cameras",
    )(jnp.stack([cameras, increment]))
    cam_blocks = every.shape[0]
    cam_table = jnp.concatenate([every[:, 9:19], jnp.zeros((cam_blocks, 6, CB), jnp.float32)], axis=1)

    obs_count = obs_camera.shape[0]
    rows = obs_count // LANES
    per = math.gcd(rows, BLOCKS_PER_STEP)
    grid = (rows // per,)
    point_blocks = points.shape[1] // PB
    chunks = math.gcd(point_blocks // 8, CHUNKS)
    oc = obs_camera.reshape(rows, LANES)
    op = obs_point.reshape(rows, LANES)

    def whole(*shape):
        return pl.BlockSpec(shape, lambda i, *_: (0,) * len(shape))

    params = pltpu.CompilerParams(dimension_semantics=("arbitrary",), vmem_limit_bytes=50 * 2**20)
    planes = pl.pallas_call(
        couple_kernel,
        grid_spec=pltpu.PrefetchScalarGridSpec(
            num_scalar_prefetch=2,
            grid=grid,
            in_specs=[
                pl.BlockSpec((18, per * LANES), lambda i, *_: (0, i)),
                pl.BlockSpec((6, per * LANES), lambda i, *_: (0, i)),
                pl.BlockSpec((per, LANES), lambda i, *_: (i, 0)),
                pl.BlockSpec((per, LANES), lambda i, *_: (i, 0)),
                whole(cam_blocks, 24, CB),
            ],
            out_specs=whole(2 * chunks, 3, point_blocks // chunks, LANES),
            scratch_shapes=[
                pltpu.VMEM((point_blocks * 8, LANES), jnp.float32),
            ]
            + [pltpu.VMEM((point_blocks * COARSE_ROWS, FINE), jnp.float32)] * SPLIT
            + [
                pltpu.VMEM((count * PITCH, LANES), jnp.float32) for count in (9, 24, 24, 10, 10)
            ]
            * PAIRS,
        ),
        out_shape=jax.ShapeDtypeStruct((2 * chunks, 3, point_blocks // chunks, LANES), jnp.float32),
        compiler_params=params,
        name="couple",
    )(tile_block, tile_points, cam_jacobian, point_jacobian, oc, op, every)

    own_rows = point_blocks
    anywhere = pl.BlockSpec(memory_space=pl.ANY)
    smem = pl.BlockSpec(memory_space=pltpu.SMEM)
    seen = observed.reshape(2, rows, LANES).transpose(1, 0, 2).reshape(2 * rows, LANES)
    residual, point_table, sums = pl.pallas_call(
        functools.partial(finish_kernel, n_pts, n_cam),
        in_specs=[smem, smem, vmem, vmem] + [anywhere] * 6,
        out_specs=[vmem, vmem, vmem],
        out_shape=[
            jax.ShapeDtypeStruct((2 * rows, LANES), jnp.float32),
            jax.ShapeDtypeStruct((point_blocks * 8, LANES), jnp.float32),
            jax.ShapeDtypeStruct((1, LANES), jnp.float32),
        ],
        scratch_shapes=[
            pltpu.VMEM(planes.shape, jnp.float32),
            pltpu.VMEM((2, chunks, 3, own_rows // chunks, LANES), jnp.float32),
            pltpu.VMEM((3, own_rows * LANES), jnp.float32),
            pltpu.VMEM((3, own_rows * LANES), jnp.float32),
            pltpu.VMEM((9, own_rows * LANES), jnp.float32),
            pltpu.VMEM((15 * (own_rows + 1), LANES), jnp.float32),
            pltpu.VMEM((rows, LANES), jnp.int32),
            pltpu.VMEM((rows, LANES), jnp.int32),
            pltpu.VMEM((2 * rows, LANES), jnp.float32),
            pltpu.VMEM((10, rows, LANES), jnp.float32),
            pltpu.VMEM((n_pts * n_cam, LANES), jnp.float32),
            pltpu.SemaphoreType.DMA((6,)),
        ]
        + [pltpu.SemaphoreType.DMA((2, chunks))] * 4
        + dma_sems(n_pts * n_cam, n_pts * n_cam)
        + [pltpu.VMEM((10 * PITCH, LANES), jnp.float32)] * SPREAD,
        compiler_params=remote(1),
        name="finish",
    )(
        tile_block, tile_points, planes, cam_table, points, point_gradient,
        point_inverse, oc, op, seen,
    )
    residual, cost, accepted_points, accepted_cameras = pl.pallas_call(
        functools.partial(emit_kernel, 1.0 / (2.0 * obs_count * n_pts * n_cam)),
        in_specs=[smem] + [vmem] * 6,
        out_specs=[anywhere, smem, vmem, vmem],
        out_shape=[
            jax.ShapeDtypeStruct((2 * rows, LANES), jnp.float32),
            jax.ShapeDtypeStruct((1,), jnp.float32),
            jax.ShapeDtypeStruct(points.shape, jnp.float32),
            jax.ShapeDtypeStruct(cameras.shape, jnp.float32),
        ],
        scratch_shapes=[pltpu.SemaphoreType.DMA],
        compiler_params=pltpu.CompilerParams(vmem_limit_bytes=16 * 2**20),
        name="emit",
    )(accept.reshape(1), sums, residual, point_table, points, cameras, increment)
    residual = residual.reshape(rows, 2, LANES).transpose(1, 0, 2).reshape(2, obs_count)
    return residual, cost.reshape(()), accepted_points, accepted_cameras


def solution(mesh):
    in_specs = (
        P(None, ("pts", "cam")),
        P(None, ("pts", "cam")),
        P(None, "pts"),
        P(None, "pts"),
        P(None, "pts"),
        P(None, ("pts", "cam")),
        P(None, ("pts", "cam")),
        P(None, ("pts", "cam")),
        P(("pts", "cam")),
        P(("pts", "cam")),
        P(("pts", "cam")),
        P(("pts", "cam")),
        P(),
    )
    out_specs = (P(None, ("pts", "cam")), P(), P(None, "pts"), P(None, ("pts", "cam")))
    return jax.shard_map(
        on_device, mesh=mesh, in_specs=in_specs, out_specs=out_specs, check_vma=False
    )
```

```python
import functools
import math

import jax
import jax.numpy as jnp
from jax import lax
from jax.experimental import pallas as pl
from jax.experimental.pallas import tpu as pltpu
from jax.sharding import PartitionSpec as P

CB = 128
PB = 256
TILE = 256
LANES = 128
PITCH = 9
FINE = 64
FINE_BITS = 6
COARSE_ROWS = 32
PAIRS = 16
SPLIT = 2
TILES = 8
SPREAD = 32
CHUNKS = 16
LAG = 5
BLOCKS_PER_STEP = 256
MESH = pl.DeviceIdType.MESH


LANE_GATHER = lax.GatherDimensionNumbers(
    offset_dims=(),
    collapsed_slice_dims=(1,),
    start_index_map=(1,),
    operand_batching_dims=(0,),
    start_indices_batching_dims=(0,),
)


def lane_take(slab, index):
    return lax.gather(
        slab, index[:, :, None], LANE_GATHER, (1, 1), mode=lax.GatherScatterMode.PROMISE_IN_BOUNDS
    )


def couple_kernel(
    tile_block, tile_points, cam_jac, point_jac, obs_cam, obs_point, table, out, packed, *scratch
):
    step = pl.program_id(0)
    tiles_per_step = obs_cam.shape[0] // 2
    totals, scratch = scratch[:SPLIT], scratch[SPLIT:]
    buffers = [scratch[5 * u : 5 * u + 5] for u in range(PAIRS)]
    blocks = packed.shape[0] // 8

    @pl.when(step == 0)
    def _():
        for total in totals:
            total[...] = jnp.zeros_like(total)
        for _, _, _, low, high in buffers:
            low[...] = jnp.zeros_like(low)
            high[...] = jnp.zeros_like(high)

    wide = lax.broadcasted_iota(jnp.int32, (16, LANES), 0)
    fine = [(wide + 16 * k).astype(jnp.float32).astype(jnp.bfloat16) for k in range(FINE // 16)]
    half = (wide >= 8).astype(jnp.float32)
    coarse = [(half + 2.0 * k).astype(jnp.bfloat16) for k in range(PB // FINE // 2)]
    one = jnp.ones((16, LANES), jnp.bfloat16)
    zero = jnp.zeros((16, LANES), jnp.bfloat16)

    def twice(row):
        return jnp.broadcast_to(row, (16, LANES)).astype(jnp.bfloat16)

    def group(block, steps, *halves):
        jacs, sides = halves[:2], halves[2:]
        row = pl.multiple_of(block * 2 * TILES, 2 * TILES)
        tile = step * tiles_per_step + block * TILES
        for t in range(TILES):
            slab = table.at[tile_block[tile + t]]
            steps[pl.ds(t, 8, stride=PITCH), :] = slab[0:8, :]
            steps[pl.ds(8 * PITCH + t, 1), :] = slab[8:9, :]
            for h in range(2):
                lane = pl.ds(pl.multiple_of((row + 2 * t + h) * LANES, LANES), LANES)
                jac = cam_jac[:, lane].astype(jnp.float32)
                jacs[h][pl.ds(t, 8, stride=PITCH), :] = jac[0:8]
                jacs[h][pl.ds(8 * PITCH + t, 8, stride=PITCH), :] = jac[8:16]
                jacs[h][pl.ds(16 * PITCH + t, 2, stride=PITCH), :] = jac[16:18]
                jacs[h][pl.ds(18 * PITCH + t, 6, stride=PITCH), :] = point_jac[:, lane].astype(jnp.float32)
        sources = [steps[PITCH * m : PITCH * m + 8, :] for m in range(9)]
        for h in range(2):
            at = pl.ds(row + h, TILES, stride=2)
            index = obs_cam[at, :]
            moves = [lane_take(source, index) for source in sources]
            jac = [jacs[h][PITCH * m : PITCH * m + 8, :] for m in range(24)]
            first = sum((jac[m] * moves[m] for m in range(1, 9)), jac[0] * moves[0])
            second = sum((jac[9 + m] * moves[m] for m in range(1, 9)), jac[9] * moves[0])
            side = sides[h]
            for n in range(3):
                value = jac[18 + n] * first + jac[21 + n] * second
                head = value.astype(jnp.bfloat16).astype(jnp.float32)
                side[PITCH * n : PITCH * n + 8, :] = head
                side[PITCH * (n + 4) : PITCH * (n + 4) + 8, :] = value - head
            point = obs_point[at, :]
            side[PITCH * 8 : PITCH * 8 + 8, :] = (point & (FINE - 1)).astype(jnp.float32)
            side[PITCH * 9 : PITCH * 9 + 8, :] = (point >> FINE_BITS).astype(jnp.float32)
        for t in range(TILES):
            heads, hots = [], []
            for h in range(2):
                value = sides[h][pl.ds(t, 8, stride=PITCH), :]
                value = jnp.concatenate([value, value], axis=0).astype(jnp.bfloat16)
                low = twice(sides[h][pl.ds(8 * PITCH + t, 1), :])
                high = twice(sides[h][pl.ds(9 * PITCH + t, 1), :])
                heads.append(jnp.concatenate([jnp.where(k == high, value, zero) for k in coarse], axis=0))
                hots.append(jnp.concatenate([jnp.where(k == low, one, zero) for k in fine], axis=0))
            summed = lax.dot_general(
                jnp.concatenate(heads, axis=1),
                jnp.concatenate(hots, axis=1),
                (((1,), (1,)), ((), ())),
                preferred_element_type=jnp.float32,
            )
            place = pl.ds(pl.multiple_of(tile_points[tile + t] * COARSE_ROWS, COARSE_ROWS), COARSE_ROWS)
            total = totals[t % SPLIT]
            total[place, :] = total[place, :] + summed

    def turn(i, carry):
        for u in range(PAIRS):
            group(i * PAIRS + u, *buffers[u])
        return carry

    lax.fori_loop(0, obs_cam.shape[0] // (2 * TILES * PAIRS), turn, 0)

    @pl.when(step == pl.num_programs(0) - 1)
    def _():
        top = lax.broadcasted_iota(jnp.int32, (8, LANES), 0) < 4

        def fold(i, carry):
            for u in range(64):
                k = i * 64 + u
                base = pl.multiple_of(k * COARSE_ROWS, COARSE_ROWS)
                parts = [sum(total[pl.ds(base + 8 * j, 8), :] for total in totals) for j in range(4)]
                pair = [jnp.concatenate(parts[2 * j : 2 * j + 2], axis=1) for j in range(2)]
                pair = [value + pltpu.roll(value, 4, 0) for value in pair]
                packed[pl.ds(pl.multiple_of(k * 8, 8), 8), :] = jnp.where(top, *pair)
            return carry

        lax.fori_loop(0, blocks // 64, fold, 0)
        count = out.shape[2]
        for i in range(out.shape[0]):
            for n in range(3):
                out[i, n] = packed[pl.ds(4 * count * i + n, count, stride=4), :]


def camera_rows(trial):
    w = trial[0:3]
    angle = jnp.sqrt(w[0:1] * w[0:1] + w[1:2] * w[1:2] + w[2:3] * w[2:3])
    head = math.sqrt(2.0) * jnp.cos(0.5 * angle)
    still = angle == 0.0
    ratio = jnp.where(still, 0.5, jnp.sin(0.5 * angle) / jnp.where(still, 1.0, angle))
    tail = math.sqrt(2.0) * ratio * w
    return jnp.concatenate([head, tail, trial[3:9]], axis=0)


def greet(axis, size, me):
    barrier = pltpu.get_barrier_semaphore()
    for d in range(1, size):
        pl.semaphore_signal(
            barrier, inc=1, device_id={axis: lax.rem(me + d, size)}, device_id_type=MESH
        )


def send_round(axis, size, me, source, target, send, recv):
    copies = []
    for d in range(1, size):
        peer = lax.rem(me + d, size)
        copies.append(
            pltpu.make_async_remote_copy(
                src_ref=source(peer, d),
                dst_ref=target(peer, d),
                send_sem=send.at[d - 1],
                recv_sem=recv.at[d - 1],
                device_id={axis: peer},
                device_id_type=MESH,
            )
        )
    for copy in copies:
        copy.start()
    return copies


def gather_kernel(n_pts, n_cam, own, out, send_cam, recv_cam, send_pts, recv_pts):
    p, c = lax.axis_index("pts"), lax.axis_index("cam")
    greet("pts", n_pts, p)
    greet("cam", n_cam, c)
    count = own.shape[2] // CB
    base = (p * n_cam + c) * count
    for i in range(count):
        lanes = slice(i * CB, (i + 1) * CB)
        move = own[1, :, lanes]
        trial = own[0, :, lanes] + move
        out[base + i, 0:9, :] = move
        out[base + i, 9:19, :] = camera_rows(trial)
    pl.semaphore_wait(pltpu.get_barrier_semaphore(), n_pts + n_cam - 2)

    def blocks(j):
        owner = p * n_cam + lax.rem(c - j + n_cam, n_cam)
        return out.at[pl.ds(owner * count, count), 0:19]

    def forward(j):
        return send_round("pts", n_pts, p, lambda *_: blocks(j), lambda *_: blocks(j), send_pts.at[j], recv_pts.at[j])

    copies = send_round("cam", n_cam, c, lambda *_: blocks(0), lambda *_: blocks(0), send_cam, recv_cam)
    forwarded = forward(0)
    for j in sorted(range(1, n_cam), key=lambda j: min(j, n_cam - j)):
        copies[j - 1].wait_recv()
        forwarded += forward(j)
    for copy in copies:
        copy.wait_send()
    for copy in forwarded:
        copy.wait()


def finish_kernel(
    n_pts, n_cam, tile_block, tile_points, planes, cam_table, points, gradient, inverse, hbm_cam, hbm_point,
    hbm_seen, residual, point_table, sums, out, landed, own_points, own_gradient, own_inverse, work, obs_cam, obs_point,
    observed, cam_store, slots, in_sem, send_sum, recv_sum, send_out,
    recv_out, send_cost, recv_cost, *buffers,
):
    p, c = lax.axis_index("pts"), lax.axis_index("cam")
    streams = [
        pltpu.make_async_copy(source, target, in_sem.at[3 + i])
        for i, (source, target) in enumerate(
            ((hbm_cam, obs_cam), (hbm_point, obs_point), (hbm_seen, observed))
        )
    ]
    for stream in streams:
        stream.start()
    last = n_cam - 1
    chunks = landed.shape[1]
    count = planes.shape[2]
    rows = count * chunks
    span, pitch = rows * LANES, rows + 1
    low_end, high_end = c == 0, c == last
    at_end = jnp.logical_or(low_end, high_end)
    own_base = jnp.where(low_end, 0, rows)
    loads = [
        pltpu.make_async_copy(
            source.at[:, pl.ds(pl.multiple_of(own_base * LANES, LANES), span)], target, in_sem.at[i]
        )
        for i, (source, target) in enumerate(
            ((points, own_points), (gradient, own_gradient), (inverse, own_inverse))
        )
    ]

    @pl.when(at_end)
    def _():
        for load in loads:
            load.start()

    greet("pts", n_pts, p)
    barrier = pltpu.get_barrier_semaphore()

    def peer(step):
        return lax.rem(c + step + n_cam, n_cam)

    @pl.when(c > 0)
    def _():
        pl.semaphore_signal(barrier, inc=1, device_id={"cam": peer(-1)}, device_id_type=MESH)

    @pl.when(c < last)
    def _():
        pl.semaphore_signal(barrier, inc=1, device_id={"cam": peer(1)}, device_id_type=MESH)

    def take_cameras(i, carry):
        for u in range(SPREAD):
            block = i * SPREAD + u
            row = pl.multiple_of(block * 2 * TILES, 2 * TILES)
            buf = buffers[u]
            for t in range(TILES):
                slab = cam_table[tile_block[block * TILES + t]]
                buf[pl.ds(t, 8, stride=PITCH), :] = slab[0:8]
                buf[pl.ds(8 * PITCH + t, 2, stride=PITCH), :] = slab[8:10]
            sources = [buf[PITCH * m : PITCH * m + 8, :] for m in range(10)]
            for h in range(2):
                index = obs_cam[pl.ds(row + h, TILES, stride=2), :]
                for m in range(10):
                    cam_store[m, pl.ds(row + TILES * h, TILES), :] = lane_take(sources[m], index)
        return carry

    turns = obs_cam.shape[0] // (2 * TILES * SPREAD)
    early = turns // 4
    streams[0].wait()
    lax.fori_loop(0, early, take_cameras, 0)
    pl.semaphore_wait(barrier, n_pts - 1 + jnp.where(at_end, 1, 2))

    def place(way, k):
        return k + chunks if way == 0 else k

    def toward(way):
        return peer(1) if way == 0 else peer(-1)

    def sum_copy(way, k, source):
        return pltpu.make_async_remote_copy(
            src_ref=source,
            dst_ref=landed.at[way, k],
            send_sem=send_sum.at[way, k],
            recv_sem=recv_sum.at[way, k],
            device_id={"cam": toward(way)},
            device_id_type=MESH,
        )

    def out_copy(way, k):
        part = out.at[place(way, k)]
        return pltpu.make_async_remote_copy(
            src_ref=part,
            dst_ref=part,
            send_sem=send_out.at[way, k],
            recv_sem=recv_out.at[way, k],
            device_id={"cam": toward(1 - way)},
            device_id_type=MESH,
        )

    for way, first in ((0, low_end), (1, high_end)):

        @pl.when(first)
        def _(way=way):
            def begin(k, carry):
                sum_copy(way, k, planes.at[place(way, k)]).start()
                return carry

            lax.fori_loop(0, chunks, begin, 0)

    lax.fori_loop(early, turns, take_cameras, 0)

    @pl.when(at_end)
    def _():
        for load in loads:
            load.wait()

        def spread(i, carry):
            for u in range(8):
                k = i * 8 + u
                lanes = pl.ds(pl.multiple_of(k * LANES, LANES), LANES)
                work[pl.ds(k, 3, stride=pitch), :] = own_points[:, lanes]
                work[pl.ds(3 * pitch + k, 3, stride=pitch), :] = own_gradient[:, lanes]
                block = own_inverse[:, lanes]
                work[pl.ds(6 * pitch + k, 8, stride=pitch), :] = block[0:8]
                work[pl.ds(14 * pitch + k, 1), :] = block[8:9]
            return carry

        lax.fori_loop(0, rows // 8, spread, 0)

    def solved(way, k):
        def row(m):
            return work[pl.ds(m * pitch + k * count, count), :]

        total = landed[way, k] + planes[place(way, k)]
        residue = [row(3 + n) - total[n] for n in range(3)]
        for n in range(3):
            move = row(6 + 3 * n) * residue[0] + row(7 + 3 * n) * residue[1] + row(8 + 3 * n) * residue[2]
            out[place(way, k), n] = row(n) + move

    def turn(s, carry):
        for way, hops in ((0, c), (1, last - c)):
            k = s - LAG * hops
            live = jnp.logical_and(hops > 0, jnp.logical_and(k >= 0, k < chunks))

            @pl.when(live)
            def _(way=way, k=k, hops=hops):
                sum_copy(way, k, landed.at[way, k]).wait_recv()

                @pl.when(hops < last)
                def _():
                    landed[way, k] = landed[way, k] + planes[place(way, k)]
                    sum_copy(way, k, landed.at[way, k]).start()

                @pl.when(hops == last)
                def _():
                    solved(way, k)
                    out_copy(way, k).start()

        for way, hops in ((0, last - c), (1, c)):
            k = s - LAG * (last + hops)
            live = jnp.logical_and(hops > 0, jnp.logical_and(k >= 0, k < chunks))

            @pl.when(live)
            def _(way=way, k=k, hops=hops):
                out_copy(way, k).wait_recv()

                @pl.when(hops < last)
                def _():
                    out_copy(way, k).start()

        return carry

    lax.fori_loop(0, chunks + 2 * LAG * last, turn, 0)

    def finish(k, carry):
        for way, first, end in ((0, low_end, high_end), (1, high_end, low_end)):

            @pl.when(jnp.logical_not(end))
            def _(way=way):
                sum_copy(way, k, landed.at[way, k]).wait_send()

            @pl.when(jnp.logical_not(first))
            def _(way=way):
                out_copy(way, k).wait_send()

        return carry

    lax.fori_loop(0, chunks, finish, 0)
    point_table[...] = jnp.zeros_like(point_table)
    for i in range(2 * chunks):
        for n in range(3):
            point_table[pl.ds(4 * count * i + n, count, stride=4), :] = out[i, n]
    point_slabs = point_table.reshape(point_table.shape[0] // 8, 8, LANES)
    for stream in streams[1:]:
        stream.wait()

    def project(i, carry):
        for u in range(SPREAD):
            block = i * SPREAD + u
            row = pl.multiple_of(block * 2 * TILES, 2 * TILES)
            buf = buffers[u]
            for t in range(TILES):
                buf[pl.ds(t, 8, stride=PITCH), :] = point_slabs[tile_points[block * TILES + t]]
            sources = [buf[PITCH * m : PITCH * m + 8, :] for m in range(8)]
            for h in range(2):
                point = obs_point[pl.ds(row + h, TILES, stride=2), :]
                local = point & (LANES - 1)
                upper = point >= LANES
                x, y, z = (
                    jnp.where(upper, lane_take(sources[4 + n], local), lane_take(sources[n], local))
                    for n in range(3)
                )
                head, a, b, c, *shift, focal, k1, k2 = (
                    cam_store[m, pl.ds(row + TILES * h, TILES), :] for m in range(10)
                )
                e, f, g = b * z - c * y, c * x - a * z, a * y - b * x
                px = x + shift[0] + (head * e + (b * g - c * f))
                py = y + shift[1] + (head * f + (c * e - a * g))
                pz = z + shift[2] + (head * g + (a * f - b * e))
                scale = 1.0 / jnp.maximum(-pz, 1.0)
                fu, fv = px * scale, py * scale
                q = fu * fu + fv * fv
                factor = focal * (1.0 + q * (k1 + k2 * q))
                at_u = pl.ds(2 * (row + h), TILES, stride=4)
                at_v = pl.ds(2 * (row + h) + 1, TILES, stride=4)
                ru = factor * fu - observed[at_u, :]
                rv = factor * fv - observed[at_v, :]
                residual[at_u, :] = ru
                residual[at_v, :] = rv
                carry = carry + (ru * ru + rv * rv)
        return carry

    cost = lax.fori_loop(0, turns, project, jnp.zeros((8, LANES), jnp.float32))
    me = p * n_cam + c
    slots[pl.ds(me, 1), :] = jnp.sum(cost, axis=0, keepdims=True)
    mine = slots.at[pl.ds(me, 1)]
    copies = []
    for j in range(1, n_pts * n_cam):
        step_p, step_c = j // n_cam, j % n_cam
        copies.append(
            pltpu.make_async_remote_copy(
                src_ref=mine,
                dst_ref=mine,
                send_sem=send_cost.at[j],
                recv_sem=recv_cost.at[j],
                device_id={"pts": lax.rem(p + step_p, n_pts), "cam": lax.rem(c + step_c, n_cam)},
                device_id_type=MESH,
            )
        )
    for copy in reversed(copies):
        copy.start()
    for copy in copies:
        copy.wait()
    sums[...] = jnp.sum(slots[...], axis=0, keepdims=True)


def emit_kernel(
    scale, accept, sums, seen, table, points, cameras, increment, residual, cost, accepted_points, accepted_cameras, sem
):
    copy = pltpu.make_async_copy(seen, residual, sem)
    copy.start()
    odd = (accept[0] & 1) == 1
    accepted_cameras[...] = cameras[...] + odd.astype(jnp.float32) * increment[...]
    cost[0] = jnp.sum(sums[...]) * scale

    def turn(i, carry):
        for u in range(16):
            k = i * 16 + u
            lanes = pl.ds(pl.multiple_of(k * LANES, LANES), LANES)
            accepted_points[:, lanes] = jnp.where(odd, table[pl.ds(4 * k, 3), :], points[:, lanes])
        return carry

    lax.fori_loop(0, table.shape[0] // 64, turn, 0)
    copy.wait()


def on_device(
    cameras, increment, points, point_gradient, point_inverse, cam_jacobian, point_jacobian,
    observed, tile_block, tile_points, obs_camera, obs_point, accept,
):
    own_blocks = cameras.shape[1] // CB
    n_pts, n_cam = lax.axis_size("pts"), lax.axis_size("cam")
    vmem = pl.BlockSpec(memory_space=pltpu.VMEM)
    hbm = pl.BlockSpec(memory_space=pltpu.HBM)

    def dma_sems(*counts):
        return [pltpu.SemaphoreType.DMA((count,)) for count in counts]

    def remote(ident):
        return pltpu.CompilerParams(
            collective_id=ident, has_side_effects=True, vmem_limit_bytes=36 * 2**20
        )

    every = pl.pallas_call(
        functools.partial(gather_kernel, n_pts, n_cam),
        in_specs=[vmem],
        out_specs=vmem,
        out_shape=jax.ShapeDtypeStruct((own_blocks * n_pts * n_cam, 24, CB), jnp.float32),
        scratch_shapes=dma_sems(n_cam - 1, n_cam - 1)
        + [pltpu.SemaphoreType.DMA((n_cam, n_pts - 1))] * 2,
        compiler_params=remote(0),
        cost_estimate=pl.CostEstimate(flops=2**30, bytes_accessed=2**20, transcendentals=0),
        name="cameras",
    )(jnp.stack([cameras, increment]))
    cam_blocks = every.shape[0]
    cam_table = jnp.concatenate([every[:, 9:19], jnp.zeros((cam_blocks, 6, CB), jnp.float32)], axis=1)

    obs_count = obs_camera.shape[0]
    rows = obs_count // LANES
    per = math.gcd(rows, BLOCKS_PER_STEP)
    grid = (rows // per,)
    point_blocks = points.shape[1] // PB
    chunks = math.gcd(point_blocks // 8, CHUNKS)
    oc = obs_camera.reshape(rows, LANES)
    op = obs_point.reshape(rows, LANES)

    def whole(*shape):
        return pl.BlockSpec(shape, lambda i, *_: (0,) * len(shape))

    params = pltpu.CompilerParams(dimension_semantics=("arbitrary",), vmem_limit_bytes=50 * 2**20)
    planes = pl.pallas_call(
        couple_kernel,
        grid_spec=pltpu.PrefetchScalarGridSpec(
            num_scalar_prefetch=2,
            grid=grid,
            in_specs=[
                pl.BlockSpec((18, per * LANES), lambda i, *_: (0, i)),
                pl.BlockSpec((6, per * LANES), lambda i, *_: (0, i)),
                pl.BlockSpec((per, LANES), lambda i, *_: (i, 0)),
                pl.BlockSpec((per, LANES), lambda i, *_: (i, 0)),
                whole(cam_blocks, 24, CB),
            ],
            out_specs=whole(2 * chunks, 3, point_blocks // chunks, LANES),
            scratch_shapes=[
                pltpu.VMEM((point_blocks * 8, LANES), jnp.float32),
            ]
            + [pltpu.VMEM((point_blocks * COARSE_ROWS, FINE), jnp.float32)] * SPLIT
            + [
                pltpu.VMEM((count * PITCH, LANES), jnp.float32) for count in (9, 24, 24, 10, 10)
            ]
            * PAIRS,
        ),
        out_shape=jax.ShapeDtypeStruct((2 * chunks, 3, point_blocks // chunks, LANES), jnp.float32),
        compiler_params=params,
        name="couple",
    )(tile_block, tile_points, cam_jacobian, point_jacobian, oc, op, every)

    own_rows = point_blocks
    anywhere = pl.BlockSpec(memory_space=pl.ANY)
    smem = pl.BlockSpec(memory_space=pltpu.SMEM)
    seen = observed.reshape(2, rows, LANES).transpose(1, 0, 2).reshape(2 * rows, LANES)
    residual, point_table, sums = pl.pallas_call(
        functools.partial(finish_kernel, n_pts, n_cam),
        in_specs=[smem, smem, vmem, vmem] + [anywhere] * 6,
        out_specs=[vmem, vmem, vmem],
        out_shape=[
            jax.ShapeDtypeStruct((2 * rows, LANES), jnp.float32),
            jax.ShapeDtypeStruct((point_blocks * 8, LANES), jnp.float32),
            jax.ShapeDtypeStruct((1, LANES), jnp.float32),
        ],
        scratch_shapes=[
            pltpu.VMEM(planes.shape, jnp.float32),
            pltpu.VMEM((2, chunks, 3, own_rows // chunks, LANES), jnp.float32),
            pltpu.VMEM((3, own_rows * LANES), jnp.float32),
            pltpu.VMEM((3, own_rows * LANES), jnp.float32),
            pltpu.VMEM((9, own_rows * LANES), jnp.float32),
            pltpu.VMEM((15 * (own_rows + 1), LANES), jnp.float32),
            pltpu.VMEM((rows, LANES), jnp.int32),
            pltpu.VMEM((rows, LANES), jnp.int32),
            pltpu.VMEM((2 * rows, LANES), jnp.float32),
            pltpu.VMEM((10, rows, LANES), jnp.float32),
            pltpu.VMEM((n_pts * n_cam, LANES), jnp.float32),
            pltpu.SemaphoreType.DMA((6,)),
        ]
        + [pltpu.SemaphoreType.DMA((2, chunks))] * 4
        + dma_sems(n_pts * n_cam, n_pts * n_cam)
        + [pltpu.VMEM((10 * PITCH, LANES), jnp.float32)] * SPREAD,
        compiler_params=remote(1),
        name="finish",
    )(
        tile_block, tile_points, planes, cam_table, points, point_gradient,
        point_inverse, oc, op, seen,
    )
    residual, cost, accepted_points, accepted_cameras = pl.pallas_call(
        functools.partial(emit_kernel, 1.0 / (2.0 * obs_count * n_pts * n_cam)),
        in_specs=[smem] + [vmem] * 6,
        out_specs=[anywhere, smem, vmem, vmem],
        out_shape=[
            jax.ShapeDtypeStruct((2 * rows, LANES), jnp.float32),
            jax.ShapeDtypeStruct((1,), jnp.float32),
            jax.ShapeDtypeStruct(points.shape, jnp.float32),
            jax.ShapeDtypeStruct(cameras.shape, jnp.float32),
        ],
        scratch_shapes=[pltpu.SemaphoreType.DMA],
        compiler_params=pltpu.CompilerParams(vmem_limit_bytes=16 * 2**20),
        name="emit",
    )(accept.reshape(1), sums, residual, point_table, points, cameras, increment)
    residual = residual.reshape(rows, 2, LANES).transpose(1, 0, 2).reshape(2, obs_count)
    return residual, cost.reshape(()), accepted_points, accepted_cameras


def solution(mesh):
    in_specs = (
        P(None, ("pts", "cam")),
        P(None, ("pts", "cam")),
        P(None, "pts"),
        P(None, "pts"),
        P(None, "pts"),
        P(None, ("pts", "cam")),
        P(None, ("pts", "cam")),
        P(None, ("pts", "cam")),
        P(("pts", "cam")),
        P(("pts", "cam")),
        P(("pts", "cam")),
        P(("pts", "cam")),
        P(),
    )
    out_specs = (P(None, ("pts", "cam")), P(), P(None, "pts"), P(None, ("pts", "cam")))
    return jax.shard_map(
        on_device, mesh=mesh, in_specs=in_specs, out_specs=out_specs, check_vma=False
    )
```
